32 devices in a mesh: freq: 8 (over z, y), cell: 4 (over x, core).
Axes of the slice: x: 2, y: 2, z: 4, core: 2. Of those that a mesh axis runs over, the one named last changes fastest.
Arguments:
- columns: float32 [2, 16, 64, 600], P(None, 'freq'), may hold values from -6 to 6
- freq_blocks: float32 [2, 16, 600, 1024], P(None, 'freq', None, 'cell'), may hold values from -0.1875 to 0.1875
- causal_cutoffs: int32 [64], replicated, may hold values from 3 to 15
- band_index: int32 [1024], P('cell'), may hold values from 0 to 7
- band_rates: float32 [8], replicated, may hold values from 0.05 to 0.45
Outputs:
- hessian_columns: float32 [2, 16, 64, 600], P(None, 'freq', 'cell')
The draws below stay inside these ranges and needn't reach their ends.
All inputs are finite; a program needn't handle non-finite values.
Results may differ from the reference program's by a relative error of at most 0.00007.
Values sent between devices are 32-bit elements; how exact they have to be, the bound alone decides.
No kernel may reach another device: no remote copies, remote signals or barrier semaphores. Data moves between devices by JAX's collectives and lax.ppermute only.
A program may use at most 64 MiB of HBM per device.

```python
import math
import jax
import jax.numpy as jnp
from jax import lax

NS = 600
SWEEPS = 4
BANDS = 8
NF = 16
EPOCH_LENGTH = 15
CURVATURE_RANKS = 64
NM = 1024


def place_ends(result, stream_key, least, largest):
    longest = result.shape.index(max(result.shape))
    spots = []
    for shift in (0, 1):
        where = [jax.random.randint(jax.random.fold_in(stream_key, axis), (), 0, length) for axis, length in enumerate(result.shape)]
        where[longest] = (where[longest] + shift) % result.shape[longest]
        spots.append(tuple(where))
    return result.at[spots[0]].set(least).at[spots[1]].set(largest)


def level_of(key, shape, split, smallest, top_value):
    level, own = 1.0, jax.random.fold_in(key, 6)
    for dim, shards_of in split:
        steps = jnp.exp(jax.random.uniform(jax.random.fold_in(own, dim), (shards_of,), jnp.float32, smallest / len(split), top_value / len(split)))
        level = level * jnp.repeat(steps, shape[dim] // shards_of).reshape([-1 if axis == dim else 1 for axis in range(len(shape))])
    return level


def scatter_about(rng, shape, width, most, cuts=(), dtype=jnp.bfloat16):
    drawn = width * jax.random.normal(rng, shape, jnp.float32)
    if cuts:
        drawn = drawn * level_of(rng, shape, cuts, -0.22, 0.18)
    return jnp.clip(drawn, -most, most).astype(dtype)


def setup_inputs(seed: int = 0) -> dict:
    streams_of = jax.random.split(jax.random.key(seed), 6)
    columns = scatter_about(streams_of[0], (2, NF, CURVATURE_RANKS, NS), 1.0, 6.0, ((1, 8),), jnp.float32)
    freq_blocks = scatter_about(streams_of[1], (2, NF, NS, NM), NM ** -0.5, 0.1875, ((1, 8), (3, 4)), jnp.float32)
    causal_cutoffs = place_ends(jax.random.randint(streams_of[2], (CURVATURE_RANKS,), EPOCH_LENGTH // 4, EPOCH_LENGTH + 1), jax.random.fold_in(streams_of[2], 1), EPOCH_LENGTH // 4, EPOCH_LENGTH).astype(jnp.int32)
    band_index = place_ends(jax.random.randint(streams_of[3], (NM,), 0, BANDS), jax.random.fold_in(streams_of[3], 1), 0, BANDS - 1).astype(jnp.int32)
    band_rates = jnp.clip(jax.random.uniform(streams_of[4], (BANDS,), jnp.float32, 0.05, 0.45), 0.05, 0.45)
    return {"columns": columns, "freq_blocks": freq_blocks, "causal_cutoffs": causal_cutoffs, "band_index": band_index, "band_rates": band_rates}


precise = lax.Precision.HIGHEST


def inverse_table(epoch_number, harmonic_number):
    cycle_length = 2 * epoch_number
    sample_moments = lax.broadcasted_iota(jnp.int32, (epoch_number, harmonic_number), 0)
    harmonic_rate = lax.broadcasted_iota(jnp.int32, (epoch_number, harmonic_number), 1)
    harmonic_offsets = ((sample_moments * harmonic_rate) % cycle_length).astype(jnp.float32) * (2.0 * math.pi / cycle_length)
    weight = jnp.where((harmonic_rate == 0) | (harmonic_rate == harmonic_number - 1), 1.0, 2.0).astype(jnp.float32) / cycle_length
    return jnp.concatenate([weight * jnp.cos(harmonic_offsets), -weight * jnp.sin(harmonic_offsets)], axis=1)


def forward_table(epoch_number, harmonic_number):
    cycle_length = 2 * epoch_number
    harmonic_rate = lax.broadcasted_iota(jnp.int32, (harmonic_number, epoch_number), 0)
    sample_moments = lax.broadcasted_iota(jnp.int32, (harmonic_number, epoch_number), 1)
    harmonic_offsets = ((sample_moments * harmonic_rate) % cycle_length).astype(jnp.float32) * (2.0 * math.pi / cycle_length)
    return jnp.concatenate([jnp.cos(harmonic_offsets), -jnp.sin(harmonic_offsets)], axis=0)


def adjoint_product(columns, blocks):
    real_part = jnp.einsum('kjs,ksm->kjm', columns[0], blocks[0], precision=precise) + jnp.einsum('kjs,ksm->kjm', columns[1], blocks[1], precision=precise)
    imag_part = jnp.einsum('kjs,ksm->kjm', columns[1], blocks[0], precision=precise) - jnp.einsum('kjs,ksm->kjm', columns[0], blocks[1], precision=precise)
    return jnp.stack([real_part, imag_part])


def forward_product(spectrum, blocks):
    real_part = jnp.einsum('kjm,ksm->kjs', spectrum[0], blocks[0], precision=precise) - jnp.einsum('kjm,ksm->kjs', spectrum[1], blocks[1], precision=precise)
    imag_part = jnp.einsum('kjm,ksm->kjs', spectrum[1], blocks[0], precision=precise) + jnp.einsum('kjm,ksm->kjs', spectrum[0], blocks[1], precision=precise)
    return jnp.stack([real_part, imag_part])


def reference(columns, freq_blocks, causal_cutoffs, band_index, band_rates):
    spectrum = adjoint_product(columns, freq_blocks)
    sampled_trace = jnp.dot(inverse_table(EPOCH_LENGTH, NF), spectrum.reshape(2 * NF, CURVATURE_RANKS * NM), precision=precise, preferred_element_type=jnp.float32)
    sampled_trace = sampled_trace.reshape(EPOCH_LENGTH, CURVATURE_RANKS, NM)
    sample_moments = lax.broadcasted_iota(jnp.int32, (EPOCH_LENGTH, CURVATURE_RANKS), 0)
    sampled_trace = jnp.where((sample_moments < causal_cutoffs[None, :])[:, :, None], sampled_trace, 0.0)
    cell_rates = jnp.take(band_rates, band_index)
    for repeat in range(SWEEPS):
        padded = jnp.pad(sampled_trace, ((0, 0), (0, 0), (1, 1)))
        sampled_trace = sampled_trace + cell_rates * (padded[:, :, :-2] - 2.0 * sampled_trace + padded[:, :, 2:])
    spectrum = jnp.dot(forward_table(EPOCH_LENGTH, NF), sampled_trace.reshape(EPOCH_LENGTH, CURVATURE_RANKS * NM), precision=precise, preferred_element_type=jnp.float32)
    spectrum = spectrum.reshape(2, NF, CURVATURE_RANKS, NM)
    return forward_product(spectrum, freq_blocks)
```

```python
import math

import jax
import jax.numpy as jnp
from jax import lax
from jax.sharding import PartitionSpec as P

MODE_SHARE_WIDTH = 8
C_DEV = 256
SWEEPS = 4
BANDS = 8


precise = lax.Precision.HIGHEST


def extended(shard, sides, width):
    for axis, dim in sides:
        devices, length = (lax.axis_size(axis), shard.shape[dim])
        up = [(i, (i + 1) % devices) for i in range(devices - 1)]
        down = [(j, i) for i, j in up]
        last = lax.slice_in_dim(shard, length - width, length, axis=dim)
        leading = lax.slice_in_dim(shard, 0, width, axis=dim)
        before = lax.ppermute(last, axis, up)
        after = lax.ppermute(leading, axis, down)
        shard = jnp.concatenate([before, shard, after], axis=dim)
    return shard


def inverse_table(epoch_number, harmonic_number):
    cycle_length = 2 * epoch_number
    sample_moments = lax.broadcasted_iota(jnp.int32, (epoch_number, harmonic_number), 0)
    harmonic_rate = lax.broadcasted_iota(jnp.int32, (epoch_number, harmonic_number), 1)
    harmonic_offsets = (sample_moments * harmonic_rate % cycle_length).astype(jnp.float32) * (
        2.0 * math.pi / cycle_length
    )
    weight = (
        jnp.where((harmonic_rate == 0) | (harmonic_rate == harmonic_number - 1), 1.0, 2.0).astype(
            jnp.float32
        )
        / cycle_length
    )
    return jnp.concatenate(
        [weight * jnp.cos(harmonic_offsets), -weight * jnp.sin(harmonic_offsets)], axis=1
    )


def forward_table(epoch_number, harmonic_number):
    cycle_length = 2 * epoch_number
    harmonic_rate = lax.broadcasted_iota(jnp.int32, (harmonic_number, epoch_number), 0)
    sample_moments = lax.broadcasted_iota(jnp.int32, (harmonic_number, epoch_number), 1)
    harmonic_offsets = (sample_moments * harmonic_rate % cycle_length).astype(jnp.float32) * (
        2.0 * math.pi / cycle_length
    )
    return jnp.concatenate([jnp.cos(harmonic_offsets), -jnp.sin(harmonic_offsets)], axis=0)


def adjoint_product(columns, blocks):
    real_part = jnp.einsum("kjs,ksm->kjm", columns[0], blocks[0], precision=precise) + jnp.einsum(
        "kjs,ksm->kjm", columns[1], blocks[1], precision=precise
    )
    imag_part = jnp.einsum("kjs,ksm->kjm", columns[1], blocks[0], precision=precise) - jnp.einsum(
        "kjs,ksm->kjm", columns[0], blocks[1], precision=precise
    )
    return jnp.stack([real_part, imag_part])


def forward_product(spectrum, blocks):
    real_part = jnp.einsum("kjm,ksm->kjs", spectrum[0], blocks[0], precision=precise) - jnp.einsum(
        "kjm,ksm->kjs", spectrum[1], blocks[1], precision=precise
    )
    imag_part = jnp.einsum("kjm,ksm->kjs", spectrum[1], blocks[0], precision=precise) + jnp.einsum(
        "kjm,ksm->kjs", spectrum[0], blocks[1], precision=precise
    )
    return jnp.stack([real_part, imag_part])


def on_device(columns, freq_blocks, causal_cutoffs, band_index, band_rates):
    col_total = columns.shape[2]
    local_spectrum = adjoint_product(columns, freq_blocks)
    gathered = lax.all_to_all(local_spectrum, "freq", split_axis=2, concat_axis=1, tiled=True)
    freq_total = gathered.shape[1]
    horizon_span = freq_total - 1
    sampled_trace = jnp.dot(
        inverse_table(horizon_span, freq_total),
        gathered.reshape(2 * freq_total, MODE_SHARE_WIDTH * C_DEV),
        precision=precise,
        preferred_element_type=jnp.float32,
    )
    sampled_trace = sampled_trace.reshape(horizon_span, MODE_SHARE_WIDTH, C_DEV)
    device_ranges = lax.dynamic_slice_in_dim(
        causal_cutoffs, lax.axis_index("freq") * MODE_SHARE_WIDTH, MODE_SHARE_WIDTH
    )
    sample_moments = lax.broadcasted_iota(jnp.int32, (horizon_span, MODE_SHARE_WIDTH), 0)
    sampled_trace = jnp.where(
        (sample_moments < device_ranges[None, :])[:, :, None], sampled_trace, 0.0
    )
    flat = sampled_trace.reshape(horizon_span * MODE_SHARE_WIDTH, C_DEV)
    levels = lax.broadcasted_iota(jnp.int32, (BANDS, C_DEV), 0)
    cell_rates = jnp.sum(jnp.where(levels == band_index[None, :], band_rates[:, None], 0.0), axis=0)
    stacked = jnp.concatenate([flat, cell_rates[None, :]], axis=0)
    padded = extended(stacked, (("cell", 1),), SWEEPS)
    field = padded[:-1]
    margin_rates = padded[-1]
    for repeat in range(SWEEPS):
        inner_rates = margin_rates[1:-1]
        field = field[:, 1:-1] + inner_rates * (field[:, :-2] - 2.0 * field[:, 1:-1] + field[:, 2:])
        margin_rates = inner_rates
    flat = field
    spectrum = jnp.dot(
        forward_table(horizon_span, freq_total),
        flat.reshape(horizon_span, MODE_SHARE_WIDTH * C_DEV),
        precision=precise,
        preferred_element_type=jnp.float32,
    )
    spectrum = spectrum.reshape(2, freq_total, MODE_SHARE_WIDTH, C_DEV)
    returned = lax.all_to_all(spectrum, "freq", split_axis=1, concat_axis=2, tiled=True)
    partial_terms = forward_product(returned, freq_blocks)
    share = col_total // lax.axis_size("cell")
    blocks = partial_terms.reshape(partial_terms.shape[:2] + (lax.axis_size("cell"), share, partial_terms.shape[3]))
    mine = lax.all_to_all(blocks, "cell", split_axis=2, concat_axis=2, tiled=True)
    return jnp.sum(mine, axis=2)


def solution(mesh):
    placed = (P(None, "freq", None, None), P(None, "freq", None, "cell"), P(), P("cell"), P())
    return jax.shard_map(
        on_device,
        mesh=mesh,
        in_specs=placed,
        out_specs=P(None, "freq", "cell", None),
        check_vma=False,
    )
```

```python
import math

import jax
import jax.numpy as jnp
import numpy as np
from jax import lax
from jax.experimental import pallas as pl
from jax.experimental.pallas import tpu as pltpu
from jax.sharding import PartitionSpec as P

SWEEPS = 4
BANDS = 8
ROWS = 8
LANES = 128
UNROLLED_FREQS = 32


def split(x):
    high = x.astype(jnp.bfloat16)
    return high, (x - high.astype(jnp.float32)).astype(jnp.bfloat16)


def product(a, b, contract):
    return lax.dot_general(a, b, (contract, ((), ())), preferred_element_type=jnp.float32)


def inverse_table(steps, freqs):
    cycle = 2 * steps
    turns = np.outer(np.arange(steps), np.arange(freqs)) % cycle
    angle = turns * (2.0 * math.pi / cycle)
    weight = np.where((np.arange(freqs) == 0) | (np.arange(freqs) == freqs - 1), 1.0, 2.0) / cycle
    return weight * np.cos(angle), -weight * np.sin(angle)


def forward_table(steps, freqs):
    cycle = 2 * steps
    turns = np.outer(np.arange(freqs), np.arange(steps)) % cycle
    angle = turns * (2.0 * math.pi / cycle)
    return np.cos(angle), -np.sin(angle)


def adjoint_kernel(v_ref, f_ref, out_ref, parts):
    part = pl.program_id(1)
    shards, _, _, rows, cells = out_ref.shape
    cols = v_ref.shape[2]

    @pl.when(part == 0)
    def _():
        for c in range(2):
            high, low = split(v_ref[c, 0])
            parts[c * cols : (c + 1) * cols] = high
            parts[(2 + c) * cols : (3 + c) * cols] = low

    high, low = split(f_ref[0, 0])
    both = product(parts[...], high, ((1,), (0,)))
    both = both[: 2 * cols] + both[2 * cols :] + product(parts[: 2 * cols], low, ((1,), (0,)))
    first = both[:cols].reshape(shards, rows, cells)
    second = both[cols:].reshape(shards, rows, cells)

    @pl.when(part == 0)
    def _():
        out_ref[:, 0, 0] = first
        out_ref[:, 1, 0] = second

    @pl.when(part == 1)
    def _():
        out_ref[:, 0, 0] += second
        out_ref[:, 1, 0] -= first


def adjoint(columns, blocks, shards):
    _, freqs, cols, sensors = columns.shape
    cells = blocks.shape[3]
    return pl.pallas_call(
        adjoint_kernel,
        grid=(freqs, 2),
        in_specs=[
            pl.BlockSpec((2, 1, cols, sensors), lambda k, c: (0, k, 0, 0)),
            pl.BlockSpec((1, 1, sensors, cells), lambda k, c: (c, k, 0, 0)),
        ],
        out_specs=pl.BlockSpec((shards, 2, 1, cols // shards, cells), lambda k, c: (0, 0, k, 0, 0)),
        out_shape=jax.ShapeDtypeStruct((shards, 2, freqs, cols // shards, cells), jnp.float32),
        scratch_shapes=[pltpu.VMEM((4 * cols, sensors), jnp.bfloat16)],
        cost_estimate=pl.CostEstimate(
            flops=24 * freqs * cols * sensors * cells, bytes_accessed=8 * freqs * sensors * cells, transcendentals=0
        ),
        name="adjoint",
    )(columns, blocks)


def middle_kernel(x_ref, cut_ref, out_ref):
    shards, _, held, rows, cells = x_ref.shape
    freqs = shards * held
    steps = freqs - 1
    half = freqs // 2
    to_cos, to_sin = inverse_table(steps, freqs)
    from_cos, from_sin = forward_table(steps, freqs)
    base = lax.axis_index("freq") * rows
    row = lax.broadcasted_iota(jnp.int32, (rows, LANES), 0)
    cutoff = jnp.zeros((rows, LANES), jnp.int32)
    for r in range(rows):
        cutoff = jnp.where(row == r, cut_ref[base + r], cutoff)
    for lane in range(0, cells, LANES):
        at = pl.ds(lane, LANES)
        even, odd = [], []
        for k in range(half):
            a, b = divmod(k, held)
            c, d = divmod(freqs - 1 - k, held)
            re, im = x_ref[a, 0, b, :, at], x_ref[a, 1, b, :, at]
            re2, im2 = x_ref[c, 0, d, :, at], x_ref[c, 1, d, :, at]
            even += [re + re2, im - im2]
            odd += [re - re2, im + im2]
        series = []
        for t in range(steps):
            total = None
            for k in range(half):
                pair = odd if t % 2 else even
                for value, table in ((pair[2 * k], to_cos), (pair[2 * k + 1], to_sin)):
                    term = value * float(table[t, k])
                    total = term if total is None else total + term
            series.append(jnp.where(cutoff > t, total, 0.0))
        for k in range(half):
            a, b = divmod(k, held)
            c, d = divmod(freqs - 1 - k, held)
            sums = []
            for table in (from_cos, from_sin):
                for parity in (0, 1):
                    total = None
                    for t in range(parity, steps, 2):
                        term = series[t] * float(table[k, t])
                        total = term if total is None else total + term
                    sums.append(total)
            out_ref[a, 0, b, :, at] = sums[0] + sums[1]
            out_ref[c, 0, d, :, at] = sums[0] - sums[1]
            out_ref[a, 1, b, :, at] = sums[2] + sums[3]
            out_ref[c, 1, d, :, at] = sums[3] - sums[2]


def middle(gathered, causal_cutoffs):
    shards, _, held, rows, cells = gathered.shape
    freqs = shards * held
    steps = freqs - 1
    if freqs <= UNROLLED_FREQS and freqs % 2 == 0:
        return pl.pallas_call(
            middle_kernel,
            in_specs=[pl.BlockSpec(memory_space=pltpu.VMEM), pl.BlockSpec(memory_space=pltpu.SMEM)],
            out_specs=pl.BlockSpec(memory_space=pltpu.VMEM),
            out_shape=jax.ShapeDtypeStruct(gathered.shape, jnp.float32),
            cost_estimate=pl.CostEstimate(
                flops=8 * freqs * steps * rows * cells, bytes_accessed=16 * freqs * rows * cells, transcendentals=0
            ),
            name="middle",
        )(gathered, causal_cutoffs)
    to_time = jnp.asarray(np.concatenate(inverse_table(steps, freqs), axis=1), jnp.float32)
    to_freq = jnp.asarray(np.concatenate(forward_table(steps, freqs), axis=0), jnp.float32)
    x = gathered.transpose(1, 0, 2, 3, 4).reshape(2 * freqs, rows * cells)
    series = jnp.dot(to_time, x, precision=lax.Precision.HIGHEST).reshape(steps, rows, cells)
    cutoff = lax.dynamic_slice_in_dim(causal_cutoffs, lax.axis_index("freq") * rows, rows)
    moment = lax.broadcasted_iota(jnp.int32, (steps, rows), 0)
    series = jnp.where((moment < cutoff[None, :])[:, :, None], series, 0.0)
    x = jnp.dot(to_freq, series.reshape(steps, rows * cells), precision=lax.Precision.HIGHEST)
    return x.reshape(2, shards, held, rows, cells).transpose(1, 0, 2, 3, 4)


def edges_kernel(left_ref, right_ref, band_ref, rates_ref, first_ref, last_ref):
    held = left_ref.shape[1]
    cells = band_ref.shape[1]
    rates = rates_of(band_ref, rates_ref)
    for c in range(2):
        for k in range(held):
            first_ref[c * held + k] = left_ref[c, k].T[:ROWS]
            last_ref[c * held + k] = right_ref[c, k].T[LANES - ROWS :]
    sensors = first_ref.shape[2]
    for ref, lanes, rows in (
        (first_ref, rates[:, :LANES], slice(0, ROWS)),
        (last_ref, rates[:, cells - LANES :], slice(LANES - ROWS, LANES)),
    ):
        spread = jnp.broadcast_to(lanes, (LANES, LANES)).T[rows]
        ref[2 * held] = jnp.zeros((ROWS, sensors), jnp.float32)
        ref[2 * held, :, :LANES] = spread


def rates_of(band_ref, rates_ref):
    band = band_ref[...]
    rates = jnp.zeros(band.shape, jnp.float32)
    for b in range(BANDS):
        rates = jnp.where(band == b, rates_ref[b], rates)
    return rates


def edges(blocks, band_index, band_rates):
    _, held, sensors, cells = blocks.shape
    last = cells // LANES - 1
    shape = jax.ShapeDtypeStruct((2 * held + 1, ROWS, sensors), jnp.float32)
    return pl.pallas_call(
        edges_kernel,
        grid=(1,),
        in_specs=[
            pl.BlockSpec((2, held, sensors, LANES), lambda i: (0, 0, 0, 0)),
            pl.BlockSpec((2, held, sensors, LANES), lambda i: (0, 0, 0, last)),
            pl.BlockSpec((1, cells), lambda i: (0, 0)),
            pl.BlockSpec(memory_space=pltpu.SMEM),
        ],
        out_specs=[pl.BlockSpec(shape.shape, lambda i: (0, 0, 0))] * 2,
        out_shape=[shape, shape],
        cost_estimate=pl.CostEstimate(flops=10**8, bytes_accessed=16 * held * sensors * LANES, transcendentals=0),
        name="edges",
    )(blocks, blocks, band_index.reshape(1, cells), band_rates)


def smooth_kernel(f_ref, before_ref, after_ref, band_ref, rates_ref, high_ref, low_ref, a_high, a_low):
    held = pl.num_programs(0)
    cells = f_ref.shape[3]
    width = cells + LANES
    k, c = pl.program_id(0), pl.program_id(1)

    @pl.when((k == 0) & (c == 0))
    def _():
        lane = lax.broadcasted_iota(jnp.int32, (1, LANES), 1)
        side = jnp.zeros((1, LANES), jnp.float32)
        for i in range(ROWS):
            side = jnp.where(lane == i, after_ref[2 * held, i : i + 1, :LANES], side)
            side = jnp.where(lane == LANES - ROWS + i, before_ref[2 * held, i : i + 1, :LANES], side)
        rates = jnp.concatenate([rates_of(band_ref, rates_ref), side], axis=1)
        step = 2 * ROWS

        def build(i, carry):
            row = lax.broadcasted_iota(jnp.int32, (step, width), 0) + i * step
            spot = jnp.where(row < cells + ROWS, row, row + (width - cells - 2 * ROWS))
            w = jnp.where(lax.broadcasted_iota(jnp.int32, (step, width), 1) == spot, 1.0, 0.0)
            for _ in range(SWEEPS):
                z = rates * w
                w = w - 2.0 * z + pltpu.roll(z, 1, 1) + pltpu.roll(z, width - 1, 1)
            high, low = split(w[:, :cells])
            at = pl.ds(pl.multiple_of(i * step, step), step)
            a_high[at] = high
            a_low[at] = low
            return carry

        lax.fori_loop(0, cells // step + 1, build, 0)

    high, low = split(f_ref[0, 0])
    own = slice(0, cells)
    total = product(high, a_high[own], ((1,), (0,))) + product(low, a_high[own], ((1,), (0,)))
    total += product(high, a_low[own], ((1,), (0,)))
    at = c * held + k
    halo = jnp.concatenate([after_ref[at], before_ref[at]], axis=0)
    high, low = split(halo)
    beyond = slice(cells, cells + 2 * ROWS)
    halo = jnp.concatenate([high, low, high], axis=0)
    matrix = jnp.concatenate([a_high[beyond], a_high[beyond], a_low[beyond]], axis=0)
    total += product(halo, matrix, ((0,), (0,)))
    high, low = split(total)
    high_ref[0, 0] = high
    low_ref[0, 0] = low


def smooth(blocks, before, after, band_index, band_rates):
    _, held, sensors, cells = blocks.shape
    shape = jax.ShapeDtypeStruct(blocks.shape, jnp.bfloat16)
    block = pl.BlockSpec((1, 1, sensors, cells), lambda k, c: (c, k, 0, 0))
    edge = pl.BlockSpec(before.shape, lambda k, c: (0, 0, 0))
    return pl.pallas_call(
        smooth_kernel,
        grid=(held, 2),
        in_specs=[
            block,
            edge,
            edge,
            pl.BlockSpec((1, cells), lambda k, c: (0, 0)),
            pl.BlockSpec(memory_space=pltpu.SMEM),
        ],
        out_specs=[block, block],
        out_shape=[shape, shape],
        scratch_shapes=[pltpu.VMEM((cells + 2 * ROWS, cells), jnp.bfloat16)] * 2,
        cost_estimate=pl.CostEstimate(
            flops=12 * held * sensors * cells * cells, bytes_accessed=16 * held * sensors * cells, transcendentals=0
        ),
        name="smooth",
    )(blocks, before, after, band_index.reshape(1, cells), band_rates)


def forward_kernel(x_ref, high_ref, low_ref, out_ref):
    _, chips, _, held, share, sensors = out_ref.shape
    per = share // ROWS
    cell = lax.axis_index("cell")
    chip, core = cell // 2, cell % 2
    cells = x_ref.shape[4]
    order = []
    for q in range(2):
        for s in range(chips):
            target = 2 * lax.rem(chip + s, chips) + (core if q == 0 else 1 - core)
            order.append(target * per)
    rows = 2 * chips * share
    for k in range(held):
        parts = []
        for c in range(2):
            for first in order:
                parts.append(x_ref[pl.ds(first, per), c, k].reshape(share, cells))
        high, low = split(jnp.concatenate(parts, axis=0))
        both = jnp.concatenate([high, low], axis=0)
        terms = []
        for c in range(2):
            wide = product(both, high_ref[c, k], ((1,), (1,)))
            terms.append(wide[: 2 * rows] + wide[2 * rows :] + product(high, low_ref[c, k], ((1,), (1,))))
        re = terms[0][:rows] - terms[1][rows:]
        im = terms[0][rows:] + terms[1][:rows]
        out_ref[:, :, 0, k] = re.reshape(2, chips, share, sensors)
        out_ref[:, :, 1, k] = im.reshape(2, chips, share, sensors)


def forward(returned, high, low, chips):
    shards, _, held, rows, cells = returned.shape
    sensors = high.shape[2]
    share = shards * rows // (2 * chips)
    vmem = pl.BlockSpec(memory_space=pltpu.VMEM)
    return pl.pallas_call(
        forward_kernel,
        in_specs=[vmem, vmem, vmem],
        out_specs=vmem,
        out_shape=jax.ShapeDtypeStruct((2, chips, 2, held, share, sensors), jnp.float32),
        cost_estimate=pl.CostEstimate(
            flops=24 * held * shards * rows * sensors * cells,
            bytes_accessed=8 * held * sensors * cells,
            transcendentals=0,
        ),
        name="forward",
    )(returned, high, low)


def on_device(columns, freq_blocks, causal_cutoffs, band_index, band_rates):
    shards, strips = lax.axis_size("freq"), lax.axis_size("cell")
    chips = strips // 2
    spectrum = adjoint(columns, freq_blocks, shards)
    gathered = lax.all_to_all(spectrum, "freq", split_axis=0, concat_axis=0, tiled=True)
    first, last = edges(freq_blocks, band_index, band_rates)
    before = lax.ppermute(last, "cell", [(i, i + 1) for i in range(strips - 1)])
    after = lax.ppermute(first, "cell", [(i + 1, i) for i in range(strips - 1)])
    high, low = smooth(freq_blocks, before, after, band_index, band_rates)
    spectrum = middle(gathered, causal_cutoffs)
    returned = lax.all_to_all(spectrum, "freq", split_axis=0, concat_axis=0, tiled=True)
    partial_terms = forward(returned, high, low, chips)
    other = lax.ppermute(partial_terms[1], "cell", [(i, i ^ 1) for i in range(strips)])
    total = partial_terms[0] + other
    result = total[0]
    for s in range(1, chips):
        pairs = [(i, 2 * ((i // 2 + s) % chips) + i % 2) for i in range(strips)]
        result = result + lax.ppermute(total[s], "cell", pairs)
    return result


def solution(mesh):
    placed = (P(None, "freq", None, None), P(None, "freq", None, "cell"), P(), P("cell"), P())
    return jax.shard_map(
        on_device,
        mesh=mesh,
        in_specs=placed,
        out_specs=P(None, "freq", "cell", None),
        check_vma=False,
    )
```

```python
import math

import jax
import jax.numpy as jnp
import numpy as np
from jax import lax
from jax.experimental import pallas as pl
from jax.experimental.pallas import tpu as pltpu
from jax.sharding import PartitionSpec as P

SWEEPS = 4
BANDS = 8
ROWS = 8
LANES = 128
UNROLLED_FREQS = 32


VMEM_SPEC = pl.BlockSpec(memory_space=pltpu.VMEM)


def grant(mib):
    return pltpu.CompilerParams(vmem_limit_bytes=mib * 2**20)


def split(x):
    high = x.astype(jnp.bfloat16)
    return high, (x - high.astype(jnp.float32)).astype(jnp.bfloat16)


def product(a, b, contract):
    return lax.dot_general(a, b, (contract, ((), ())), preferred_element_type=jnp.float32)


def inverse_table(steps, freqs):
    cycle = 2 * steps
    turns = np.outer(np.arange(steps), np.arange(freqs)) % cycle
    angle = turns * (2.0 * math.pi / cycle)
    weight = np.where((np.arange(freqs) == 0) | (np.arange(freqs) == freqs - 1), 1.0, 2.0) / cycle
    return weight * np.cos(angle), -weight * np.sin(angle)


def forward_table(steps, freqs):
    cycle = 2 * steps
    turns = np.outer(np.arange(freqs), np.arange(steps)) % cycle
    angle = turns * (2.0 * math.pi / cycle)
    return np.cos(angle), -np.sin(angle)


def adjoint_kernel(v_hbm, f_hbm, out_ref, v_ref, f_ref, v_sem, f_sem):
    shards, _, held, rows, cells = out_ref.shape
    cols = v_ref.shape[2]
    v_copies, f_copies = [], []
    for k in range(held):
        v_copies.append(pltpu.make_async_copy(v_hbm.at[:, k], v_ref.at[:, k], v_sem.at[k]))
        v_copies[k].start()
        for c in range(2):
            copy = pltpu.make_async_copy(f_hbm.at[c, k], f_ref.at[c, k], f_sem.at[2 * k + c])
            f_copies.append(copy)
            copy.start()
    for k in range(held):
        v_copies[k].wait()
        high, low = split(v_ref[:, k].reshape(2 * cols, v_ref.shape[3]))
        parts = jnp.concatenate([high, low], axis=0)
        sums = []
        for c in range(2):
            f_copies[2 * k + c].wait()
            f_high, f_low = split(f_ref[c, k])
            both = product(parts, f_high, ((1,), (0,)))
            both = both[: 2 * cols] + both[2 * cols :] + product(high, f_low, ((1,), (0,)))
            sums.append(both)
        re = sums[0][:cols] + sums[1][cols:]
        im = sums[0][cols:] - sums[1][:cols]
        out_ref[:, 0, k] = re.reshape(shards, rows, cells)
        out_ref[:, 1, k] = im.reshape(shards, rows, cells)


def adjoint(columns, blocks, shards):
    _, held, cols, sensors = columns.shape
    cells = blocks.shape[3]
    return pl.pallas_call(
        adjoint_kernel,
        in_specs=[pl.BlockSpec(memory_space=pl.ANY)] * 2,
        out_specs=VMEM_SPEC,
        out_shape=jax.ShapeDtypeStruct((shards, 2, held, cols // shards, cells), jnp.float32),
        scratch_shapes=[
            pltpu.VMEM(columns.shape, jnp.float32),
            pltpu.VMEM(blocks.shape, jnp.float32),
            pltpu.SemaphoreType.DMA((held,)),
            pltpu.SemaphoreType.DMA((2 * held,)),
        ],
        compiler_params=grant(16),
        cost_estimate=pl.CostEstimate(
            flops=24 * held * cols * sensors * cells, bytes_accessed=8 * held * sensors * cells, transcendentals=0
        ),
        name="adjoint",
    )(columns, blocks)


def middle_kernel(x_ref, cut_ref, out_ref):
    shards, _, held, rows, cells = x_ref.shape
    freqs = shards * held
    steps = freqs - 1
    half = freqs // 2
    to_cos, to_sin = inverse_table(steps, freqs)
    from_cos, from_sin = forward_table(steps, freqs)
    base = lax.axis_index("freq") * rows
    row = lax.broadcasted_iota(jnp.int32, (rows, LANES), 0)
    cutoff = jnp.zeros((rows, LANES), jnp.int32)
    for r in range(rows):
        cutoff = jnp.where(row == r, cut_ref[base + r], cutoff)
    for lane in range(0, cells, LANES):
        at = pl.ds(lane, LANES)
        even, odd = [], []
        for k in range(half):
            a, b = divmod(k, held)
            c, d = divmod(freqs - 1 - k, held)
            re, im = x_ref[a, 0, b, :, at], x_ref[a, 1, b, :, at]
            re2, im2 = x_ref[c, 0, d, :, at], x_ref[c, 1, d, :, at]
            even += [re + re2, im - im2]
            odd += [re - re2, im + im2]
        series = []
        for t in range(steps):
            total = None
            for k in range(half):
                pair = odd if t % 2 else even
                for value, table in ((pair[2 * k], to_cos), (pair[2 * k + 1], to_sin)):
                    term = value * float(table[t, k])
                    total = term if total is None else total + term
            series.append(jnp.where(cutoff > t, total, 0.0))
        for k in range(half):
            a, b = divmod(k, held)
            c, d = divmod(freqs - 1 - k, held)
            sums = []
            for table in (from_cos, from_sin):
                for parity in (0, 1):
                    total = None
                    for t in range(parity, steps, 2):
                        term = series[t] * float(table[k, t])
                        total = term if total is None else total + term
                    sums.append(total)
            out_ref[a, 0, b, :, at] = sums[0] + sums[1]
            out_ref[c, 0, d, :, at] = sums[0] - sums[1]
            out_ref[a, 1, b, :, at] = sums[2] + sums[3]
            out_ref[c, 1, d, :, at] = sums[3] - sums[2]


def middle(gathered, causal_cutoffs):
    shards, _, held, rows, cells = gathered.shape
    freqs = shards * held
    steps = freqs - 1
    if freqs <= UNROLLED_FREQS and freqs % 2 == 0:
        return pl.pallas_call(
            middle_kernel,
            in_specs=[VMEM_SPEC, pl.BlockSpec(memory_space=pltpu.SMEM)],
            out_specs=VMEM_SPEC,
            out_shape=jax.ShapeDtypeStruct(gathered.shape, jnp.float32),
            compiler_params=grant(8),
            cost_estimate=pl.CostEstimate(
                flops=8 * freqs * steps * rows * cells, bytes_accessed=16 * freqs * rows * cells, transcendentals=0
            ),
            name="middle",
        )(gathered, causal_cutoffs)
    to_time = jnp.asarray(np.concatenate(inverse_table(steps, freqs), axis=1), jnp.float32)
    to_freq = jnp.asarray(np.concatenate(forward_table(steps, freqs), axis=0), jnp.float32)
    x = gathered.transpose(1, 0, 2, 3, 4).reshape(2 * freqs, rows * cells)
    series = jnp.dot(to_time, x, precision=lax.Precision.HIGHEST).reshape(steps, rows, cells)
    cutoff = lax.dynamic_slice_in_dim(causal_cutoffs, lax.axis_index("freq") * rows, rows)
    moment = lax.broadcasted_iota(jnp.int32, (steps, rows), 0)
    series = jnp.where((moment < cutoff[None, :])[:, :, None], series, 0.0)
    x = jnp.dot(to_freq, series.reshape(steps, rows * cells), precision=lax.Precision.HIGHEST)
    return x.reshape(2, shards, held, rows, cells).transpose(1, 0, 2, 3, 4)


def rates_of(band_ref, rates_ref):
    band = band_ref[...]
    rates = jnp.zeros(band.shape, jnp.float32)
    for b in range(BANDS):
        rates = jnp.where(band == b, rates_ref[b], rates)
    return rates


def edges_kernel(left_ref, right_ref, band_ref, rates_ref, inner_ref, outer_ref):
    held = left_ref.shape[1]
    cells = band_ref.shape[1]
    sensors = inner_ref.shape[2]
    rates = rates_of(band_ref, rates_ref)
    odd = lax.axis_index("cell") % 2 == 1
    for at in range(2 * held + 1):
        if at < 2 * held:
            c, k = divmod(at, held)
            first = left_ref[c, k].T[:ROWS]
            last = right_ref[c, k].T[LANES - ROWS :]
        else:
            inner_ref[at] = jnp.zeros((ROWS, sensors), jnp.float32)
            outer_ref[at] = jnp.zeros((ROWS, sensors), jnp.float32)
            first = jnp.broadcast_to(rates[:, :LANES], (LANES, LANES)).T[:ROWS]
            last = jnp.broadcast_to(rates[:, cells - LANES :], (LANES, LANES)).T[LANES - ROWS :]
        width = first.shape[1]
        inner_ref[at, :, :width] = jnp.where(odd, first, last)
        outer_ref[at, :, :width] = jnp.where(odd, last, first)


def edges(blocks, band_index, band_rates):
    _, held, sensors, cells = blocks.shape
    last = cells // LANES - 1
    shape = jax.ShapeDtypeStruct((2 * held + 1, ROWS, sensors), jnp.float32)
    return pl.pallas_call(
        edges_kernel,
        grid=(1,),
        in_specs=[
            pl.BlockSpec((2, held, sensors, LANES), lambda i: (0, 0, 0, 0)),
            pl.BlockSpec((2, held, sensors, LANES), lambda i: (0, 0, 0, last)),
            pl.BlockSpec((1, cells), lambda i: (0, 0)),
            pl.BlockSpec(memory_space=pltpu.SMEM),
        ],
        out_specs=[VMEM_SPEC] * 2,
        out_shape=[shape, shape],
        compiler_params=grant(12),
        cost_estimate=pl.CostEstimate(flops=10**8, bytes_accessed=16 * held * sensors * LANES, transcendentals=0),
        name="edges",
    )(blocks, blocks, band_index.reshape(1, cells), band_rates)


def smooth_kernel(f_ref, inner_ref, outer_ref, band_ref, rates_ref, high_ref, low_ref, a_both, a_side, sides):
    held = pl.num_programs(0)
    cells = f_ref.shape[3]
    sensors = f_ref.shape[2]
    width = cells + LANES
    k, c = pl.program_id(0), pl.program_id(1)
    odd = lax.axis_index("cell") % 2 == 1

    @pl.when((k == 0) & (c == 0))
    def _():
        lane = lax.broadcasted_iota(jnp.int32, (1, LANES), 1)
        side = jnp.zeros((1, LANES), jnp.float32)
        for i in range(ROWS):
            inner = inner_ref[2 * held, i : i + 1, :LANES]
            outer = outer_ref[2 * held, i : i + 1, :LANES]
            side = jnp.where(lane == i, jnp.where(odd, outer, inner), side)
            side = jnp.where(lane == LANES - ROWS + i, jnp.where(odd, inner, outer), side)
        rates = jnp.concatenate([rates_of(band_ref, rates_ref), side], axis=1)
        middle = ROWS
        diagonals = jnp.where(lax.broadcasted_iota(jnp.int32, (2 * ROWS, width), 0) == middle, 1.0, 0.0)
        for _ in range(SWEEPS):
            up = pltpu.roll(pltpu.roll(diagonals, 1, 1), 2 * ROWS - 1, 0)
            down = pltpu.roll(pltpu.roll(diagonals, width - 1, 1), 1, 0)
            diagonals = diagonals + rates * (up - 2.0 * diagonals + down)
        for lanes in range(0, width, LANES):
            column = lax.broadcasted_iota(jnp.int32, (LANES, LANES), 1)
            row = lax.broadcasted_iota(jnp.int32, (LANES, LANES), 0)
            for rows in range(0, cells, LANES):
                shift = rows - lanes
                offset = row - column + shift
                if lanes == cells:
                    offset = jnp.where(column < LANES // 2, offset, offset + width)
                tile = jnp.zeros((LANES, LANES), jnp.float32)
                for o in range(-SWEEPS, SWEEPS + 1):
                    entry = diagonals[middle + o : middle + o + 1, lanes : lanes + LANES]
                    tile = jnp.where(offset == o, entry, tile)
                high, low = split(tile)
                if lanes < cells:
                    a_both[rows : rows + LANES, lanes : lanes + LANES] = high
                    a_both[cells + rows : cells + rows + LANES, lanes : lanes + LANES] = low
                else:
                    a_side[rows : rows + LANES] = high
                    a_side[cells + rows : cells + rows + LANES] = low
        sides[...] = jnp.zeros_like(sides)

    high, low = split(f_ref[0, 0])
    both = product(a_both[...], high, ((1,), (1,)))
    total = both[:cells] + both[cells:] + product(a_both[:cells], low, ((1,), (1,)))
    at = c * held + k
    inner, outer = inner_ref[at], outer_ref[at]
    sides[:ROWS] = jnp.where(odd, outer, inner)
    sides[LANES - ROWS :] = jnp.where(odd, inner, outer)
    high, low = split(sides[...])
    both = product(a_side[...], high, ((1,), (0,)))
    total += both[:cells] + both[cells:] + product(a_side[:cells], low, ((1,), (0,)))
    high, low = split(total)
    high_ref[c, k] = high
    low_ref[c, k] = low


def smooth(blocks, inner, outer, band_index, band_rates):
    _, held, sensors, cells = blocks.shape
    shape = jax.ShapeDtypeStruct((2, held, cells, sensors), jnp.bfloat16)
    return pl.pallas_call(
        smooth_kernel,
        grid=(held, 2),
        in_specs=[
            pl.BlockSpec((1, 1, sensors, cells), lambda k, c: (c, k, 0, 0)),
            VMEM_SPEC,
            VMEM_SPEC,
            pl.BlockSpec((1, cells), lambda k, c: (0, 0)),
            pl.BlockSpec(memory_space=pltpu.SMEM),
        ],
        out_specs=[VMEM_SPEC] * 2,
        out_shape=[shape, shape],
        scratch_shapes=[
            pltpu.VMEM((2 * cells, cells), jnp.bfloat16),
            pltpu.VMEM((2 * cells, LANES), jnp.bfloat16),
            pltpu.VMEM((LANES, sensors), jnp.float32),
        ],
        compiler_params=grant(16),
        cost_estimate=pl.CostEstimate(
            flops=12 * held * sensors * cells * cells, bytes_accessed=16 * held * sensors * cells, transcendentals=0
        ),
        name="smooth",
    )(blocks, inner, outer, band_index.reshape(1, cells), band_rates)


def forward_kernel(x_ref, high_ref, low_ref, away_ref, home_ref):
    chips, _, held, share, sensors = home_ref.shape
    per = share // ROWS
    cell = lax.axis_index("cell")
    chip, core = cell // 2, cell % 2
    cells = x_ref.shape[4]
    order = []
    for side in (1 - core, core):
        for s in range(chips):
            order.append((2 * lax.rem(chip + s, chips) + side) * per)
    rows = 2 * chips * share
    for k in range(held):
        parts = []
        for c in range(2):
            for first in order:
                parts.append(x_ref[pl.ds(first, per), c, k].reshape(share, cells))
        high, low = split(jnp.concatenate(parts, axis=0))
        both = jnp.concatenate([high, low], axis=0)
        terms = []
        for c in range(2):
            wide = product(both, high_ref[c, k], ((1,), (0,)))
            terms.append(wide[: 2 * rows] + wide[2 * rows :] + product(high, low_ref[c, k], ((1,), (0,))))
        re = (terms[0][:rows] - terms[1][rows:]).reshape(2, chips, share, sensors)
        im = (terms[0][rows:] + terms[1][:rows]).reshape(2, chips, share, sensors)
        for side, ref in enumerate((away_ref, home_ref)):
            ref[:, 0, k] = re[side]
            ref[:, 1, k] = im[side]


def forward(returned, high, low, chips):
    shards, _, held, rows, cells = returned.shape
    sensors = high.shape[3]
    share = shards * rows // (2 * chips)
    shape = jax.ShapeDtypeStruct((chips, 2, held, share, sensors), jnp.float32)
    return pl.pallas_call(
        forward_kernel,
        in_specs=[VMEM_SPEC] * 3,
        out_specs=[VMEM_SPEC] * 2,
        out_shape=[shape, shape],
        compiler_params=grant(16),
        cost_estimate=pl.CostEstimate(
            flops=24 * held * shards * rows * sensors * cells,
            bytes_accessed=8 * held * sensors * cells,
            transcendentals=0,
        ),
        name="forward",
    )(returned, high, low)


def on_device(columns, freq_blocks, causal_cutoffs, band_index, band_rates):
    shards, strips = lax.axis_size("freq"), lax.axis_size("cell")
    chips = strips // 2
    spectrum = adjoint(columns, freq_blocks, shards)
    spectrum, blocks = lax.optimization_barrier((spectrum, freq_blocks))
    gathered = lax.all_to_all(spectrum, "freq", split_axis=0, concat_axis=0, tiled=True)
    inner, outer = edges(blocks, band_index, band_rates)
    inner = lax.ppermute(inner, "cell", [(i, i ^ 1) for i in range(strips)])
    pairs = [(i, i + 1) for i in range(1, strips - 1, 2)]
    outer = lax.ppermute(outer, "cell", pairs + [(j, i) for i, j in pairs])
    high, low = smooth(blocks, inner, outer, band_index, band_rates)
    spectrum = middle(gathered, causal_cutoffs)
    returned = lax.all_to_all(spectrum, "freq", split_axis=0, concat_axis=0, tiled=True)
    away, home = forward(returned, high, low, chips)
    total = home + lax.ppermute(away, "cell", [(i, i ^ 1) for i in range(strips)])
    result = total[0]
    for s in range(1, chips):
        pairs = [(i, 2 * ((i // 2 + s) % chips) + i % 2) for i in range(strips)]
        result = result + lax.ppermute(total[s], "cell", pairs)
    return result


def solution(mesh):
    placed = (P(None, "freq", None, None), P(None, "freq", None, "cell"), P(), P("cell"), P())
    return jax.shard_map(
        on_device,
        mesh=mesh,
        in_specs=placed,
        out_specs=P(None, "freq", "cell", None),
        check_vma=False,
    )
```

```python
import math

import jax
import jax.numpy as jnp
import numpy as np
from jax import lax
from jax.experimental import pallas as pl
from jax.experimental.pallas import tpu as pltpu
from jax.sharding import PartitionSpec as P

SWEEPS = 4
BANDS = 8
ROWS = 8
LANES = 128
UNROLLED_FREQS = 32


VMEM_SPEC = pl.BlockSpec(memory_space=pltpu.VMEM)
SMEM_SPEC = pl.BlockSpec(memory_space=pltpu.SMEM)
HBM_SPEC = pl.BlockSpec(memory_space=pltpu.HBM)


def grant(mib):
    return pltpu.CompilerParams(vmem_limit_bytes=mib * 2**20)


def split(x):
    high = x.astype(jnp.bfloat16)
    return high, (x - high.astype(jnp.float32)).astype(jnp.bfloat16)


def product(a, b, contract):
    return lax.dot_general(a, b, (contract, ((), ())), preferred_element_type=jnp.float32)


def inverse_table(steps, freqs):
    cycle = 2 * steps
    turns = np.outer(np.arange(steps), np.arange(freqs)) % cycle
    angle = turns * (2.0 * math.pi / cycle)
    weight = np.where((np.arange(freqs) == 0) | (np.arange(freqs) == freqs - 1), 1.0, 2.0) / cycle
    return weight * np.cos(angle), -weight * np.sin(angle)


def forward_table(steps, freqs):
    cycle = 2 * steps
    turns = np.outer(np.arange(freqs), np.arange(steps)) % cycle
    angle = turns * (2.0 * math.pi / cycle)
    return np.cos(angle), -np.sin(angle)


def adjoint_kernel(v_hbm, f_hbm, out_ref, v_ref, f_ref, v_sem, f_sem):
    shards, _, held, rows, cells = out_ref.shape
    cols = v_ref.shape[2]
    v_copies, f_copies = [], []
    for k in range(held):
        v_copies.append(pltpu.make_async_copy(v_hbm.at[:, k], v_ref.at[:, k], v_sem.at[k]))
        v_copies[k].start()
        for c in range(2):
            copy = pltpu.make_async_copy(f_hbm.at[c, k], f_ref.at[c, k], f_sem.at[2 * k + c])
            f_copies.append(copy)
            copy.start()
    for k in range(held):
        v_copies[k].wait()
        high, low = split(v_ref[:, k].reshape(2 * cols, v_ref.shape[3]))
        parts = jnp.concatenate([high, low], axis=0)
        sums = []
        for c in range(2):
            f_copies[2 * k + c].wait()
            f_high, f_low = split(f_ref[c, k])
            both = product(parts, f_high, ((1,), (0,)))
            both = both[: 2 * cols] + both[2 * cols :] + product(high, f_low, ((1,), (0,)))
            sums.append(both)
        re = sums[0][:cols] + sums[1][cols:]
        im = sums[0][cols:] - sums[1][:cols]
        out_ref[:, 0, k] = re.reshape(shards, rows, cells)
        out_ref[:, 1, k] = im.reshape(shards, rows, cells)


def adjoint(columns, blocks, shards):
    _, held, cols, sensors = columns.shape
    cells = blocks.shape[3]
    return pl.pallas_call(
        adjoint_kernel,
        in_specs=[HBM_SPEC] * 2,
        out_specs=VMEM_SPEC,
        out_shape=jax.ShapeDtypeStruct((shards, 2, held, cols // shards, cells), jnp.float32),
        scratch_shapes=[
            pltpu.VMEM(columns.shape, jnp.float32),
            pltpu.VMEM(blocks.shape, jnp.float32),
            pltpu.SemaphoreType.DMA((held,)),
            pltpu.SemaphoreType.DMA((2 * held,)),
        ],
        compiler_params=grant(16),
        cost_estimate=pl.CostEstimate(
            flops=24 * held * cols * sensors * cells, bytes_accessed=8 * held * sensors * cells, transcendentals=0
        ),
        name="adjoint",
    )(columns, blocks)


def middle_kernel(x_ref, cut_ref, out_ref):
    shards, _, held, rows, cells = x_ref.shape
    freqs = shards * held
    steps = freqs - 1
    half = freqs // 2
    to_cos, to_sin = inverse_table(steps, freqs)
    from_cos, from_sin = forward_table(steps, freqs)
    base = lax.axis_index("freq") * rows
    row = lax.broadcasted_iota(jnp.int32, (rows, LANES), 0)
    cutoff = jnp.zeros((rows, LANES), jnp.int32)
    for r in range(rows):
        cutoff = jnp.where(row == r, cut_ref[base + r], cutoff)
    for lane in range(0, cells, LANES):
        at = pl.ds(lane, LANES)
        even, odd = [], []
        for k in range(half):
            a, b = divmod(k, held)
            c, d = divmod(freqs - 1 - k, held)
            re, im = x_ref[a, 0, b, :, at], x_ref[a, 1, b, :, at]
            re2, im2 = x_ref[c, 0, d, :, at], x_ref[c, 1, d, :, at]
            even += [re + re2, im - im2]
            odd += [re - re2, im + im2]
        series = []
        for t in range(steps):
            total = None
            for k in range(half):
                pair = odd if t % 2 else even
                for value, table in ((pair[2 * k], to_cos), (pair[2 * k + 1], to_sin)):
                    term = value * float(table[t, k])
                    total = term if total is None else total + term
            series.append(jnp.where(cutoff > t, total, 0.0))
        for k in range(half):
            a, b = divmod(k, held)
            c, d = divmod(freqs - 1 - k, held)
            sums = []
            for table in (from_cos, from_sin):
                for parity in (0, 1):
                    total = None
                    for t in range(parity, steps, 2):
                        term = series[t] * float(table[k, t])
                        total = term if total is None else total + term
                    sums.append(total)
            out_ref[a, 0, b, :, at] = sums[0] + sums[1]
            out_ref[c, 0, d, :, at] = sums[0] - sums[1]
            out_ref[a, 1, b, :, at] = sums[2] + sums[3]
            out_ref[c, 1, d, :, at] = sums[3] - sums[2]


def middle(gathered, causal_cutoffs):
    shards, _, held, rows, cells = gathered.shape
    freqs = shards * held
    steps = freqs - 1
    if freqs <= UNROLLED_FREQS and freqs % 2 == 0:
        return pl.pallas_call(
            middle_kernel,
            in_specs=[VMEM_SPEC, SMEM_SPEC],
            out_specs=VMEM_SPEC,
            out_shape=jax.ShapeDtypeStruct(gathered.shape, jnp.float32),
            compiler_params=grant(8),
            cost_estimate=pl.CostEstimate(
                flops=8 * freqs * steps * rows * cells, bytes_accessed=16 * freqs * rows * cells, transcendentals=0
            ),
            name="middle",
        )(gathered, causal_cutoffs)
    to_time = jnp.asarray(np.concatenate(inverse_table(steps, freqs), axis=1), jnp.float32)
    to_freq = jnp.asarray(np.concatenate(forward_table(steps, freqs), axis=0), jnp.float32)
    x = gathered.transpose(1, 0, 2, 3, 4).reshape(2 * freqs, rows * cells)
    series = jnp.dot(to_time, x, precision=lax.Precision.HIGHEST).reshape(steps, rows, cells)
    cutoff = lax.dynamic_slice_in_dim(causal_cutoffs, lax.axis_index("freq") * rows, rows)
    moment = lax.broadcasted_iota(jnp.int32, (steps, rows), 0)
    series = jnp.where((moment < cutoff[None, :])[:, :, None], series, 0.0)
    x = jnp.dot(to_freq, series.reshape(steps, rows * cells), precision=lax.Precision.HIGHEST)
    return x.reshape(2, shards, held, rows, cells).transpose(1, 0, 2, 3, 4)


def rates_of(band_ref, rates_ref):
    band = band_ref[...]
    rates = jnp.zeros(band.shape, jnp.float32)
    for b in range(BANDS):
        rates = jnp.where(band == b, rates_ref[b], rates)
    return rates


def edges_kernel(f_hbm, band_ref, rates_ref, inner_ref, outer_ref, f_ref, f_sem):
    held = f_hbm.shape[1]
    cells = band_ref.shape[1]
    sensors = inner_ref.shape[2]
    copies = []
    for side, lanes in enumerate((0, cells - LANES)):
        copies.append(pltpu.make_async_copy(f_hbm.at[:, :, :, pl.ds(lanes, LANES)], f_ref.at[side], f_sem.at[side]))
        copies[side].start()
    rates = rates_of(band_ref, rates_ref)
    odd = lax.axis_index("cell") % 2 == 1
    for copy in copies:
        copy.wait()
    for at in range(2 * held + 1):
        if at < 2 * held:
            c, k = divmod(at, held)
            first = f_ref[0, c, k].T[:ROWS]
            last = f_ref[1, c, k].T[LANES - ROWS :]
        else:
            inner_ref[at] = jnp.zeros((ROWS, sensors), jnp.float32)
            outer_ref[at] = jnp.zeros((ROWS, sensors), jnp.float32)
            first = jnp.broadcast_to(rates[:, :LANES], (LANES, LANES)).T[:ROWS]
            last = jnp.broadcast_to(rates[:, cells - LANES :], (LANES, LANES)).T[LANES - ROWS :]
        width = first.shape[1]
        inner_ref[at, :, :width] = jnp.where(odd, first, last)
        outer_ref[at, :, :width] = jnp.where(odd, last, first)


def edges(blocks, band_index, band_rates):
    _, held, sensors, cells = blocks.shape
    shape = jax.ShapeDtypeStruct((2 * held + 1, ROWS, sensors), jnp.float32)
    return pl.pallas_call(
        edges_kernel,
        in_specs=[HBM_SPEC, VMEM_SPEC, SMEM_SPEC],
        out_specs=[VMEM_SPEC] * 2,
        out_shape=[shape, shape],
        scratch_shapes=[pltpu.VMEM((2, 2, held, sensors, LANES), jnp.float32), pltpu.SemaphoreType.DMA((2,))],
        compiler_params=grant(12),
        cost_estimate=pl.CostEstimate(flops=10**8, bytes_accessed=16 * held * sensors * LANES, transcendentals=0),
        name="edges",
    )(blocks, band_index.reshape(1, cells), band_rates)


def smooth_kernel(
    f_hbm, inner_ref, outer_ref, band_ref, rates_ref, high_ref, low_ref, f_ref, a_both, a_side, sides, f_sem
):
    _, held, sensors, cells = f_hbm.shape
    width = cells + LANES
    copies = []
    for at in range(2 * held):
        c, k = divmod(at, held)
        copies.append(pltpu.make_async_copy(f_hbm.at[c, k], f_ref.at[c, k], f_sem.at[at]))
        copies[at].start()
    odd = lax.axis_index("cell") % 2 == 1

    lane = lax.broadcasted_iota(jnp.int32, (1, LANES), 1)
    side = jnp.zeros((1, LANES), jnp.float32)
    for i in range(ROWS):
        inner = inner_ref[2 * held, i : i + 1, :LANES]
        outer = outer_ref[2 * held, i : i + 1, :LANES]
        side = jnp.where(lane == i, jnp.where(odd, outer, inner), side)
        side = jnp.where(lane == LANES - ROWS + i, jnp.where(odd, inner, outer), side)
    rates = jnp.concatenate([rates_of(band_ref, rates_ref), side], axis=1)
    middle = ROWS
    diagonals = jnp.where(lax.broadcasted_iota(jnp.int32, (2 * ROWS, width), 0) == middle, 1.0, 0.0)
    for _ in range(SWEEPS):
        up = pltpu.roll(pltpu.roll(diagonals, 1, 1), 2 * ROWS - 1, 0)
        down = pltpu.roll(pltpu.roll(diagonals, width - 1, 1), 1, 0)
        diagonals = diagonals + rates * (up - 2.0 * diagonals + down)
    for lanes in range(0, width, LANES):
        column = lax.broadcasted_iota(jnp.int32, (LANES, LANES), 1)
        row = lax.broadcasted_iota(jnp.int32, (LANES, LANES), 0)
        for rows in range(0, cells, LANES):
            shift = rows - lanes
            offset = row - column + shift
            if lanes == cells:
                offset = jnp.where(column < LANES // 2, offset, offset + width)
            tile = jnp.zeros((LANES, LANES), jnp.float32)
            for o in range(-SWEEPS, SWEEPS + 1):
                entry = diagonals[middle + o : middle + o + 1, lanes : lanes + LANES]
                tile = jnp.where(offset == o, entry, tile)
            high, low = split(tile)
            if lanes < cells:
                a_both[rows : rows + LANES, lanes : lanes + LANES] = high
                a_both[cells + rows : cells + rows + LANES, lanes : lanes + LANES] = low
            else:
                a_side[rows : rows + LANES] = high
                a_side[cells + rows : cells + rows + LANES] = low
    sides[...] = jnp.zeros_like(sides)

    for at in range(2 * held):
        c, k = divmod(at, held)
        inner, outer = inner_ref[at], outer_ref[at]
        sides[:ROWS] = jnp.where(odd, outer, inner)
        sides[LANES - ROWS :] = jnp.where(odd, inner, outer)
        high, low = split(sides[...])
        both = product(a_side[...], high, ((1,), (0,)))
        total = both[:cells] + both[cells:] + product(a_side[:cells], low, ((1,), (0,)))
        copies[at].wait()
        high, low = split(f_ref[c, k])
        both = product(a_both[...], high, ((1,), (1,)))
        total += both[:cells] + both[cells:] + product(a_both[:cells], low, ((1,), (1,)))
        high, low = split(total)
        high_ref[c, k] = high
        low_ref[c, k] = low


def smooth(blocks, inner, outer, band_index, band_rates):
    _, held, sensors, cells = blocks.shape
    shape = jax.ShapeDtypeStruct((2, held, cells, sensors), jnp.bfloat16)
    return pl.pallas_call(
        smooth_kernel,
        in_specs=[HBM_SPEC, VMEM_SPEC, VMEM_SPEC, VMEM_SPEC, SMEM_SPEC],
        out_specs=[VMEM_SPEC] * 2,
        out_shape=[shape, shape],
        scratch_shapes=[
            pltpu.VMEM(blocks.shape, jnp.float32),
            pltpu.VMEM((2 * cells, cells), jnp.bfloat16),
            pltpu.VMEM((2 * cells, LANES), jnp.bfloat16),
            pltpu.VMEM((LANES, sensors), jnp.float32),
            pltpu.SemaphoreType.DMA((2 * held,)),
        ],
        compiler_params=grant(16),
        cost_estimate=pl.CostEstimate(
            flops=12 * held * sensors * cells * cells, bytes_accessed=16 * held * sensors * cells, transcendentals=0
        ),
        name="smooth",
    )(blocks, inner, outer, band_index.reshape(1, cells), band_rates)


def forward_kernel(x_ref, high_ref, low_ref, away_ref, home_ref):
    chips, _, held, share, sensors = home_ref.shape
    per = share // ROWS
    cell = lax.axis_index("cell")
    chip, core = cell // 2, cell % 2
    cells = x_ref.shape[4]
    order = []
    for side in (1 - core, core):
        for s in range(chips):
            order.append((2 * lax.rem(chip + s, chips) + side) * per)
    rows = 2 * chips * share
    for k in range(held):
        parts = []
        for c in range(2):
            for first in order:
                parts.append(x_ref[pl.ds(first, per), c, k].reshape(share, cells))
        high, low = split(jnp.concatenate(parts, axis=0))
        both = jnp.concatenate([high, low], axis=0)
        terms = []
        for c in range(2):
            wide = product(both, high_ref[c, k], ((1,), (0,)))
            terms.append(wide[: 2 * rows] + wide[2 * rows :] + product(high, low_ref[c, k], ((1,), (0,))))
        re = (terms[0][:rows] - terms[1][rows:]).reshape(2, chips, share, sensors)
        im = (terms[0][rows:] + terms[1][:rows]).reshape(2, chips, share, sensors)
        for side, ref in enumerate((away_ref, home_ref)):
            ref[:, 0, k] = re[side]
            ref[:, 1, k] = im[side]


def forward(returned, high, low, chips):
    shards, _, held, rows, cells = returned.shape
    sensors = high.shape[3]
    share = shards * rows // (2 * chips)
    shape = jax.ShapeDtypeStruct((chips, 2, held, share, sensors), jnp.float32)
    return pl.pallas_call(
        forward_kernel,
        in_specs=[VMEM_SPEC] * 3,
        out_specs=[VMEM_SPEC] * 2,
        out_shape=[shape, shape],
        compiler_params=grant(16),
        cost_estimate=pl.CostEstimate(
            flops=24 * held * shards * rows * sensors * cells,
            bytes_accessed=8 * held * sensors * cells,
            transcendentals=0,
        ),
        name="forward",
    )(returned, high, low)


def on_device(columns, freq_blocks, causal_cutoffs, band_index, band_rates):
    shards, strips = lax.axis_size("freq"), lax.axis_size("cell")
    chips = strips // 2
    spectrum = adjoint(
        pltpu.with_memory_space_constraint(columns, pltpu.HBM),
        pltpu.with_memory_space_constraint(freq_blocks, pltpu.HBM),
        shards,
    )
    spectrum, blocks = lax.optimization_barrier((spectrum, freq_blocks))
    blocks = pltpu.with_memory_space_constraint(blocks, pltpu.HBM)
    gathered = lax.all_to_all(spectrum, "freq", split_axis=0, concat_axis=0, tiled=True)
    inner, outer = edges(blocks, band_index, band_rates)
    inner = lax.ppermute(inner, "cell", [(i, i ^ 1) for i in range(strips)])
    pairs = [(i, i + 1) for i in range(1, strips - 1, 2)]
    outer = lax.ppermute(outer, "cell", pairs + [(j, i) for i, j in pairs])
    gathered, inner, outer = lax.optimization_barrier((gathered, inner, outer))
    spectrum = middle(gathered, causal_cutoffs)
    high, low = smooth(blocks, inner, outer, band_index, band_rates)
    returned = lax.all_to_all(spectrum, "freq", split_axis=0, concat_axis=0, tiled=True)
    away, home = forward(returned, high, low, chips)
    total = home + lax.ppermute(away, "cell", [(i, i ^ 1) for i in range(strips)])
    result = total[0]
    for s in range(1, chips):
        pairs = [(i, 2 * ((i // 2 + s) % chips) + i % 2) for i in range(strips)]
        result = result + lax.ppermute(total[s], "cell", pairs)
    return result


def solution(mesh):
    placed = (P(None, "freq", None, None), P(None, "freq", None, "cell"), P(), P("cell"), P())
    return jax.shard_map(
        on_device,
        mesh=mesh,
        in_specs=placed,
        out_specs=P(None, "freq", "cell", None),
        check_vma=False,
    )
```

```python
import functools
import math

import jax
import jax.numpy as jnp
import numpy as np
from jax import lax
from jax.experimental import pallas as pl
from jax.experimental.pallas import tpu as pltpu
from jax.sharding import PartitionSpec as P

SWEEPS = 4
BANDS = 8
ROWS = 8
LANES = 128
UNROLLED_FREQS = 32


VMEM_SPEC = pl.BlockSpec(memory_space=pltpu.VMEM)
SMEM_SPEC = pl.BlockSpec(memory_space=pltpu.SMEM)
HBM_SPEC = pl.BlockSpec(memory_space=pltpu.HBM)


def grant(mib):
    return pltpu.CompilerParams(vmem_limit_bytes=mib * 2**20)


def in_hbm(x):
    return pltpu.with_memory_space_constraint(x, pltpu.HBM)


def split(x):
    high = x.astype(jnp.bfloat16)
    return high, (x - high.astype(jnp.float32)).astype(jnp.bfloat16)


def product(a, b, contract):
    return lax.dot_general(a, b, (contract, ((), ())), preferred_element_type=jnp.float32)


def inverse_table(steps, freqs):
    cycle = 2 * steps
    turns = np.outer(np.arange(steps), np.arange(freqs)) % cycle
    angle = turns * (2.0 * math.pi / cycle)
    weight = np.where((np.arange(freqs) == 0) | (np.arange(freqs) == freqs - 1), 1.0, 2.0) / cycle
    return weight * np.cos(angle), -weight * np.sin(angle)


def forward_table(steps, freqs):
    cycle = 2 * steps
    turns = np.outer(np.arange(freqs), np.arange(steps)) % cycle
    angle = turns * (2.0 * math.pi / cycle)
    return np.cos(angle), -np.sin(angle)


def rates_of(band_ref, rates_ref):
    band = band_ref[...]
    rates = jnp.zeros(band.shape, jnp.float32)
    for b in range(BANDS):
        rates = jnp.where(band == b, rates_ref[b], rates)
    return rates


def adjoint_kernel(
    v_hbm, f_hbm, band_hbm, rates_hbm, out_hbm, inner_ref, outer_ref,
    v_ref, f_ref, band_ref, rates_ref, out_ref, v_sem, f_sem, band_sem, rates_sem, out_sem,
):
    shards, _, held, rows, cells = out_hbm.shape
    cols, sensors = v_ref.shape[2:]
    v_copies, f_copies, out_copies = [], [], []
    for k in range(held):
        v_copies.append(pltpu.make_async_copy(v_hbm.at[:, k], v_ref.at[:, k], v_sem.at[k]))
        v_copies[k].start()
        for c in range(2):
            copy = pltpu.make_async_copy(f_hbm.at[c, k], f_ref.at[c, k], f_sem.at[2 * k + c])
            f_copies.append(copy)
            copy.start()
    band_copy = pltpu.make_async_copy(band_hbm, band_ref, band_sem)
    rates_copy = pltpu.make_async_copy(rates_hbm, rates_ref, rates_sem)
    band_copy.start()
    rates_copy.start()
    odd = lax.axis_index("cell") % 2 == 1
    inner_ref[...] = jnp.zeros_like(inner_ref)
    outer_ref[...] = jnp.zeros_like(outer_ref)

    def edge(at, first, last):
        first = first.T[:SWEEPS]
        last = last.T[LANES - SWEEPS :]
        place = slice(at * SWEEPS, (at + 1) * SWEEPS)
        inner_ref[place, : first.shape[1]] = jnp.where(odd, first, last)
        outer_ref[place, : first.shape[1]] = jnp.where(odd, last, first)

    for k in range(held):
        v_copies[k].wait()
        high, low = split(v_ref[:, k].reshape(2 * cols, sensors))
        parts = jnp.concatenate([high, low], axis=0)
        sums = []
        for c in range(2):
            f_copies[2 * k + c].wait()
            block = f_ref[c, k]
            f_high, f_low = split(block)
            both = product(parts, f_high, ((1,), (0,)))
            both = both[: 2 * cols] + both[2 * cols :] + product(high, f_low, ((1,), (0,)))
            sums.append(both)
            edge(c * held + k, block[:, :LANES], block[:, cells - LANES :])
        re = sums[0][:cols] + sums[1][cols:]
        im = sums[0][cols:] - sums[1][:cols]
        out_ref[:, 0, k] = re.reshape(shards, rows, cells)
        out_ref[:, 1, k] = im.reshape(shards, rows, cells)
        copy = pltpu.make_async_copy(out_ref.at[:, :, k], out_hbm.at[:, :, k], out_sem.at[k])
        out_copies.append(copy)
        copy.start()
    band_copy.wait()
    rates_copy.wait()
    rates = rates_of(band_ref, rates_ref)
    square = (LANES, LANES)
    edge(
        2 * held,
        jnp.broadcast_to(rates[:, :LANES], square),
        jnp.broadcast_to(rates[:, cells - LANES :], square),
    )
    for copy in out_copies:
        copy.wait()


def adjoint(columns, blocks, band_index, band_rates, shards):
    _, held, cols, sensors = columns.shape
    cells = blocks.shape[3]
    out = (shards, 2, held, cols // shards, cells)
    edge = jax.ShapeDtypeStruct((-(-(2 * held + 1) * SWEEPS // ROWS) * ROWS, sensors), jnp.float32)
    return pl.pallas_call(
        adjoint_kernel,
        in_specs=[HBM_SPEC] * 4,
        out_specs=[HBM_SPEC, VMEM_SPEC, VMEM_SPEC],
        out_shape=[pltpu.HBM(out, jnp.float32), edge, edge],
        scratch_shapes=[
            pltpu.VMEM(columns.shape, jnp.float32),
            pltpu.VMEM(blocks.shape, jnp.float32),
            pltpu.VMEM((1, cells), jnp.int32),
            pltpu.SMEM(band_rates.shape, jnp.float32),
            pltpu.VMEM(out, jnp.float32),
            pltpu.SemaphoreType.DMA((held,)),
            pltpu.SemaphoreType.DMA((2 * held,)),
            pltpu.SemaphoreType.DMA,
            pltpu.SemaphoreType.DMA,
            pltpu.SemaphoreType.DMA((held,)),
        ],
        compiler_params=grant(16),
        cost_estimate=pl.CostEstimate(
            flops=24 * held * cols * sensors * cells, bytes_accessed=8 * held * sensors * cells, transcendentals=0
        ),
        name="adjoint",
    )(columns, blocks, in_hbm(band_index.reshape(1, cells)), in_hbm(band_rates))


def middle_kernel(x_ref, cut_ref, out_hbm, out_ref, out_sem):
    shards, _, held, rows, cells = x_ref.shape
    freqs = shards * held
    steps = freqs - 1
    half = freqs // 2
    to_cos, to_sin = inverse_table(steps, freqs)
    from_cos, from_sin = forward_table(steps, freqs)
    base = lax.axis_index("freq") * rows
    row = lax.broadcasted_iota(jnp.int32, (rows, LANES), 0)
    cutoff = jnp.zeros((rows, LANES), jnp.int32)
    for r in range(rows):
        cutoff = jnp.where(row == r, cut_ref[base + r], cutoff)
    copies = []
    for lane in range(0, cells, LANES):
        at = pl.ds(lane, LANES)
        even, odd = [], []
        for k in range(half):
            a, b = divmod(k, held)
            c, d = divmod(freqs - 1 - k, held)
            re, im = x_ref[a, 0, b, :, at], x_ref[a, 1, b, :, at]
            re2, im2 = x_ref[c, 0, d, :, at], x_ref[c, 1, d, :, at]
            even += [re + re2, im - im2]
            odd += [re - re2, im + im2]
        series = []
        for t in range(steps):
            total = None
            for k in range(half):
                pair = odd if t % 2 else even
                for value, table in ((pair[2 * k], to_cos), (pair[2 * k + 1], to_sin)):
                    term = value * float(table[t, k])
                    total = term if total is None else total + term
            series.append(jnp.where(cutoff > t, total, 0.0))
        for k in range(half):
            a, b = divmod(k, held)
            c, d = divmod(freqs - 1 - k, held)
            sums = []
            for table in (from_cos, from_sin):
                for parity in (0, 1):
                    total = None
                    for t in range(parity, steps, 2):
                        term = series[t] * float(table[k, t])
                        total = term if total is None else total + term
                    sums.append(total)
            out_ref[a, 0, b, :, at] = sums[0] + sums[1]
            out_ref[c, 0, d, :, at] = sums[0] - sums[1]
            out_ref[a, 1, b, :, at] = sums[2] + sums[3]
            out_ref[c, 1, d, :, at] = sums[3] - sums[2]
        source, target = out_ref.at[:, :, :, :, at], out_hbm.at[:, :, :, :, at]
        copy = pltpu.make_async_copy(source, target, out_sem.at[lane // LANES])
        copies.append(copy)
        copy.start()
    for copy in copies:
        copy.wait()


def middle(gathered, causal_cutoffs):
    shards, _, held, rows, cells = gathered.shape
    freqs = shards * held
    steps = freqs - 1
    if freqs <= UNROLLED_FREQS and freqs % 2 == 0:
        return pl.pallas_call(
            middle_kernel,
            in_specs=[VMEM_SPEC, SMEM_SPEC],
            out_specs=HBM_SPEC,
            out_shape=pltpu.HBM(gathered.shape, jnp.float32),
            scratch_shapes=[
                pltpu.VMEM(gathered.shape, jnp.float32),
                pltpu.SemaphoreType.DMA((cells // LANES,)),
            ],
            compiler_params=grant(8),
            cost_estimate=pl.CostEstimate(
                flops=8 * freqs * steps * rows * cells, bytes_accessed=16 * freqs * rows * cells, transcendentals=0
            ),
            name="middle",
        )(gathered, causal_cutoffs)
    to_time = jnp.asarray(np.concatenate(inverse_table(steps, freqs), axis=1), jnp.float32)
    to_freq = jnp.asarray(np.concatenate(forward_table(steps, freqs), axis=0), jnp.float32)
    x = gathered.transpose(1, 0, 2, 3, 4).reshape(2 * freqs, rows * cells)
    series = jnp.dot(to_time, x, precision=lax.Precision.HIGHEST).reshape(steps, rows, cells)
    cutoff = lax.dynamic_slice_in_dim(causal_cutoffs, lax.axis_index("freq") * rows, rows)
    moment = lax.broadcasted_iota(jnp.int32, (steps, rows), 0)
    series = jnp.where((moment < cutoff[None, :])[:, :, None], series, 0.0)
    x = jnp.dot(to_freq, series.reshape(steps, rows * cells), precision=lax.Precision.HIGHEST)
    return x.reshape(2, shards, held, rows, cells).transpose(1, 0, 2, 3, 4)


def smooth_kernel(
    f_hbm, inner_ref, outer_ref, band_ref, rates_ref, high_ref, low_ref, f_ref, a_both, a_side, sides, f_sem
):
    _, held, sensors, cells = f_hbm.shape
    width = cells + LANES
    copies = []
    for at in range(2 * held):
        c, k = divmod(at, held)
        copies.append(pltpu.make_async_copy(f_hbm.at[c, k], f_ref.at[c, k], f_sem.at[at]))
        copies[at].start()
    odd = lax.axis_index("cell") % 2 == 1

    lane = lax.broadcasted_iota(jnp.int32, (1, LANES), 1)
    side = jnp.zeros((1, LANES), jnp.float32)
    for i in range(SWEEPS):
        place = slice(2 * held * SWEEPS + i, 2 * held * SWEEPS + i + 1)
        inner, outer = inner_ref[place, :LANES], outer_ref[place, :LANES]
        side = jnp.where(lane == i, jnp.where(odd, outer, inner), side)
        side = jnp.where(lane == LANES - SWEEPS + i, jnp.where(odd, inner, outer), side)
    rates = jnp.concatenate([rates_of(band_ref, rates_ref), side], axis=1)
    middle = ROWS
    diagonals = jnp.where(lax.broadcasted_iota(jnp.int32, (2 * ROWS, width), 0) == middle, 1.0, 0.0)
    for _ in range(SWEEPS):
        up = pltpu.roll(pltpu.roll(diagonals, 1, 1), 2 * ROWS - 1, 0)
        down = pltpu.roll(pltpu.roll(diagonals, width - 1, 1), 1, 0)
        diagonals = diagonals + rates * (up - 2.0 * diagonals + down)
    for lanes in range(0, width, LANES):
        column = lax.broadcasted_iota(jnp.int32, (LANES, LANES), 1)
        row = lax.broadcasted_iota(jnp.int32, (LANES, LANES), 0)
        for rows in range(0, cells, LANES):
            shift = rows - lanes
            offset = row - column + shift
            if lanes == cells:
                offset = jnp.where(column < LANES // 2, offset, offset + width)
            tile = jnp.zeros((LANES, LANES), jnp.float32)
            for o in range(-SWEEPS, SWEEPS + 1):
                entry = diagonals[middle + o : middle + o + 1, lanes : lanes + LANES]
                tile = jnp.where(offset == o, entry, tile)
            high, low = split(tile)
            if lanes < cells:
                a_both[rows : rows + LANES, lanes : lanes + LANES] = high
                a_both[cells + rows : cells + rows + LANES, lanes : lanes + LANES] = low
            else:
                a_side[rows : rows + LANES] = high
                a_side[cells + rows : cells + rows + LANES] = low
    sides[...] = jnp.zeros_like(sides)

    for at in range(2 * held):
        c, k = divmod(at, held)
        place = slice(at * SWEEPS, (at + 1) * SWEEPS)
        inner, outer = inner_ref[place], outer_ref[place]
        sides[:SWEEPS] = jnp.where(odd, outer, inner)
        sides[LANES - SWEEPS :] = jnp.where(odd, inner, outer)
        high, low = split(sides[...])
        both = product(a_side[...], high, ((1,), (0,)))
        total = both[:cells] + both[cells:] + product(a_side[:cells], low, ((1,), (0,)))
        copies[at].wait()
        high, low = split(f_ref[c, k])
        both = product(a_both[...], high, ((1,), (1,)))
        total += both[:cells] + both[cells:] + product(a_both[:cells], low, ((1,), (1,)))
        high, low = split(total)
        high_ref[c, k] = high
        low_ref[c, k] = low


def smooth(blocks, inner, outer, band_index, band_rates):
    _, held, sensors, cells = blocks.shape
    shape = jax.ShapeDtypeStruct((2, held, cells, sensors), jnp.bfloat16)
    return pl.pallas_call(
        smooth_kernel,
        in_specs=[HBM_SPEC, VMEM_SPEC, VMEM_SPEC, VMEM_SPEC, SMEM_SPEC],
        out_specs=[VMEM_SPEC] * 2,
        out_shape=[shape, shape],
        scratch_shapes=[
            pltpu.VMEM(blocks.shape, jnp.float32),
            pltpu.VMEM((2 * cells, cells), jnp.bfloat16),
            pltpu.VMEM((2 * cells, LANES), jnp.bfloat16),
            pltpu.VMEM((LANES, sensors), jnp.float32),
            pltpu.SemaphoreType.DMA((2 * held,)),
        ],
        compiler_params=grant(16),
        cost_estimate=pl.CostEstimate(
            flops=12 * held * sensors * cells * cells, bytes_accessed=16 * held * sensors * cells, transcendentals=0
        ),
        name="smooth",
    )(blocks, inner, outer, band_index.reshape(1, cells), band_rates)


def forward_kernel(away, x_ref, high_ref, low_ref, out_ref):
    chips, _, held, share, sensors = out_ref.shape
    per = share // ROWS
    cell = lax.axis_index("cell")
    chip, core = cell // 2, cell % 2
    cells = x_ref.shape[4]
    side = 1 - core if away else core
    order = [(2 * lax.rem(chip + s, chips) + side) * per for s in range(chips)]
    rows = chips * share
    for k in range(held):
        parts = []
        for c in range(2):
            for first in order:
                parts.append(x_ref[pl.ds(first, per), c, k].reshape(share, cells))
        high, low = split(jnp.concatenate(parts, axis=0))
        both = jnp.concatenate([high, low], axis=0)
        terms = []
        for c in range(2):
            wide = product(both, high_ref[c, k], ((1,), (0,)))
            terms.append(wide[: 2 * rows] + wide[2 * rows :] + product(high, low_ref[c, k], ((1,), (0,))))
        out_ref[:, 0, k] = (terms[0][:rows] - terms[1][rows:]).reshape(chips, share, sensors)
        out_ref[:, 1, k] = (terms[0][rows:] + terms[1][:rows]).reshape(chips, share, sensors)


def forward(returned, high, low, chips, away):
    shards, _, held, rows, cells = returned.shape
    sensors = high.shape[3]
    share = shards * rows // (2 * chips)
    shape = jax.ShapeDtypeStruct((chips, 2, held, share, sensors), jnp.float32)
    return pl.pallas_call(
        functools.partial(forward_kernel, away),
        in_specs=[VMEM_SPEC] * 3,
        out_specs=VMEM_SPEC,
        out_shape=shape,
        compiler_params=grant(16),
        cost_estimate=pl.CostEstimate(
            flops=12 * held * shards * rows * sensors * cells,
            bytes_accessed=8 * held * sensors * cells,
            transcendentals=0,
        ),
        name="away" if away else "home",
    )(returned, high, low)


def on_device(columns, freq_blocks, causal_cutoffs, band_index, band_rates):
    shards, strips = lax.axis_size("freq"), lax.axis_size("cell")
    chips = strips // 2
    columns, blocks = in_hbm(columns), in_hbm(freq_blocks)
    spectrum, inner, outer = adjoint(columns, blocks, band_index, band_rates, shards)
    gathered = lax.all_to_all(spectrum, "freq", split_axis=0, concat_axis=0, tiled=True)
    inner = lax.ppermute(inner, "cell", [(i, i ^ 1) for i in range(strips)])
    pairs = [(i, i + 1) for i in range(1, strips - 1, 2)]
    outer = lax.ppermute(outer, "cell", pairs + [(j, i) for i, j in pairs])
    gathered, inner, outer = lax.optimization_barrier((gathered, inner, outer))
    spectrum = middle(gathered, causal_cutoffs)
    high, low = smooth(blocks, inner, outer, band_index, band_rates)
    returned = lax.all_to_all(spectrum, "freq", split_axis=0, concat_axis=0, tiled=True)
    away = forward(returned, high, low, chips, True)
    away = lax.ppermute(away, "cell", [(i, i ^ 1) for i in range(strips)])
    home = forward(returned, high, low, chips, False)
    total = home + away
    result = total[0]
    for s in range(1, chips):
        pairs = [(i, 2 * ((i // 2 + s) % chips) + i % 2) for i in range(strips)]
        result = result + lax.ppermute(total[s], "cell", pairs)
    return result


def solution(mesh):
    placed = (P(None, "freq", None, None), P(None, "freq", None, "cell"), P(), P("cell"), P())
    return jax.shard_map(
        on_device,
        mesh=mesh,
        in_specs=placed,
        out_specs=P(None, "freq", "cell", None),
        check_vma=False,
    )
```

```python
import functools
import math

import jax
import jax.numpy as jnp
import numpy as np
from jax import lax
from jax.experimental import pallas as pl
from jax.experimental.pallas import tpu as pltpu
from jax.sharding import PartitionSpec as P

SWEEPS = 4
BANDS = 8
ROWS = 8
LANES = 128
UNROLLED_FREQS = 32


VMEM_SPEC = pl.BlockSpec(memory_space=pltpu.VMEM)
SMEM_SPEC = pl.BlockSpec(memory_space=pltpu.SMEM)
HBM_SPEC = pl.BlockSpec(memory_space=pltpu.HBM)


def grant(mib):
    return pltpu.CompilerParams(vmem_limit_bytes=mib * 2**20)


def in_hbm(x):
    return pltpu.with_memory_space_constraint(x, pltpu.HBM)


def split(x):
    high = x.astype(jnp.bfloat16)
    return high, (x - high.astype(jnp.float32)).astype(jnp.bfloat16)


def product(a, b, contract):
    return lax.dot_general(a, b, (contract, ((), ())), preferred_element_type=jnp.float32)


def inverse_table(steps, freqs):
    cycle = 2 * steps
    turns = np.outer(np.arange(steps), np.arange(freqs)) % cycle
    angle = turns * (2.0 * math.pi / cycle)
    weight = np.where((np.arange(freqs) == 0) | (np.arange(freqs) == freqs - 1), 1.0, 2.0) / cycle
    return weight * np.cos(angle), -weight * np.sin(angle)


def forward_table(steps, freqs):
    cycle = 2 * steps
    turns = np.outer(np.arange(freqs), np.arange(steps)) % cycle
    angle = turns * (2.0 * math.pi / cycle)
    return np.cos(angle), -np.sin(angle)


def rates_of(band_ref, rates_ref):
    band = band_ref[...]
    rates = jnp.zeros(band.shape, jnp.float32)
    for b in range(BANDS):
        rates = jnp.where(band == b, rates_ref[b], rates)
    return rates


def adjoint_kernel(
    v_hbm, f_hbm, band_hbm, rates_hbm, cut_hbm, out_hbm, inner_ref, outer_ref, cutoff_ref,
    v_ref, f_ref, band_ref, rates_ref, cut_ref, out_ref, v_sem, f_sem, out_sem, small_sem,
):
    shards, _, held, rows, cells = out_hbm.shape
    cols, sensors = v_ref.shape[2:]
    v_copies, f_copies, out_copies = [], [], []
    for k in range(held):
        v_copies.append(pltpu.make_async_copy(v_hbm.at[:, k], v_ref.at[:, k], v_sem.at[k]))
        v_copies[k].start()
        for c in range(2):
            copy = pltpu.make_async_copy(f_hbm.at[c, k], f_ref.at[c, k], f_sem.at[2 * k + c])
            f_copies.append(copy)
            copy.start()
    small = []
    for at, (source, target) in enumerate(((band_hbm, band_ref), (rates_hbm, rates_ref), (cut_hbm, cut_ref))):
        small.append(pltpu.make_async_copy(source, target, small_sem.at[at]))
        small[at].start()
    odd = lax.axis_index("cell") % 2 == 1
    inner_ref[...] = jnp.zeros_like(inner_ref)
    outer_ref[...] = jnp.zeros_like(outer_ref)

    def edge(at, first, last):
        first = first.T[:SWEEPS]
        last = last.T[LANES - SWEEPS :]
        place = slice(at * SWEEPS, (at + 1) * SWEEPS)
        inner_ref[place, : first.shape[1]] = jnp.where(odd, first, last)
        outer_ref[place, : first.shape[1]] = jnp.where(odd, last, first)

    for k in range(held):
        for copy in (v_copies[k], f_copies[2 * k], f_copies[2 * k + 1]):
            copy.wait()
        high, low = split(v_ref[:, k].reshape(2 * cols, sensors))
        parts = jnp.concatenate([high, low], axis=0)
        sums = []
        for c in range(2):
            f_high, f_low = split(f_ref[c, k])
            both = product(parts, f_high, ((1,), (0,)))
            both = both[: 2 * cols] + both[2 * cols :] + product(high, f_low, ((1,), (0,)))
            sums.append(both)
        re = sums[0][:cols] + sums[1][cols:]
        im = sums[0][cols:] - sums[1][:cols]
        out_ref[:, 0, k] = re.reshape(shards, rows, cells)
        out_ref[:, 1, k] = im.reshape(shards, rows, cells)
        copy = pltpu.make_async_copy(out_ref.at[:, :, k], out_hbm.at[:, :, k], out_sem.at[k])
        out_copies.append(copy)
        copy.start()
        for c in range(2):
            edge(c * held + k, f_ref[c, k, :, :LANES], f_ref[c, k, :, cells - LANES :])
    for copy in small:
        copy.wait()
    rates = rates_of(band_ref, rates_ref)
    square = (LANES, LANES)
    edge(
        2 * held,
        jnp.broadcast_to(rates[:, :LANES], square),
        jnp.broadcast_to(rates[:, cells - LANES :], square),
    )
    base = lax.axis_index("freq") * rows
    row = lax.broadcasted_iota(jnp.int32, (rows, LANES), 0)
    cutoff = jnp.zeros((rows, LANES), jnp.int32)
    for r in range(rows):
        cutoff = jnp.where(row == r, cut_ref[base + r], cutoff)
    cutoff_ref[...] = cutoff
    for copy in out_copies:
        copy.wait()


def adjoint(columns, blocks, band_index, band_rates, causal_cutoffs, shards):
    _, held, cols, sensors = columns.shape
    cells = blocks.shape[3]
    out = (shards, 2, held, cols // shards, cells)
    edge = jax.ShapeDtypeStruct((-(-(2 * held + 1) * SWEEPS // ROWS) * ROWS, sensors), jnp.float32)
    return pl.pallas_call(
        adjoint_kernel,
        in_specs=[HBM_SPEC] * 5,
        out_specs=[HBM_SPEC, VMEM_SPEC, VMEM_SPEC, VMEM_SPEC],
        out_shape=[
            pltpu.HBM(out, jnp.float32),
            edge,
            edge,
            jax.ShapeDtypeStruct((cols // shards, LANES), jnp.int32),
        ],
        scratch_shapes=[
            pltpu.VMEM(columns.shape, jnp.float32),
            pltpu.VMEM(blocks.shape, jnp.float32),
            pltpu.VMEM((1, cells), jnp.int32),
            pltpu.SMEM(band_rates.shape, jnp.float32),
            pltpu.SMEM(causal_cutoffs.shape, jnp.int32),
            pltpu.VMEM(out, jnp.float32),
            pltpu.SemaphoreType.DMA((held,)),
            pltpu.SemaphoreType.DMA((2 * held,)),
            pltpu.SemaphoreType.DMA((held,)),
            pltpu.SemaphoreType.DMA((3,)),
        ],
        compiler_params=grant(16),
        cost_estimate=pl.CostEstimate(
            flops=24 * held * cols * sensors * cells, bytes_accessed=8 * held * sensors * cells, transcendentals=0
        ),
        name="adjoint",
    )(columns, blocks, in_hbm(band_index.reshape(1, cells)), in_hbm(band_rates), in_hbm(causal_cutoffs))


def middle_kernel(x_ref, cutoff_ref, out_hbm, out_ref, out_sem):
    shards, _, held, rows, cells = x_ref.shape
    freqs = shards * held
    steps = freqs - 1
    half = freqs // 2
    to_cos, to_sin = inverse_table(steps, freqs)
    from_cos, from_sin = forward_table(steps, freqs)
    cutoff = cutoff_ref[...]
    copies = []
    for lane in range(0, cells, LANES):
        at = pl.ds(lane, LANES)
        even, odd = [], []
        for k in range(half):
            a, b = divmod(k, held)
            c, d = divmod(freqs - 1 - k, held)
            re, im = x_ref[a, 0, b, :, at], x_ref[a, 1, b, :, at]
            re2, im2 = x_ref[c, 0, d, :, at], x_ref[c, 1, d, :, at]
            even += [re + re2, im - im2]
            odd += [re - re2, im + im2]
        series = []
        for t in range(steps):
            total = None
            for k in range(half):
                pair = odd if t % 2 else even
                for value, table in ((pair[2 * k], to_cos), (pair[2 * k + 1], to_sin)):
                    term = value * float(table[t, k])
                    total = term if total is None else total + term
            series.append(jnp.where(cutoff > t, total, 0.0))
        for k in range(half):
            a, b = divmod(k, held)
            c, d = divmod(freqs - 1 - k, held)
            sums = []
            for table in (from_cos, from_sin):
                for parity in (0, 1):
                    total = None
                    for t in range(parity, steps, 2):
                        term = series[t] * float(table[k, t])
                        total = term if total is None else total + term
                    sums.append(total)
            out_ref[a, 0, b, :, at] = sums[0] + sums[1]
            out_ref[c, 0, d, :, at] = sums[0] - sums[1]
            out_ref[a, 1, b, :, at] = sums[2] + sums[3]
            out_ref[c, 1, d, :, at] = sums[3] - sums[2]
        source, target = out_ref.at[:, :, :, :, at], out_hbm.at[:, :, :, :, at]
        copy = pltpu.make_async_copy(source, target, out_sem.at[lane // LANES])
        copies.append(copy)
        copy.start()
    for copy in copies:
        copy.wait()


def middle(gathered, cutoff):
    shards, _, held, rows, cells = gathered.shape
    freqs = shards * held
    steps = freqs - 1
    if freqs <= UNROLLED_FREQS and freqs % 2 == 0:
        return pl.pallas_call(
            middle_kernel,
            in_specs=[VMEM_SPEC, VMEM_SPEC],
            out_specs=HBM_SPEC,
            out_shape=pltpu.HBM(gathered.shape, jnp.float32),
            scratch_shapes=[
                pltpu.VMEM(gathered.shape, jnp.float32),
                pltpu.SemaphoreType.DMA((cells // LANES,)),
            ],
            compiler_params=grant(8),
            cost_estimate=pl.CostEstimate(
                flops=8 * freqs * steps * rows * cells, bytes_accessed=16 * freqs * rows * cells, transcendentals=0
            ),
            name="middle",
        )(gathered, cutoff)
    to_time = jnp.asarray(np.concatenate(inverse_table(steps, freqs), axis=1), jnp.float32)
    to_freq = jnp.asarray(np.concatenate(forward_table(steps, freqs), axis=0), jnp.float32)
    x = gathered.transpose(1, 0, 2, 3, 4).reshape(2 * freqs, rows * cells)
    series = jnp.dot(to_time, x, precision=lax.Precision.HIGHEST).reshape(steps, rows, cells)
    moment = lax.broadcasted_iota(jnp.int32, (steps, rows), 0)
    series = jnp.where((moment < cutoff[None, :, 0])[:, :, None], series, 0.0)
    x = jnp.dot(to_freq, series.reshape(steps, rows * cells), precision=lax.Precision.HIGHEST)
    return x.reshape(2, shards, held, rows, cells).transpose(1, 0, 2, 3, 4)


def smooth_kernel(
    f_hbm, inner_ref, outer_ref, band_ref, rates_ref, high_ref, low_ref, f_ref, a_both, a_side, sides, f_sem
):
    _, held, sensors, cells = f_hbm.shape
    width = cells + LANES
    copies = []
    for at in range(2 * held):
        c, k = divmod(at, held)
        copies.append(pltpu.make_async_copy(f_hbm.at[c, k], f_ref.at[c, k], f_sem.at[at]))
        copies[at].start()
    odd = lax.axis_index("cell") % 2 == 1

    lane = lax.broadcasted_iota(jnp.int32, (1, LANES), 1)
    side = jnp.zeros((1, LANES), jnp.float32)
    for i in range(SWEEPS):
        place = slice(2 * held * SWEEPS + i, 2 * held * SWEEPS + i + 1)
        inner, outer = inner_ref[place, :LANES], outer_ref[place, :LANES]
        side = jnp.where(lane == i, jnp.where(odd, outer, inner), side)
        side = jnp.where(lane == LANES - SWEEPS + i, jnp.where(odd, inner, outer), side)
    rates = jnp.concatenate([rates_of(band_ref, rates_ref), side], axis=1)
    middle = ROWS
    diagonals = jnp.where(lax.broadcasted_iota(jnp.int32, (2 * ROWS, width), 0) == middle, 1.0, 0.0)
    for _ in range(SWEEPS):
        up = pltpu.roll(pltpu.roll(diagonals, 1, 1), 2 * ROWS - 1, 0)
        down = pltpu.roll(pltpu.roll(diagonals, width - 1, 1), 1, 0)
        diagonals = diagonals + rates * (up - 2.0 * diagonals + down)
    for lanes in range(0, width, LANES):
        column = lax.broadcasted_iota(jnp.int32, (LANES, LANES), 1)
        row = lax.broadcasted_iota(jnp.int32, (LANES, LANES), 0)
        for rows in range(0, cells, LANES):
            shift = rows - lanes
            offset = row - column + shift
            if lanes == cells:
                offset = jnp.where(column < LANES // 2, offset, offset + width)
            tile = jnp.zeros((LANES, LANES), jnp.float32)
            for o in range(-SWEEPS, SWEEPS + 1):
                entry = diagonals[middle + o : middle + o + 1, lanes : lanes + LANES]
                tile = jnp.where(offset == o, entry, tile)
            high, low = split(tile)
            if lanes < cells:
                a_both[rows : rows + LANES, lanes : lanes + LANES] = high
                a_both[cells + rows : cells + rows + LANES, lanes : lanes + LANES] = low
            else:
                a_side[rows : rows + LANES] = high
                a_side[cells + rows : cells + rows + LANES] = low
    sides[...] = jnp.zeros_like(sides)

    for at in range(2 * held):
        c, k = divmod(at, held)
        place = slice(at * SWEEPS, (at + 1) * SWEEPS)
        inner, outer = inner_ref[place], outer_ref[place]
        sides[:SWEEPS] = jnp.where(odd, outer, inner)
        sides[LANES - SWEEPS :] = jnp.where(odd, inner, outer)
        high, low = split(sides[...])
        both = product(a_side[...], high, ((1,), (0,)))
        total = both[:cells] + both[cells:] + product(a_side[:cells], low, ((1,), (0,)))
        copies[at].wait()
        high, low = split(f_ref[c, k])
        both = product(a_both[...], high, ((1,), (1,)))
        total += both[:cells] + both[cells:] + product(a_both[:cells], low, ((1,), (1,)))
        high, low = split(total)
        high_ref[c, k] = high
        low_ref[c, k] = low


def smooth(blocks, inner, outer, band_index, band_rates):
    _, held, sensors, cells = blocks.shape
    shape = jax.ShapeDtypeStruct((2, held, cells, sensors), jnp.bfloat16)
    return pl.pallas_call(
        smooth_kernel,
        in_specs=[HBM_SPEC, VMEM_SPEC, VMEM_SPEC, VMEM_SPEC, SMEM_SPEC],
        out_specs=[VMEM_SPEC] * 2,
        out_shape=[shape, shape],
        scratch_shapes=[
            pltpu.VMEM(blocks.shape, jnp.float32),
            pltpu.VMEM((2 * cells, cells), jnp.bfloat16),
            pltpu.VMEM((2 * cells, LANES), jnp.bfloat16),
            pltpu.VMEM((LANES, sensors), jnp.float32),
            pltpu.SemaphoreType.DMA((2 * held,)),
        ],
        compiler_params=grant(16),
        cost_estimate=pl.CostEstimate(
            flops=12 * held * sensors * cells * cells, bytes_accessed=16 * held * sensors * cells, transcendentals=0
        ),
        name="smooth",
    )(blocks, inner, outer, band_index.reshape(1, cells), band_rates)


def forward_kernel(steps, chips, x_ref, high_ref, low_ref, away_ref, home_ref):
    _, _, held, share, sensors = home_ref.shape
    per = share // ROWS
    cell = lax.axis_index("cell")
    chip, core = cell // 2, cell % 2
    cells = x_ref.shape[4]
    order = []
    for side in (1 - core, core):
        for s in steps:
            order.append((2 * lax.rem(chip + s, chips) + side) * per)
    rows = len(order) * share
    for k in range(held):
        parts = []
        for c in range(2):
            for first in order:
                parts.append(x_ref[pl.ds(first, per), c, k].reshape(share, cells))
        high, low = split(jnp.concatenate(parts, axis=0))
        both = jnp.concatenate([high, low], axis=0)
        terms = []
        for c in range(2):
            wide = product(both, high_ref[c, k], ((1,), (0,)))
            terms.append(wide[: 2 * rows] + wide[2 * rows :] + product(high, low_ref[c, k], ((1,), (0,))))
        re = (terms[0][:rows] - terms[1][rows:]).reshape(2, len(steps), share, sensors)
        im = (terms[0][rows:] + terms[1][:rows]).reshape(2, len(steps), share, sensors)
        for side, ref in enumerate((away_ref, home_ref)):
            ref[:, 0, k] = re[side]
            ref[:, 1, k] = im[side]


def forward(returned, high, low, steps, chips, name):
    shards, _, held, rows, cells = returned.shape
    sensors = high.shape[3]
    share = shards * rows // (2 * chips)
    shape = jax.ShapeDtypeStruct((len(steps), 2, held, share, sensors), jnp.float32)
    return pl.pallas_call(
        functools.partial(forward_kernel, steps, chips),
        in_specs=[VMEM_SPEC] * 3,
        out_specs=[VMEM_SPEC] * 2,
        out_shape=[shape, shape],
        compiler_params=grant(16),
        cost_estimate=pl.CostEstimate(
            flops=48 * len(steps) * held * share * sensors * cells,
            bytes_accessed=8 * held * sensors * cells,
            transcendentals=0,
        ),
        name=name,
    )(returned, high, low)


def on_device(columns, freq_blocks, causal_cutoffs, band_index, band_rates):
    shards, strips = lax.axis_size("freq"), lax.axis_size("cell")
    chips = strips // 2
    columns, blocks = in_hbm(columns), in_hbm(freq_blocks)
    spectrum, inner, outer, cutoff = adjoint(columns, blocks, band_index, band_rates, causal_cutoffs, shards)
    gathered = lax.all_to_all(spectrum, "freq", split_axis=0, concat_axis=0, tiled=True)
    inner = lax.ppermute(inner, "cell", [(i, i ^ 1) for i in range(strips)])
    pairs = [(i, i + 1) for i in range(1, strips - 1, 2)]
    outer = lax.ppermute(outer, "cell", pairs + [(j, i) for i, j in pairs])
    gathered, inner, outer = lax.optimization_barrier((gathered, inner, outer))
    spectrum = middle(gathered, cutoff)
    high, low = smooth(blocks, inner, outer, band_index, band_rates)
    returned = lax.all_to_all(spectrum, "freq", split_axis=0, concat_axis=0, tiled=True)
    swap = [(i, i ^ 1) for i in range(strips)]
    arrived = []
    if chips > 1:
        away, home = forward(returned, high, low, range(1, chips), chips, "leaving")
        leaving = home + lax.ppermute(away, "cell", swap)
        for s in range(1, chips):
            pairs = [(i, 2 * ((i // 2 + s) % chips) + i % 2) for i in range(strips)]
            arrived.append(lax.ppermute(leaving[s - 1], "cell", pairs))
    away, home = forward(returned, high, low, range(1), chips, "staying")
    result = home[0] + lax.ppermute(away, "cell", swap)[0]
    for term in arrived:
        result = result + term
    return result


def solution(mesh):
    placed = (P(None, "freq", None, None), P(None, "freq", None, "cell"), P(), P("cell"), P())
    return jax.shard_map(
        on_device,
        mesh=mesh,
        in_specs=placed,
        out_specs=P(None, "freq", "cell", None),
        check_vma=False,
    )
```

```python
import functools
import math

import jax
import jax.numpy as jnp
import numpy as np
from jax import lax
from jax.experimental import pallas as pl
from jax.experimental.pallas import tpu as pltpu
from jax.sharding import PartitionSpec as P


SWEEPS = 4
BANDS = 8
ROWS = 8
LANES = 128
UNROLLED_FREQS = 32
GROUPS = LANES // SWEEPS


VMEM_SPEC = pl.BlockSpec(memory_space=pltpu.VMEM)
SMEM_SPEC = pl.BlockSpec(memory_space=pltpu.SMEM)
HBM_SPEC = pl.BlockSpec(memory_space=pltpu.HBM)


def grant(mib):
    return pltpu.CompilerParams(vmem_limit_bytes=mib * 2**20)


def in_hbm(x):
    return pltpu.with_memory_space_constraint(x, pltpu.HBM)


def split(x):
    high = x.astype(jnp.bfloat16)
    return high, (x - high.astype(jnp.float32)).astype(jnp.bfloat16)


def product(a, b, contract):
    return lax.dot_general(a, b, (contract, ((), ())), preferred_element_type=jnp.float32)


def inverse_table(steps, freqs):
    cycle = 2 * steps
    turns = np.outer(np.arange(steps), np.arange(freqs)) % cycle
    angle = turns * (2.0 * math.pi / cycle)
    weight = np.where((np.arange(freqs) == 0) | (np.arange(freqs) == freqs - 1), 1.0, 2.0) / cycle
    return weight * np.cos(angle), -weight * np.sin(angle)


def forward_table(steps, freqs):
    cycle = 2 * steps
    turns = np.outer(np.arange(freqs), np.arange(steps)) % cycle
    angle = turns * (2.0 * math.pi / cycle)
    return np.cos(angle), -np.sin(angle)


def rates_of(band_ref, rates_ref):
    band = band_ref[...]
    rates = jnp.zeros(band.shape, jnp.float32)
    for b in range(BANDS):
        rates = jnp.where(band == b, rates_ref[b], rates)
    return rates


def adjoint_kernel(
    v_hbm, f_hbm, band_hbm, rates_hbm, cut_hbm, out_hbm, inner_ref, outer_ref, cutoff_ref,
    v_ref, f_ref, band_ref, rates_ref, cut_ref, out_ref, v_sem, f_sem, out_sem, small_sem,
):
    shards, _, held, rows, cells = out_hbm.shape
    cols, sensors = v_ref.shape[2:]
    v_copies, f_copies, out_copies = [], [], []
    for k in range(held):
        v_copies.append(pltpu.make_async_copy(v_hbm.at[:, k], v_ref.at[:, k], v_sem.at[k]))
        v_copies[k].start()
        for c in range(2):
            copy = pltpu.make_async_copy(f_hbm.at[c, k], f_ref.at[c, k], f_sem.at[2 * k + c])
            f_copies.append(copy)
            copy.start()
    small = []
    for at, (source, target) in enumerate(((band_hbm, band_ref), (rates_hbm, rates_ref), (cut_hbm, cut_ref))):
        small.append(pltpu.make_async_copy(source, target, small_sem.at[at]))
        small[at].start()
    odd = lax.axis_index("cell") % 2
    last = cells - LANES
    inner_at, inner_shift = pl.multiple_of((1 - odd) * last, LANES), (1 - odd) * SWEEPS
    outer_at, outer_shift = pl.multiple_of(odd * last, LANES), odd * SWEEPS
    lane_group = lax.broadcasted_iota(jnp.int32, (ROWS, LANES), 1) // SWEEPS

    def edge(at, block):
        for ref, lanes, shift in ((inner_ref, inner_at, inner_shift), (outer_ref, outer_at, outer_shift)):
            for first in range(0, sensors, ROWS * GROUPS):
                packed = jnp.zeros((ROWS, LANES), jnp.float32)
                for group in range(min(GROUPS, (sensors - first) // ROWS)):
                    rows_at = first + group * ROWS
                    cells_there = block[rows_at : rows_at + ROWS, pl.ds(lanes, LANES)]
                    moved = pltpu.roll(cells_there, group * SWEEPS + shift, 1)
                    packed = jnp.where(lane_group == group, moved, packed)
                ref[at, first // GROUPS : first // GROUPS + ROWS] = packed

    for k in range(held):
        for copy in (v_copies[k], f_copies[2 * k], f_copies[2 * k + 1]):
            copy.wait()
        high, low = split(v_ref[:, k].reshape(2 * cols, sensors))
        parts = jnp.concatenate([high, low], axis=0)
        sums = []
        for c in range(2):
            f_high, f_low = split(f_ref[c, k])
            both = product(parts, f_high, ((1,), (0,)))
            both = both[: 2 * cols] + both[2 * cols :] + product(high, f_low, ((1,), (0,)))
            sums.append(both)
        re = sums[0][:cols] + sums[1][cols:]
        im = sums[0][cols:] - sums[1][:cols]
        out_ref[:, 0, k] = re.reshape(shards, rows, cells)
        out_ref[:, 1, k] = im.reshape(shards, rows, cells)
        copy = pltpu.make_async_copy(out_ref.at[:, :, k], out_hbm.at[:, :, k], out_sem.at[k])
        out_copies.append(copy)
        copy.start()
        for c in range(2):
            edge(c * held + k, f_ref.at[c, k])
    for copy in small:
        copy.wait()
    rates = rates_of(band_ref, rates_ref)
    for ref, at in ((inner_ref, 1 - odd), (outer_ref, odd)):
        facing = jnp.where(at == 0, rates[:, :LANES], rates[:, last:])
        ref[2 * held] = jnp.broadcast_to(facing, ref.shape[1:])
    base = lax.axis_index("freq") * rows
    row = lax.broadcasted_iota(jnp.int32, (rows, LANES), 0)
    cutoff = jnp.zeros((rows, LANES), jnp.int32)
    for r in range(rows):
        cutoff = jnp.where(row == r, cut_ref[base + r], cutoff)
    cutoff_ref[...] = cutoff
    for copy in out_copies:
        copy.wait()


def adjoint(columns, blocks, band_index, band_rates, causal_cutoffs, shards):
    _, held, cols, sensors = columns.shape
    cells = blocks.shape[3]
    out = (shards, 2, held, cols // shards, cells)
    packed = -(-sensors // (ROWS * GROUPS)) * ROWS
    edge = jax.ShapeDtypeStruct((2 * held + 1, packed, LANES), jnp.float32)
    return pl.pallas_call(
        adjoint_kernel,
        in_specs=[HBM_SPEC] * 5,
        out_specs=[HBM_SPEC, VMEM_SPEC, VMEM_SPEC, VMEM_SPEC],
        out_shape=[
            pltpu.HBM(out, jnp.float32),
            edge,
            edge,
            jax.ShapeDtypeStruct((cols // shards, LANES), jnp.int32),
        ],
        scratch_shapes=[
            pltpu.VMEM(columns.shape, jnp.float32),
            pltpu.VMEM(blocks.shape, jnp.float32),
            pltpu.VMEM((1, cells), jnp.int32),
            pltpu.SMEM(band_rates.shape, jnp.float32),
            pltpu.SMEM(causal_cutoffs.shape, jnp.int32),
            pltpu.VMEM(out, jnp.float32),
            pltpu.SemaphoreType.DMA((held,)),
            pltpu.SemaphoreType.DMA((2 * held,)),
            pltpu.SemaphoreType.DMA((held,)),
            pltpu.SemaphoreType.DMA((3,)),
        ],
        compiler_params=grant(16),
        cost_estimate=pl.CostEstimate(
            flops=24 * held * cols * sensors * cells, bytes_accessed=8 * held * sensors * cells, transcendentals=0
        ),
        name="adjoint",
    )(columns, blocks, in_hbm(band_index.reshape(1, cells)), in_hbm(band_rates), in_hbm(causal_cutoffs))


def middle_kernel(x_ref, cutoff_ref, out_hbm, out_ref, out_sem):
    shards, _, held, _, cells = x_ref.shape
    freqs = shards * held
    steps = freqs - 1
    half = freqs // 2
    to_cos, to_sin = inverse_table(steps, freqs)
    from_cos, from_sin = forward_table(steps, freqs)
    cutoff = cutoff_ref[...]
    copies = []
    for lane in range(0, cells, LANES):
        at = pl.ds(lane, LANES)
        even, odd = [], []
        for k in range(half):
            a, b = divmod(k, held)
            c, d = divmod(freqs - 1 - k, held)
            re, im = x_ref[a, 0, b, :, at], x_ref[a, 1, b, :, at]
            re2, im2 = x_ref[c, 0, d, :, at], x_ref[c, 1, d, :, at]
            even += [re + re2, im - im2]
            odd += [re - re2, im + im2]
        series = []
        for t in range(steps):
            total = None
            for k in range(half):
                pair = odd if t % 2 else even
                for value, table in ((pair[2 * k], to_cos), (pair[2 * k + 1], to_sin)):
                    term = value * float(table[t, k])
                    total = term if total is None else total + term
            series.append(jnp.where(cutoff > t, total, 0.0))
        for k in range(half):
            a, b = divmod(k, held)
            c, d = divmod(freqs - 1 - k, held)
            sums = []
            for table in (from_cos, from_sin):
                for parity in (0, 1):
                    total = None
                    for t in range(parity, steps, 2):
                        term = series[t] * float(table[k, t])
                        total = term if total is None else total + term
                    sums.append(total)
            out_ref[a, 0, b, :, at] = sums[0] + sums[1]
            out_ref[c, 0, d, :, at] = sums[0] - sums[1]
            out_ref[a, 1, b, :, at] = sums[2] + sums[3]
            out_ref[c, 1, d, :, at] = sums[3] - sums[2]
        source, target = out_ref.at[:, :, :, :, at], out_hbm.at[:, :, :, :, at]
        copy = pltpu.make_async_copy(source, target, out_sem.at[lane // LANES])
        copies.append(copy)
        copy.start()
    for copy in copies:
        copy.wait()


def middle(gathered, cutoff):
    shards, _, held, rows, cells = gathered.shape
    freqs = shards * held
    steps = freqs - 1
    if freqs <= UNROLLED_FREQS and freqs % 2 == 0:
        return pl.pallas_call(
            middle_kernel,
            in_specs=[VMEM_SPEC, VMEM_SPEC],
            out_specs=HBM_SPEC,
            out_shape=pltpu.HBM(gathered.shape, jnp.float32),
            scratch_shapes=[
                pltpu.VMEM(gathered.shape, jnp.float32),
                pltpu.SemaphoreType.DMA((cells // LANES,)),
            ],
            compiler_params=grant(8),
            cost_estimate=pl.CostEstimate(
                flops=8 * freqs * steps * rows * cells, bytes_accessed=16 * freqs * rows * cells, transcendentals=0
            ),
            name="middle",
        )(gathered, cutoff)
    to_time = jnp.asarray(np.concatenate(inverse_table(steps, freqs), axis=1), jnp.float32)
    to_freq = jnp.asarray(np.concatenate(forward_table(steps, freqs), axis=0), jnp.float32)
    x = gathered.transpose(1, 0, 2, 3, 4).reshape(2 * freqs, rows * cells)
    series = jnp.dot(to_time, x, precision=lax.Precision.HIGHEST).reshape(steps, rows, cells)
    moment = lax.broadcasted_iota(jnp.int32, (steps, rows), 0)
    series = jnp.where((moment < cutoff[None, :, 0])[:, :, None], series, 0.0)
    x = jnp.dot(to_freq, series.reshape(steps, rows * cells), precision=lax.Precision.HIGHEST)
    return x.reshape(2, shards, held, rows, cells).transpose(1, 0, 2, 3, 4)


def smooth_kernel(
    f_hbm, inner_ref, outer_ref, band_ref, rates_ref, high_ref, low_ref, f_ref, a_both, a_side, sides, f_sem
):
    _, held, sensors, cells = f_hbm.shape
    width = cells + LANES
    copies = []
    for at in range(2 * held):
        c, k = divmod(at, held)
        copies.append(pltpu.make_async_copy(f_hbm.at[c, k], f_ref.at[c, k], f_sem.at[at]))
        copies[at].start()
    odd = lax.axis_index("cell") % 2
    lane = lax.broadcasted_iota(jnp.int32, (ROWS, LANES), 1)
    after_is_inner = odd == 0

    def beyond(at, group, rows):
        inner, outer = inner_ref[at, rows], outer_ref[at, rows]
        after = jnp.where(after_is_inner, inner, outer)
        before = jnp.where(after_is_inner, outer, inner)
        if group is not None:
            after = pltpu.roll(after, (LANES - group * SWEEPS) % LANES, 1)
            before = pltpu.roll(before, (LANES - (group + 1) * SWEEPS) % LANES, 1)
        cells_there = jnp.where(lane < SWEEPS, after, before)
        return jnp.where((lane < SWEEPS) | (lane >= LANES - SWEEPS), cells_there, 0.0)

    side = beyond(2 * held, None, slice(0, ROWS))[:1]
    rates = jnp.concatenate([rates_of(band_ref, rates_ref), side], axis=1)
    middle = ROWS
    diagonals = jnp.where(lax.broadcasted_iota(jnp.int32, (2 * ROWS, width), 0) == middle, 1.0, 0.0)
    for _ in range(SWEEPS):
        up = pltpu.roll(pltpu.roll(diagonals, 1, 1), 2 * ROWS - 1, 0)
        down = pltpu.roll(pltpu.roll(diagonals, width - 1, 1), 1, 0)
        diagonals = diagonals + rates * (up - 2.0 * diagonals + down)
    for lanes in range(0, width, LANES):
        column = lax.broadcasted_iota(jnp.int32, (LANES, LANES), 1)
        row = lax.broadcasted_iota(jnp.int32, (LANES, LANES), 0)
        for rows in range(0, cells, LANES):
            shift = rows - lanes
            offset = row - column + shift
            if lanes == cells:
                offset = jnp.where(column < LANES // 2, offset, offset + width)
            tile = jnp.zeros((LANES, LANES), jnp.float32)
            for o in range(-SWEEPS, SWEEPS + 1):
                entry = diagonals[middle + o : middle + o + 1, lanes : lanes + LANES]
                tile = jnp.where(offset == o, entry, tile)
            high, low = split(tile)
            if lanes < cells:
                a_both[rows : rows + LANES, lanes : lanes + LANES] = high
                a_both[cells + rows : cells + rows + LANES, lanes : lanes + LANES] = low
            else:
                a_side[rows : rows + LANES] = high
                a_side[cells + rows : cells + rows + LANES] = low
    for at in range(2 * held):
        c, k = divmod(at, held)
        for first in range(0, sensors, ROWS * GROUPS):
            for group in range(min(GROUPS, (sensors - first) // ROWS)):
                rows_at = first + group * ROWS
                packed = slice(first // GROUPS, first // GROUPS + ROWS)
                sides[rows_at : rows_at + ROWS] = beyond(at, group, packed)
        high, low = split(sides[...])
        both = product(a_side[...], high, ((1,), (1,)))
        total = both[:cells] + both[cells:] + product(a_side[:cells], low, ((1,), (1,)))
        copies[at].wait()
        high, low = split(f_ref[c, k])
        both = product(a_both[...], high, ((1,), (1,)))
        total += both[:cells] + both[cells:] + product(a_both[:cells], low, ((1,), (1,)))
        high, low = split(total)
        high_ref[c, k] = high
        low_ref[c, k] = low


def smooth(blocks, inner, outer, band_index, band_rates):
    _, held, sensors, cells = blocks.shape
    shape = jax.ShapeDtypeStruct((2, held, cells, sensors), jnp.bfloat16)
    return pl.pallas_call(
        smooth_kernel,
        in_specs=[HBM_SPEC, VMEM_SPEC, VMEM_SPEC, VMEM_SPEC, SMEM_SPEC],
        out_specs=[VMEM_SPEC] * 2,
        out_shape=[shape, shape],
        scratch_shapes=[
            pltpu.VMEM(blocks.shape, jnp.float32),
            pltpu.VMEM((2 * cells, cells), jnp.bfloat16),
            pltpu.VMEM((2 * cells, LANES), jnp.bfloat16),
            pltpu.VMEM((sensors, LANES), jnp.float32),
            pltpu.SemaphoreType.DMA((2 * held,)),
        ],
        compiler_params=grant(16),
        cost_estimate=pl.CostEstimate(
            flops=12 * held * sensors * cells * cells, bytes_accessed=16 * held * sensors * cells, transcendentals=0
        ),
        name="smooth",
    )(blocks, inner, outer, band_index.reshape(1, cells), band_rates)


def forward_kernel(steps, chips, x_ref, high_ref, low_ref, away_ref, home_ref):
    _, _, held, share, sensors = home_ref.shape
    per = share // ROWS
    cell = lax.axis_index("cell")
    chip, core = cell // 2, cell % 2
    cells = x_ref.shape[4]
    order = []
    for side in (1 - core, core):
        for s in steps:
            order.append((2 * lax.rem(chip + s, chips) + side) * per)
    rows = len(order) * share
    for k in range(held):
        parts = []
        for c in range(2):
            for first in order:
                parts.append(x_ref[pl.ds(first, per), c, k].reshape(share, cells))
        high, low = split(jnp.concatenate(parts, axis=0))
        both = jnp.concatenate([high, low], axis=0)
        terms = []
        for c in range(2):
            wide = product(both, high_ref[c, k], ((1,), (0,)))
            terms.append(wide[: 2 * rows] + wide[2 * rows :] + product(high, low_ref[c, k], ((1,), (0,))))
        re = (terms[0][:rows] - terms[1][rows:]).reshape(2, len(steps), share, sensors)
        im = (terms[0][rows:] + terms[1][:rows]).reshape(2, len(steps), share, sensors)
        for side, ref in enumerate((away_ref, home_ref)):
            ref[:, 0, k] = re[side]
            ref[:, 1, k] = im[side]


def forward(returned, high, low, steps, chips):
    shards, _, held, rows, cells = returned.shape
    sensors = high.shape[3]
    share = shards * rows // (2 * chips)
    shape = jax.ShapeDtypeStruct((len(steps), 2, held, share, sensors), jnp.float32)
    return pl.pallas_call(
        functools.partial(forward_kernel, steps, chips),
        in_specs=[VMEM_SPEC] * 3,
        out_specs=[VMEM_SPEC] * 2,
        out_shape=[shape, shape],
        compiler_params=grant(16),
        cost_estimate=pl.CostEstimate(
            flops=48 * len(steps) * held * share * sensors * cells,
            bytes_accessed=8 * held * sensors * cells,
            transcendentals=0,
        ),
    )(returned, high, low)


def on_device(columns, freq_blocks, causal_cutoffs, band_index, band_rates):
    shards, strips = lax.axis_size("freq"), lax.axis_size("cell")
    chips = strips // 2
    columns, blocks = in_hbm(columns), in_hbm(freq_blocks)
    spectrum, inner, outer, cutoff = adjoint(columns, blocks, band_index, band_rates, causal_cutoffs, shards)
    gathered = lax.all_to_all(spectrum, "freq", split_axis=0, concat_axis=0, tiled=True)
    inner = lax.ppermute(inner, "cell", [(i, i ^ 1) for i in range(strips)])
    pairs = [(i, i + 1) for i in range(1, strips - 1, 2)]
    outer = lax.ppermute(outer, "cell", pairs + [(j, i) for i, j in pairs])
    gathered, inner, outer = lax.optimization_barrier((gathered, inner, outer))
    spectrum = middle(gathered, cutoff)
    high, low = smooth(blocks, inner, outer, band_index, band_rates)
    returned = lax.all_to_all(spectrum, "freq", split_axis=0, concat_axis=0, tiled=True)
    swap = [(i, i ^ 1) for i in range(strips)]
    arrived = []
    if chips > 1:
        away, home = forward(returned, high, low, range(1, chips), chips)
        leaving = home + lax.ppermute(away, "cell", swap)
        for s in range(1, chips):
            pairs = [(i, 2 * ((i // 2 + s) % chips) + i % 2) for i in range(strips)]
            arrived.append(lax.ppermute(leaving[s - 1], "cell", pairs))
    away, home = forward(returned, high, low, range(1), chips)
    away = lax.ppermute(away, "cell", swap)
    result = home[0] + away[0]
    for term in arrived:
        result = result + term
    return result


def solution(mesh):
    placed = (P(None, "freq", None, None), P(None, "freq", None, "cell"), P(), P("cell"), P())
    return jax.shard_map(
        on_device,
        mesh=mesh,
        in_specs=placed,
        out_specs=P(None, "freq", "cell", None),
        check_vma=False,
    )
```

```python
import functools
import math

import jax
import jax.numpy as jnp
import numpy as np
from jax import lax
from jax.experimental import pallas as pl
from jax.experimental.pallas import tpu as pltpu
from jax.sharding import PartitionSpec as P


SWEEPS = 4
BANDS = 8
ROWS = 8
LANES = 128
UNROLLED_FREQS = 32
GROUPS = LANES // SWEEPS


VMEM_SPEC = pl.BlockSpec(memory_space=pltpu.VMEM)
SMEM_SPEC = pl.BlockSpec(memory_space=pltpu.SMEM)
HBM_SPEC = pl.BlockSpec(memory_space=pltpu.HBM)


def grant(mib):
    return pltpu.CompilerParams(vmem_limit_bytes=mib * 2**20)


def in_hbm(x):
    return pltpu.with_memory_space_constraint(x, pltpu.HBM)


def split(x):
    high = x.astype(jnp.bfloat16)
    return high, (x - high.astype(jnp.float32)).astype(jnp.bfloat16)


def product(a, b, contract):
    return lax.dot_general(a, b, (contract, ((), ())), preferred_element_type=jnp.float32)


def inverse_table(steps, freqs):
    cycle = 2 * steps
    turns = np.outer(np.arange(steps), np.arange(freqs)) % cycle
    angle = turns * (2.0 * math.pi / cycle)
    weight = np.where((np.arange(freqs) == 0) | (np.arange(freqs) == freqs - 1), 1.0, 2.0) / cycle
    return weight * np.cos(angle), -weight * np.sin(angle)


def forward_table(steps, freqs):
    cycle = 2 * steps
    turns = np.outer(np.arange(freqs), np.arange(steps)) % cycle
    angle = turns * (2.0 * math.pi / cycle)
    return np.cos(angle), -np.sin(angle)


def rates_of(band_ref, rates_ref):
    band = band_ref[...]
    rates = jnp.zeros(band.shape, jnp.float32)
    for b in range(BANDS):
        rates = jnp.where(band == b, rates_ref[b], rates)
    return rates


def adjoint_kernel(
    v_hbm, f_hbm, band_hbm, rates_hbm, cut_hbm, out_hbm, inner_ref, outer_ref, cutoff_ref,
    v_ref, f_ref, band_ref, rates_ref, cut_ref, out_ref, v_sem, f_sem, out_sem, small_sem,
):
    shards, _, held, rows, cells = out_hbm.shape
    cols, sensors = v_ref.shape[2:]
    v_copies, f_copies, out_copies = [], [], []
    for k in range(held):
        v_copies.append(pltpu.make_async_copy(v_hbm.at[:, k], v_ref.at[:, k], v_sem.at[k]))
        v_copies[k].start()
        for c in range(2):
            copy = pltpu.make_async_copy(f_hbm.at[c, k], f_ref.at[c, k], f_sem.at[2 * k + c])
            f_copies.append(copy)
            copy.start()
    small = []
    for at, (source, target) in enumerate(((band_hbm, band_ref), (rates_hbm, rates_ref), (cut_hbm, cut_ref))):
        small.append(pltpu.make_async_copy(source, target, small_sem.at[at]))
        small[at].start()
    odd = lax.axis_index("cell") % 2
    last = cells - LANES
    inner_at, inner_shift = pl.multiple_of((1 - odd) * last, LANES), (1 - odd) * SWEEPS
    outer_at, outer_shift = pl.multiple_of(odd * last, LANES), odd * SWEEPS
    lane_group = lax.broadcasted_iota(jnp.int32, (ROWS, LANES), 1) // SWEEPS

    def edge(at, block):
        for ref, lanes, shift in ((inner_ref, inner_at, inner_shift), (outer_ref, outer_at, outer_shift)):
            for first in range(0, sensors, ROWS * GROUPS):
                packed = jnp.zeros((ROWS, LANES), jnp.float32)
                for group in range(min(GROUPS, (sensors - first) // ROWS)):
                    rows_at = first + group * ROWS
                    cells_there = block[rows_at : rows_at + ROWS, pl.ds(lanes, LANES)]
                    moved = pltpu.roll(cells_there, group * SWEEPS + shift, 1)
                    packed = jnp.where(lane_group == group, moved, packed)
                ref[at, first // GROUPS : first // GROUPS + ROWS] = packed

    for k in range(held):
        for copy in (v_copies[k], f_copies[2 * k], f_copies[2 * k + 1]):
            copy.wait()
        high, low = split(v_ref[:, k].reshape(2 * cols, sensors))
        parts = jnp.concatenate([high, low], axis=0)
        sums = []
        for c in range(2):
            f_high, f_low = split(f_ref[c, k])
            both = product(parts, f_high, ((1,), (0,)))
            both = both[: 2 * cols] + both[2 * cols :] + product(high, f_low, ((1,), (0,)))
            sums.append(both)
        re = sums[0][:cols] + sums[1][cols:]
        im = sums[0][cols:] - sums[1][:cols]
        out_ref[:, 0, k] = re.reshape(shards, rows, cells)
        out_ref[:, 1, k] = im.reshape(shards, rows, cells)
        copy = pltpu.make_async_copy(out_ref.at[:, :, k], out_hbm.at[:, :, k], out_sem.at[k])
        out_copies.append(copy)
        copy.start()
        for c in range(2):
            edge(c * held + k, f_ref.at[c, k])
    for copy in small:
        copy.wait()
    rates = rates_of(band_ref, rates_ref)
    for ref, at in ((inner_ref, 1 - odd), (outer_ref, odd)):
        facing = jnp.where(at == 0, rates[:, :LANES], rates[:, last:])
        ref[2 * held] = jnp.broadcast_to(facing, ref.shape[1:])
    base = lax.axis_index("freq") * rows
    row = lax.broadcasted_iota(jnp.int32, (rows, LANES), 0)
    cutoff = jnp.zeros((rows, LANES), jnp.int32)
    for r in range(rows):
        cutoff = jnp.where(row == r, cut_ref[base + r], cutoff)
    cutoff_ref[...] = cutoff
    for copy in out_copies:
        copy.wait()


def adjoint(columns, blocks, band_index, band_rates, causal_cutoffs, shards):
    _, held, cols, sensors = columns.shape
    cells = blocks.shape[3]
    out = (shards, 2, held, cols // shards, cells)
    packed = -(-sensors // (ROWS * GROUPS)) * ROWS
    edge = jax.ShapeDtypeStruct((2 * held + 1, packed, LANES), jnp.float32)
    return pl.pallas_call(
        adjoint_kernel,
        in_specs=[HBM_SPEC] * 5,
        out_specs=[HBM_SPEC, VMEM_SPEC, VMEM_SPEC, VMEM_SPEC],
        out_shape=[
            pltpu.HBM(out, jnp.float32),
            edge,
            edge,
            jax.ShapeDtypeStruct((cols // shards, LANES), jnp.int32),
        ],
        scratch_shapes=[
            pltpu.VMEM(columns.shape, jnp.float32),
            pltpu.VMEM(blocks.shape, jnp.float32),
            pltpu.VMEM((1, cells), jnp.int32),
            pltpu.SMEM(band_rates.shape, jnp.float32),
            pltpu.SMEM(causal_cutoffs.shape, jnp.int32),
            pltpu.VMEM(out, jnp.float32),
            pltpu.SemaphoreType.DMA((held,)),
            pltpu.SemaphoreType.DMA((2 * held,)),
            pltpu.SemaphoreType.DMA((held,)),
            pltpu.SemaphoreType.DMA((3,)),
        ],
        compiler_params=grant(16),
        cost_estimate=pl.CostEstimate(
            flops=24 * held * cols * sensors * cells, bytes_accessed=8 * held * sensors * cells, transcendentals=0
        ),
        name="adjoint",
    )(columns, blocks, in_hbm(band_index.reshape(1, cells)), in_hbm(band_rates), in_hbm(causal_cutoffs))


def middle_kernel(x_ref, cutoff_ref, out_hbm, out_ref, out_sem):
    shards, _, held, _, cells = x_ref.shape
    freqs = shards * held
    steps = freqs - 1
    half = freqs // 2
    to_cos, to_sin = inverse_table(steps, freqs)
    from_cos, from_sin = forward_table(steps, freqs)
    cutoff = cutoff_ref[...]
    copies = []
    for lane in range(0, cells, LANES):
        at = pl.ds(lane, LANES)
        even, odd = [], []
        for k in range(half):
            a, b = divmod(k, held)
            c, d = divmod(freqs - 1 - k, held)
            re, im = x_ref[a, 0, b, :, at], x_ref[a, 1, b, :, at]
            re2, im2 = x_ref[c, 0, d, :, at], x_ref[c, 1, d, :, at]
            even += [re + re2, im - im2]
            odd += [re - re2, im + im2]
        series = []
        for t in range(steps):
            total = None
            for k in range(half):
                pair = odd if t % 2 else even
                for value, table in ((pair[2 * k], to_cos), (pair[2 * k + 1], to_sin)):
                    term = value * float(table[t, k])
                    total = term if total is None else total + term
            series.append(jnp.where(cutoff > t, total, 0.0))
        for k in range(half):
            a, b = divmod(k, held)
            c, d = divmod(freqs - 1 - k, held)
            sums = []
            for table in (from_cos, from_sin):
                for parity in (0, 1):
                    total = None
                    for t in range(parity, steps, 2):
                        term = series[t] * float(table[k, t])
                        total = term if total is None else total + term
                    sums.append(total)
            out_ref[a, 0, b, :, at] = sums[0] + sums[1]
            out_ref[c, 0, d, :, at] = sums[0] - sums[1]
            out_ref[a, 1, b, :, at] = sums[2] + sums[3]
            out_ref[c, 1, d, :, at] = sums[3] - sums[2]
        source, target = out_ref.at[:, :, :, :, at], out_hbm.at[:, :, :, :, at]
        copy = pltpu.make_async_copy(source, target, out_sem.at[lane // LANES])
        copies.append(copy)
        copy.start()
    for copy in copies:
        copy.wait()


def middle(gathered, cutoff):
    shards, _, held, rows, cells = gathered.shape
    freqs = shards * held
    steps = freqs - 1
    if freqs <= UNROLLED_FREQS and freqs % 2 == 0:
        return pl.pallas_call(
            middle_kernel,
            in_specs=[VMEM_SPEC, VMEM_SPEC],
            out_specs=HBM_SPEC,
            out_shape=pltpu.HBM(gathered.shape, jnp.float32),
            scratch_shapes=[
                pltpu.VMEM(gathered.shape, jnp.float32),
                pltpu.SemaphoreType.DMA((cells // LANES,)),
            ],
            compiler_params=grant(8),
            cost_estimate=pl.CostEstimate(
                flops=8 * freqs * steps * rows * cells, bytes_accessed=16 * freqs * rows * cells, transcendentals=0
            ),
            name="middle",
        )(gathered, cutoff)
    to_time = jnp.asarray(np.concatenate(inverse_table(steps, freqs), axis=1), jnp.float32)
    to_freq = jnp.asarray(np.concatenate(forward_table(steps, freqs), axis=0), jnp.float32)
    x = gathered.transpose(1, 0, 2, 3, 4).reshape(2 * freqs, rows * cells)
    series = jnp.dot(to_time, x, precision=lax.Precision.HIGHEST).reshape(steps, rows, cells)
    moment = lax.broadcasted_iota(jnp.int32, (steps, rows), 0)
    series = jnp.where((moment < cutoff[None, :, 0])[:, :, None], series, 0.0)
    x = jnp.dot(to_freq, series.reshape(steps, rows * cells), precision=lax.Precision.HIGHEST)
    return x.reshape(2, shards, held, rows, cells).transpose(1, 0, 2, 3, 4)


def smooth_kernel(
    f_hbm, inner_ref, outer_ref, band_ref, rates_ref, high_ref, low_ref, f_ref, a_both, a_side, sides, f_sem
):
    _, held, sensors, cells = f_hbm.shape
    width = cells + LANES
    copies = []
    for at in range(2 * held):
        c, k = divmod(at, held)
        copies.append(pltpu.make_async_copy(f_hbm.at[c, k], f_ref.at[c, k], f_sem.at[at]))
        copies[at].start()
    odd = lax.axis_index("cell") % 2
    lane = lax.broadcasted_iota(jnp.int32, (ROWS, LANES), 1)
    after_is_inner = odd == 0

    def beyond(at, group, rows):
        inner, outer = inner_ref[at, rows], outer_ref[at, rows]
        after = jnp.where(after_is_inner, inner, outer)
        before = jnp.where(after_is_inner, outer, inner)
        if group is not None:
            after = pltpu.roll(after, (LANES - group * SWEEPS) % LANES, 1)
            before = pltpu.roll(before, (LANES - (group + 1) * SWEEPS) % LANES, 1)
        cells_there = jnp.where(lane < SWEEPS, after, before)
        return jnp.where((lane < SWEEPS) | (lane >= LANES - SWEEPS), cells_there, 0.0)

    side = beyond(2 * held, None, slice(0, ROWS))[:1]
    rates = jnp.concatenate([rates_of(band_ref, rates_ref), side], axis=1)
    middle = ROWS
    diagonals = jnp.where(lax.broadcasted_iota(jnp.int32, (2 * ROWS, width), 0) == middle, 1.0, 0.0)
    for _ in range(SWEEPS):
        up = pltpu.roll(pltpu.roll(diagonals, 1, 1), 2 * ROWS - 1, 0)
        down = pltpu.roll(pltpu.roll(diagonals, width - 1, 1), 1, 0)
        diagonals = diagonals + rates * (up - 2.0 * diagonals + down)
    for lanes in range(0, width, LANES):
        column = lax.broadcasted_iota(jnp.int32, (LANES, LANES), 1)
        row = lax.broadcasted_iota(jnp.int32, (LANES, LANES), 0)
        for rows in range(0, cells, LANES):
            shift = rows - lanes
            offset = row - column + shift
            if lanes == cells:
                offset = jnp.where(column < LANES // 2, offset, offset + width)
            tile = jnp.zeros((LANES, LANES), jnp.float32)
            for o in range(-SWEEPS, SWEEPS + 1):
                entry = diagonals[middle + o : middle + o + 1, lanes : lanes + LANES]
                tile = jnp.where(offset == o, entry, tile)
            high, low = split(tile)
            if lanes < cells:
                a_both[rows : rows + LANES, lanes : lanes + LANES] = high
                a_both[cells + rows : cells + rows + LANES, lanes : lanes + LANES] = low
            else:
                a_side[rows : rows + LANES] = high
                a_side[cells + rows : cells + rows + LANES] = low
    for at in range(2 * held):
        c, k = divmod(at, held)
        for first in range(0, sensors, ROWS * GROUPS):
            for group in range(min(GROUPS, (sensors - first) // ROWS)):
                rows_at = first + group * ROWS
                packed = slice(first // GROUPS, first // GROUPS + ROWS)
                sides[rows_at : rows_at + ROWS] = beyond(at, group, packed)
        high, low = split(sides[...])
        both = product(a_side[...], high, ((1,), (1,)))
        total = both[:cells] + both[cells:] + product(a_side[:cells], low, ((1,), (1,)))
        copies[at].wait()
        high, low = split(f_ref[c, k])
        both = product(a_both[...], high, ((1,), (1,)))
        total += both[:cells] + both[cells:] + product(a_both[:cells], low, ((1,), (1,)))
        high, low = split(total)
        high_ref[c, k] = high
        low_ref[c, k] = low


def smooth(blocks, inner, outer, band_index, band_rates):
    _, held, sensors, cells = blocks.shape
    shape = jax.ShapeDtypeStruct((2, held, cells, sensors), jnp.bfloat16)
    return pl.pallas_call(
        smooth_kernel,
        in_specs=[HBM_SPEC, VMEM_SPEC, VMEM_SPEC, VMEM_SPEC, SMEM_SPEC],
        out_specs=[VMEM_SPEC] * 2,
        out_shape=[shape, shape],
        scratch_shapes=[
            pltpu.VMEM(blocks.shape, jnp.float32),
            pltpu.VMEM((2 * cells, cells), jnp.bfloat16),
            pltpu.VMEM((2 * cells, LANES), jnp.bfloat16),
            pltpu.VMEM((sensors, LANES), jnp.float32),
            pltpu.SemaphoreType.DMA((2 * held,)),
        ],
        compiler_params=grant(16),
        cost_estimate=pl.CostEstimate(
            flops=12 * held * sensors * cells * cells, bytes_accessed=16 * held * sensors * cells, transcendentals=0
        ),
        name="smooth",
    )(blocks, inner, outer, band_index.reshape(1, cells), band_rates)


def forward_kernel(steps, chips, wanted, x_ref, high_ref, low_ref, away_ref, home_ref):
    share, sensors = home_ref.shape[3:]
    per = share // ROWS
    cell = lax.axis_index("cell")
    chip, core = cell // 2, cell % 2
    cells = x_ref.shape[4]
    order = []
    for side in (1 - core, core):
        for s in steps:
            order.append((2 * lax.rem(chip + s, chips) + side) * per)
    rows = len(order) * share
    for at, k in enumerate(wanted):
        parts = []
        for c in range(2):
            for first in order:
                parts.append(x_ref[pl.ds(first, per), c, k].reshape(share, cells))
        high, low = split(jnp.concatenate(parts, axis=0))
        both = jnp.concatenate([high, low], axis=0)
        terms = []
        for c in range(2):
            wide = product(both, high_ref[c, k], ((1,), (0,)))
            terms.append(wide[: 2 * rows] + wide[2 * rows :] + product(high, low_ref[c, k], ((1,), (0,))))
        re = (terms[0][:rows] - terms[1][rows:]).reshape(2, len(steps), share, sensors)
        im = (terms[0][rows:] + terms[1][:rows]).reshape(2, len(steps), share, sensors)
        for side, ref in enumerate((away_ref, home_ref)):
            ref[:, 0, at] = re[side]
            ref[:, 1, at] = im[side]


def forward(returned, high, low, steps, chips, wanted):
    shards, _, _, rows, cells = returned.shape
    sensors = high.shape[3]
    share = shards * rows // (2 * chips)
    shape = jax.ShapeDtypeStruct((len(steps), 2, len(wanted), share, sensors), jnp.float32)
    return pl.pallas_call(
        functools.partial(forward_kernel, steps, chips, wanted),
        in_specs=[VMEM_SPEC] * 3,
        out_specs=[VMEM_SPEC] * 2,
        out_shape=[shape, shape],
        compiler_params=grant(16),
        cost_estimate=pl.CostEstimate(
            flops=48 * len(steps) * len(wanted) * share * sensors * cells,
            bytes_accessed=8 * len(wanted) * sensors * cells,
            transcendentals=0,
        ),
    )(returned, high, low)


def total_kernel(home_ref, away_ref, *refs):
    out_ref = refs[-1]
    held = out_ref.shape[1]
    for k in range(held):
        total = home_ref[0, :, k] + away_ref[0, :, k]
        for ref in refs[k:-1:held]:
            total += ref[:, 0]
        out_ref[:, k] = total


def on_device(columns, freq_blocks, causal_cutoffs, band_index, band_rates):
    shards, strips = lax.axis_size("freq"), lax.axis_size("cell")
    chips = strips // 2
    held = columns.shape[1]
    columns, blocks = in_hbm(columns), in_hbm(freq_blocks)
    spectrum, inner, outer, cutoff = adjoint(columns, blocks, band_index, band_rates, causal_cutoffs, shards)
    gathered = lax.all_to_all(spectrum, "freq", split_axis=0, concat_axis=0, tiled=True)
    inner = lax.ppermute(inner, "cell", [(i, i ^ 1) for i in range(strips)])
    pairs = [(i, i + 1) for i in range(1, strips - 1, 2)]
    outer = lax.ppermute(outer, "cell", pairs + [(j, i) for i, j in pairs])
    gathered, inner, outer = lax.optimization_barrier((gathered, inner, outer))
    spectrum = middle(gathered, cutoff)
    high, low = smooth(blocks, inner, outer, band_index, band_rates)
    returned = lax.all_to_all(spectrum, "freq", split_axis=0, concat_axis=0, tiled=True)
    swap = [(i, i ^ 1) for i in range(strips)]
    leaving = []
    if chips > 1:
        for k in range(held):
            away, home = forward(returned, high, low, range(1, chips), chips, (k,))
            leaving.append(home + lax.ppermute(away, "cell", swap))
    arrived = []
    for s in range(1, chips):
        pairs = [(i, 2 * ((i // 2 + s) % chips) + i % 2) for i in range(strips)]
        for k in range(held):
            arrived.append(lax.ppermute(leaving[k][s - 1], "cell", pairs))
    away, home = forward(returned, high, low, range(1), chips, range(held))
    away = lax.ppermute(away, "cell", swap)
    share, sensors = home.shape[3:]
    return pl.pallas_call(
        total_kernel,
        in_specs=[VMEM_SPEC] * (2 + len(arrived)),
        out_specs=VMEM_SPEC,
        out_shape=jax.ShapeDtypeStruct((2, held, share, sensors), jnp.float32),
        compiler_params=grant(16),
        name="total",
    )(home, away, *arrived)


def solution(mesh):
    placed = (P(None, "freq", None, None), P(None, "freq", None, "cell"), P(), P("cell"), P())
    return jax.shard_map(
        on_device,
        mesh=mesh,
        in_specs=placed,
        out_specs=P(None, "freq", "cell", None),
        check_vma=False,
    )
```

```python
import functools
import math

import jax
import jax.numpy as jnp
import numpy as np
from jax import lax
from jax.experimental import pallas as pl
from jax.experimental.pallas import tpu as pltpu
from jax.sharding import PartitionSpec as P


SWEEPS = 4
BANDS = 8
ROWS = 8
LANES = 128
UNROLLED_FREQS = 32
GROUPS = LANES // SWEEPS
NEAR = 2 * ROWS


VMEM_SPEC = pl.BlockSpec(memory_space=pltpu.VMEM)
SMEM_SPEC = pl.BlockSpec(memory_space=pltpu.SMEM)
HBM_SPEC = pl.BlockSpec(memory_space=pltpu.HBM)


def grant(mib):
    return pltpu.CompilerParams(vmem_limit_bytes=mib * 2**20)


def in_hbm(x):
    return pltpu.with_memory_space_constraint(x, pltpu.HBM)


def split(x):
    high = x.astype(jnp.bfloat16)
    return high, (x - high.astype(jnp.float32)).astype(jnp.bfloat16)


def product(a, b, contract):
    return lax.dot_general(a, b, (contract, ((), ())), preferred_element_type=jnp.float32)


def inverse_table(steps, freqs):
    cycle = 2 * steps
    turns = np.outer(np.arange(steps), np.arange(freqs)) % cycle
    angle = turns * (2.0 * math.pi / cycle)
    weight = np.where((np.arange(freqs) == 0) | (np.arange(freqs) == freqs - 1), 1.0, 2.0) / cycle
    return weight * np.cos(angle), -weight * np.sin(angle)


def forward_table(steps, freqs):
    cycle = 2 * steps
    turns = np.outer(np.arange(freqs), np.arange(steps)) % cycle
    angle = turns * (2.0 * math.pi / cycle)
    return np.cos(angle), -np.sin(angle)


def rates_of(band_ref, rates_ref):
    band = band_ref[...]
    rates = jnp.zeros(band.shape, jnp.float32)
    for b in range(BANDS):
        rates = jnp.where(band == b, rates_ref[b], rates)
    return rates


def adjoint_kernel(
    v_hbm, f_hbm, band_hbm, rates_hbm, cut_hbm, out_ref, inner_ref, outer_ref, cutoff_ref,
    v_ref, f_ref, band_ref, rates_ref, cut_ref, v_sem, f_sem, small_sem,
):
    shards, _, held, rows, cells = out_ref.shape
    cols, sensors = v_ref.shape[2:]
    v_copies, f_copies = [], []
    for k in range(held):
        v_copies.append(pltpu.make_async_copy(v_hbm.at[:, k], v_ref.at[:, k], v_sem.at[k]))
        v_copies[k].start()
        for c in range(2):
            copy = pltpu.make_async_copy(f_hbm.at[c, k], f_ref.at[c, k], f_sem.at[2 * k + c])
            f_copies.append(copy)
            copy.start()
    small = []
    for at, (source, target) in enumerate(((band_hbm, band_ref), (rates_hbm, rates_ref), (cut_hbm, cut_ref))):
        small.append(pltpu.make_async_copy(source, target, small_sem.at[at]))
        small[at].start()
    odd = lax.axis_index("cell") % 2
    last = cells - LANES
    inner_at, inner_shift = pl.multiple_of((1 - odd) * last, LANES), (1 - odd) * SWEEPS
    outer_at, outer_shift = pl.multiple_of(odd * last, LANES), odd * SWEEPS
    lane_group = lax.broadcasted_iota(jnp.int32, (ROWS, LANES), 1) // SWEEPS

    def edge(at, block):
        for ref, lanes, shift in ((inner_ref, inner_at, inner_shift), (outer_ref, outer_at, outer_shift)):
            for first in range(0, sensors, ROWS * GROUPS):
                packed = jnp.zeros((ROWS, LANES), jnp.float32)
                for group in range(min(GROUPS, (sensors - first) // ROWS)):
                    rows_at = first + group * ROWS
                    cells_there = block[rows_at : rows_at + ROWS, pl.ds(lanes, LANES)]
                    moved = pltpu.roll(cells_there, group * SWEEPS + shift, 1)
                    packed = jnp.where(lane_group == group, moved, packed)
                ref[at, first // GROUPS : first // GROUPS + ROWS] = packed

    for k in range(held):
        for copy in (v_copies[k], f_copies[2 * k], f_copies[2 * k + 1]):
            copy.wait()
        high, low = split(v_ref[:, k].reshape(2 * cols, sensors))
        parts = jnp.concatenate([high, low], axis=0)
        sums = []
        for c in range(2):
            f_high, f_low = split(f_ref[c, k])
            both = product(parts, f_high, ((1,), (0,)))
            both = both[: 2 * cols] + both[2 * cols :] + product(high, f_low, ((1,), (0,)))
            sums.append(both)
        re = sums[0][:cols] + sums[1][cols:]
        im = sums[0][cols:] - sums[1][:cols]
        out_ref[:, 0, k] = re.reshape(shards, rows, cells)
        out_ref[:, 1, k] = im.reshape(shards, rows, cells)
        for c in range(2):
            edge(c * held + k, f_ref.at[c, k])
    for copy in small:
        copy.wait()
    rates = rates_of(band_ref, rates_ref)
    for ref, at in ((inner_ref, 1 - odd), (outer_ref, odd)):
        facing = jnp.where(at == 0, rates[:, :LANES], rates[:, last:])
        ref[2 * held] = jnp.broadcast_to(facing, ref.shape[1:])
    base = lax.axis_index("freq") * rows
    row = lax.broadcasted_iota(jnp.int32, (rows, LANES), 0)
    cutoff = jnp.zeros((rows, LANES), jnp.int32)
    for r in range(rows):
        cutoff = jnp.where(row == r, cut_ref[base + r], cutoff)
    cutoff_ref[...] = cutoff


def adjoint(columns, blocks, band_index, band_rates, causal_cutoffs, shards):
    _, held, cols, sensors = columns.shape
    cells = blocks.shape[3]
    out = (shards, 2, held, cols // shards, cells)
    packed = -(-sensors // (ROWS * GROUPS)) * ROWS
    edge = jax.ShapeDtypeStruct((2 * held + 1, packed, LANES), jnp.float32)
    return pl.pallas_call(
        adjoint_kernel,
        in_specs=[HBM_SPEC] * 5,
        out_specs=[VMEM_SPEC] * 4,
        out_shape=[
            jax.ShapeDtypeStruct(out, jnp.float32),
            edge,
            edge,
            jax.ShapeDtypeStruct((cols // shards, LANES), jnp.int32),
        ],
        scratch_shapes=[
            pltpu.VMEM(columns.shape, jnp.float32),
            pltpu.VMEM(blocks.shape, jnp.float32),
            pltpu.VMEM((1, cells), jnp.int32),
            pltpu.SMEM(band_rates.shape, jnp.float32),
            pltpu.SMEM(causal_cutoffs.shape, jnp.int32),
            pltpu.SemaphoreType.DMA((held,)),
            pltpu.SemaphoreType.DMA((2 * held,)),
            pltpu.SemaphoreType.DMA((3,)),
        ],
        compiler_params=grant(16),
        cost_estimate=pl.CostEstimate(
            flops=24 * held * cols * sensors * cells, bytes_accessed=8 * held * sensors * cells, transcendentals=0
        ),
        name="adjoint",
    )(columns, blocks, in_hbm(band_index.reshape(1, cells)), in_hbm(band_rates), in_hbm(causal_cutoffs))


def middle_kernel(x_ref, cutoff_ref, out_hbm, out_ref, out_sem):
    shards, _, held, _, cells = x_ref.shape
    freqs = shards * held
    steps = freqs - 1
    half = freqs // 2
    to_cos, to_sin = inverse_table(steps, freqs)
    from_cos, from_sin = forward_table(steps, freqs)
    cutoff = cutoff_ref[...]
    copies = []
    for lane in range(0, cells, LANES):
        at = pl.ds(lane, LANES)
        even, odd = [], []
        for k in range(half):
            a, b = divmod(k, held)
            c, d = divmod(freqs - 1 - k, held)
            re, im = x_ref[a, 0, b, :, at], x_ref[a, 1, b, :, at]
            re2, im2 = x_ref[c, 0, d, :, at], x_ref[c, 1, d, :, at]
            even += [re + re2, im - im2]
            odd += [re - re2, im + im2]
        series = []
        for t in range(steps):
            total = None
            for k in range(half):
                pair = odd if t % 2 else even
                for value, table in ((pair[2 * k], to_cos), (pair[2 * k + 1], to_sin)):
                    term = value * float(table[t, k])
                    total = term if total is None else total + term
            series.append(jnp.where(cutoff > t, total, 0.0))
        for k in range(half):
            a, b = divmod(k, held)
            c, d = divmod(freqs - 1 - k, held)
            sums = []
            for table in (from_cos, from_sin):
                for parity in (0, 1):
                    total = None
                    for t in range(parity, steps, 2):
                        term = series[t] * float(table[k, t])
                        total = term if total is None else total + term
                    sums.append(total)
            out_ref[a, 0, b, :, at] = sums[0] + sums[1]
            out_ref[c, 0, d, :, at] = sums[0] - sums[1]
            out_ref[a, 1, b, :, at] = sums[2] + sums[3]
            out_ref[c, 1, d, :, at] = sums[3] - sums[2]
        source, target = out_ref.at[:, :, :, :, at], out_hbm.at[:, :, :, :, at]
        copy = pltpu.make_async_copy(source, target, out_sem.at[lane // LANES])
        copies.append(copy)
        copy.start()
    for copy in copies:
        copy.wait()


def middle(gathered, cutoff):
    shards, _, held, rows, cells = gathered.shape
    freqs = shards * held
    steps = freqs - 1
    if freqs <= UNROLLED_FREQS and freqs % 2 == 0:
        return pl.pallas_call(
            middle_kernel,
            in_specs=[VMEM_SPEC, VMEM_SPEC],
            out_specs=HBM_SPEC,
            out_shape=pltpu.HBM(gathered.shape, jnp.float32),
            scratch_shapes=[
                pltpu.VMEM(gathered.shape, jnp.float32),
                pltpu.SemaphoreType.DMA((cells // LANES,)),
            ],
            compiler_params=grant(8),
            cost_estimate=pl.CostEstimate(
                flops=8 * freqs * steps * rows * cells, bytes_accessed=16 * freqs * rows * cells, transcendentals=0
            ),
            name="middle",
        )(gathered, cutoff)
    to_time = jnp.asarray(np.concatenate(inverse_table(steps, freqs), axis=1), jnp.float32)
    to_freq = jnp.asarray(np.concatenate(forward_table(steps, freqs), axis=0), jnp.float32)
    x = gathered.transpose(1, 0, 2, 3, 4).reshape(2 * freqs, rows * cells)
    series = jnp.dot(to_time, x, precision=lax.Precision.HIGHEST).reshape(steps, rows, cells)
    moment = lax.broadcasted_iota(jnp.int32, (steps, rows), 0)
    series = jnp.where((moment < cutoff[None, :, 0])[:, :, None], series, 0.0)
    x = jnp.dot(to_freq, series.reshape(steps, rows * cells), precision=lax.Precision.HIGHEST)
    return x.reshape(2, shards, held, rows, cells).transpose(1, 0, 2, 3, 4)


def diagonals_of(rates):
    width = rates.shape[1]
    diagonals = jnp.where(lax.broadcasted_iota(jnp.int32, (2 * ROWS, width), 0) == ROWS, 1.0, 0.0)
    for _ in range(SWEEPS):
        up = pltpu.roll(pltpu.roll(diagonals, 1, 1), 2 * ROWS - 1, 0)
        down = pltpu.roll(pltpu.roll(diagonals, width - 1, 1), 1, 0)
        diagonals = diagonals + rates * (up - 2.0 * diagonals + down)
    return diagonals


def spread(diagonals, offset):
    tile = jnp.zeros(offset.shape, jnp.float32)
    for o in range(-SWEEPS, SWEEPS + 1):
        tile = jnp.where(offset == o, diagonals[ROWS + o : ROWS + o + 1], tile)
    return tile


def smooth_kernel(f_hbm, band_ref, rates_ref, high_ref, low_ref, near_ref, f_ref, a_both, f_sem):
    _, held, _, cells = f_hbm.shape
    copies = []
    for at in range(2 * held):
        c, k = divmod(at, held)
        copies.append(pltpu.make_async_copy(f_hbm.at[c, k], f_ref.at[c, k], f_sem.at[at]))
        copies[at].start()
    diagonals = diagonals_of(jnp.concatenate([rates_of(band_ref, rates_ref), jnp.zeros((1, LANES), jnp.float32)], axis=1))
    for lanes in range(0, cells, LANES):
        column = lax.broadcasted_iota(jnp.int32, (LANES, LANES), 1)
        row = lax.broadcasted_iota(jnp.int32, (LANES, LANES), 0)
        for rows in range(0, cells, LANES):
            high, low = split(spread(diagonals[:, lanes : lanes + LANES], row - column + (rows - lanes)))
            a_both[rows : rows + LANES, lanes : lanes + LANES] = high
            a_both[cells + rows : cells + rows + LANES, lanes : lanes + LANES] = low
    for at in range(2 * held):
        c, k = divmod(at, held)
        copies[at].wait()
        high, low = split(f_ref[c, k])
        both = product(a_both[...], high, ((1,), (1,)))
        total = both[:cells] + both[cells:] + product(a_both[:cells], low, ((1,), (1,)))
        high, low = split(total)
        high_ref[c, k] = high
        low_ref[c, k] = low
        near_ref[c, k, :NEAR] = total[:NEAR]
        near_ref[c, k, NEAR:] = total[cells - NEAR :]


def smooth(blocks, band_index, band_rates):
    _, held, sensors, cells = blocks.shape
    shape = jax.ShapeDtypeStruct((2, held, cells, sensors), jnp.bfloat16)
    return pl.pallas_call(
        smooth_kernel,
        in_specs=[HBM_SPEC, VMEM_SPEC, SMEM_SPEC],
        out_specs=[VMEM_SPEC] * 3,
        out_shape=[shape, shape, jax.ShapeDtypeStruct((2, held, 2 * NEAR, sensors), jnp.float32)],
        scratch_shapes=[
            pltpu.VMEM(blocks.shape, jnp.float32),
            pltpu.VMEM((2 * cells, cells), jnp.bfloat16),
            pltpu.SemaphoreType.DMA((2 * held,)),
        ],
        compiler_params=grant(16),
        cost_estimate=pl.CostEstimate(
            flops=12 * held * sensors * cells * cells, bytes_accessed=16 * held * sensors * cells, transcendentals=0
        ),
        name="smooth",
    )(blocks, band_index.reshape(1, cells), band_rates)


def near_kernel(
    near_ref, own_inner_ref, own_outer_ref, inner_ref, outer_ref, band_ref, rates_ref, high_ref, low_ref, sides
):
    held = near_ref.shape[1]
    sensors = near_ref.shape[3]
    cells = band_ref.shape[1]
    even = lax.axis_index("cell") % 2 == 0
    lane = lax.broadcasted_iota(jnp.int32, (ROWS, LANES), 1)
    middle = LANES // 2
    spots = (0, middle - SWEEPS, middle, LANES - SWEEPS)

    def parts(at, rows):
        own_inner, own_outer = own_inner_ref[at, rows], own_outer_ref[at, rows]
        inner, outer = inner_ref[at, rows], outer_ref[at, rows]
        return (
            jnp.where(even, own_outer, own_inner),
            jnp.where(even, own_inner, own_outer),
            jnp.where(even, inner, outer),
            jnp.where(even, outer, inner),
        )

    _, _, after, before = parts(2 * held, slice(0, ROWS))
    side = jnp.where(lane < SWEEPS, after, jnp.where(lane >= LANES - SWEEPS, before, 0.0))[:1]
    own = rates_of(band_ref, rates_ref)
    alone = diagonals_of(jnp.concatenate([own, jnp.zeros((1, LANES), jnp.float32)], axis=1))
    full = diagonals_of(jnp.concatenate([own, side], axis=1))
    first = full[:, :LANES] - alone[:, :LANES]
    last = full[:, cells - LANES : cells] - alone[:, cells - LANES : cells]
    beyond = full[:, cells:]
    at_lane = lax.broadcasted_iota(jnp.int32, (2 * ROWS, LANES), 1)
    change = jnp.where(at_lane < middle // 2, first, beyond)
    change = jnp.where((at_lane >= middle // 2) & (at_lane < middle), pltpu.roll(last, middle, 1), change)
    change = jnp.where((at_lane >= middle) & (at_lane < middle + SWEEPS), pltpu.roll(beyond, middle, 1), change)
    column = lax.broadcasted_iota(jnp.int32, (NEAR, LANES), 1)
    row = lax.broadcasted_iota(jnp.int32, (NEAR, LANES), 0)
    at_first = row - jnp.where(column < middle, column, column - LANES)
    at_last = (row - NEAR) - (column - middle)
    matrix = jnp.concatenate([spread(change, at_first), spread(change, at_last)], axis=0)
    a_high, a_low = split(matrix)
    a_both = jnp.concatenate([a_high, a_low], axis=0)
    for at in range(2 * held):
        c, k = divmod(at, held)
        for begin in range(0, sensors, ROWS * GROUPS):
            packed = slice(begin // GROUPS, begin // GROUPS + ROWS)
            values = parts(at, packed)
            for group in range(min(GROUPS, (sensors - begin) // ROWS)):
                tile = jnp.zeros((ROWS, LANES), jnp.float32)
                for value, spot in zip(values, spots):
                    moved = pltpu.roll(value, (spot - group * SWEEPS) % LANES, 1)
                    tile = jnp.where((lane >= spot) & (lane < spot + SWEEPS), moved, tile)
                rows_at = begin + group * ROWS
                sides[rows_at : rows_at + ROWS] = tile
        high, low = split(sides[...])
        both = product(a_both, high, ((1,), (1,)))
        total = near_ref[c, k] + both[: 2 * NEAR] + both[2 * NEAR :] + product(a_high, low, ((1,), (1,)))
        high, low = split(total)
        high_ref[c, k] = high
        low_ref[c, k] = low


def near_edges(near, own_inner, own_outer, inner, outer, band_index, band_rates):
    shape = jax.ShapeDtypeStruct(near.shape, jnp.bfloat16)
    held, sensors = near.shape[1], near.shape[3]
    return pl.pallas_call(
        near_kernel,
        in_specs=[VMEM_SPEC] * 6 + [SMEM_SPEC],
        out_specs=[VMEM_SPEC] * 2,
        out_shape=[shape, shape],
        scratch_shapes=[pltpu.VMEM((sensors, LANES), jnp.float32)],
        compiler_params=grant(8),
        cost_estimate=pl.CostEstimate(
            flops=24 * held * sensors * NEAR * LANES, bytes_accessed=8 * near.size, transcendentals=0
        ),
        name="near_edges",
    )(near, own_inner, own_outer, inner, outer, band_index.reshape(1, -1), band_rates)


def forward_kernel(
    steps, chips, wanted, x_ref, high_ref, low_ref, near_high_ref, near_low_ref, away_ref, home_ref
):
    share, sensors = home_ref.shape[3:]
    per = share // ROWS
    cell = lax.axis_index("cell")
    chip, core = cell // 2, cell % 2
    cells = x_ref.shape[4]
    order = []
    for side in (1 - core, core):
        for s in steps:
            order.append((2 * lax.rem(chip + s, chips) + side) * per)
    rows = len(order) * share

    def whole(ref, near, c, k):
        inside = ref[c, k, NEAR : cells - NEAR]
        return jnp.concatenate([near[c, k, :NEAR], inside, near[c, k, NEAR:]], axis=0)

    for at, k in enumerate(wanted):
        parts = []
        for c in range(2):
            for first in order:
                parts.append(x_ref[pl.ds(first, per), c, k].reshape(share, cells))
        high, low = split(jnp.concatenate(parts, axis=0))
        both = jnp.concatenate([high, low], axis=0)
        terms = []
        for c in range(2):
            wide = product(both, whole(high_ref, near_high_ref, c, k), ((1,), (0,)))
            small = product(high, whole(low_ref, near_low_ref, c, k), ((1,), (0,)))
            terms.append(wide[: 2 * rows] + wide[2 * rows :] + small)
        re = (terms[0][:rows] - terms[1][rows:]).reshape(2, len(steps), share, sensors)
        im = (terms[0][rows:] + terms[1][:rows]).reshape(2, len(steps), share, sensors)
        for side, ref in enumerate((away_ref, home_ref)):
            ref[:, 0, at] = re[side]
            ref[:, 1, at] = im[side]


def forward(returned, matrices, steps, chips, wanted):
    shards, _, _, rows, cells = returned.shape
    sensors = matrices[0].shape[3]
    share = shards * rows // (2 * chips)
    shape = jax.ShapeDtypeStruct((len(steps), 2, len(wanted), share, sensors), jnp.float32)
    return pl.pallas_call(
        functools.partial(forward_kernel, steps, chips, wanted),
        in_specs=[VMEM_SPEC] * 5,
        out_specs=[VMEM_SPEC] * 2,
        out_shape=[shape, shape],
        compiler_params=grant(16),
        cost_estimate=pl.CostEstimate(
            flops=48 * len(steps) * len(wanted) * share * sensors * cells,
            bytes_accessed=8 * len(wanted) * sensors * cells,
            transcendentals=0,
        ),
    )(returned, *matrices)


def total_kernel(home_ref, away_ref, *refs):
    out_ref = refs[-1]
    held = out_ref.shape[1]
    for k in range(held):
        total = home_ref[0, :, k] + away_ref[0, :, k]
        for ref in refs[k:-1:held]:
            total += ref[:, 0]
        out_ref[:, k] = total


def on_device(columns, freq_blocks, causal_cutoffs, band_index, band_rates):
    shards, strips = lax.axis_size("freq"), lax.axis_size("cell")
    chips = strips // 2
    held = columns.shape[1]
    columns, blocks = in_hbm(columns), in_hbm(freq_blocks)
    spectrum, own_inner, own_outer, cutoff = adjoint(
        columns, blocks, band_index, band_rates, causal_cutoffs, shards
    )
    gathered = lax.all_to_all(spectrum, "freq", split_axis=0, concat_axis=0, tiled=True)
    spectrum = middle(gathered, cutoff)
    spectrum, own_inner, own_outer, freq_blocks = lax.optimization_barrier(
        (spectrum, own_inner, own_outer, freq_blocks)
    )
    blocks = in_hbm(freq_blocks)
    returned = lax.all_to_all(spectrum, "freq", split_axis=0, concat_axis=0, tiled=True)
    swap = [(i, i ^ 1) for i in range(strips)]
    pairs = [(i, i + 1) for i in range(1, strips - 1, 2)]
    outer = lax.ppermute(own_outer, "cell", pairs + [(j, i) for i, j in pairs])
    inner = lax.ppermute(own_inner, "cell", swap)
    high, low, near = smooth(blocks, band_index, band_rates)
    near = near_edges(near, own_inner, own_outer, inner, outer, band_index, band_rates)
    matrices = (high, low, *near)
    leaving = []
    if chips > 1:
        for k in range(held):
            away, home = forward(returned, matrices, range(1, chips), chips, (k,))
            leaving.append(home + lax.ppermute(away, "cell", swap))
    arrived = []
    for s in range(1, chips):
        pairs = [(i, 2 * ((i // 2 + s) % chips) + i % 2) for i in range(strips)]
        for k in range(held):
            arrived.append(lax.ppermute(leaving[k][s - 1], "cell", pairs))
    away, home = forward(returned, matrices, range(1), chips, range(held))
    away = lax.ppermute(away, "cell", swap)
    share, sensors = home.shape[3:]
    return pl.pallas_call(
        total_kernel,
        in_specs=[VMEM_SPEC] * (2 + len(arrived)),
        out_specs=VMEM_SPEC,
        out_shape=jax.ShapeDtypeStruct((2, held, share, sensors), jnp.float32),
        compiler_params=grant(16),
        name="total",
    )(home, away, *arrived)


def solution(mesh):
    placed = (P(None, "freq", None, None), P(None, "freq", None, "cell"), P(), P("cell"), P())
    return jax.shard_map(
        on_device,
        mesh=mesh,
        in_specs=placed,
        out_specs=P(None, "freq", "cell", None),
        check_vma=False,
    )
```

```python
import functools
import math

import jax
import jax.numpy as jnp
import numpy as np
from jax import lax
from jax.experimental import pallas as pl
from jax.experimental.pallas import tpu as pltpu
from jax.sharding import PartitionSpec as P


SWEEPS = 4
BANDS = 8
ROWS = 8
LANES = 128
UNROLLED_FREQS = 32
GROUPS = LANES // SWEEPS
NEAR = 2 * ROWS


VMEM_SPEC = pl.BlockSpec(memory_space=pltpu.VMEM)
SMEM_SPEC = pl.BlockSpec(memory_space=pltpu.SMEM)
HBM_SPEC = pl.BlockSpec(memory_space=pltpu.HBM)


def grant(mib):
    return pltpu.CompilerParams(vmem_limit_bytes=mib * 2**20)


def in_hbm(x):
    return pltpu.with_memory_space_constraint(x, pltpu.HBM)


def split(x):
    high = x.astype(jnp.bfloat16)
    return high, (x - high.astype(jnp.float32)).astype(jnp.bfloat16)


def product(a, b, contract):
    return lax.dot_general(a, b, (contract, ((), ())), preferred_element_type=jnp.float32)


def inverse_table(steps, freqs):
    cycle = 2 * steps
    turns = np.outer(np.arange(steps), np.arange(freqs)) % cycle
    angle = turns * (2.0 * math.pi / cycle)
    weight = np.where((np.arange(freqs) == 0) | (np.arange(freqs) == freqs - 1), 1.0, 2.0) / cycle
    return weight * np.cos(angle), -weight * np.sin(angle)


def forward_table(steps, freqs):
    cycle = 2 * steps
    turns = np.outer(np.arange(freqs), np.arange(steps)) % cycle
    angle = turns * (2.0 * math.pi / cycle)
    return np.cos(angle), -np.sin(angle)


def rates_of(band_ref, rates_ref):
    band = band_ref[...]
    rates = jnp.zeros(band.shape, jnp.float32)
    for b in range(BANDS):
        rates = jnp.where(band == b, rates_ref[b], rates)
    return rates


def adjoint_kernel(
    v_hbm, f_hbm, band_hbm, rates_hbm, cut_hbm, out_ref, inner_ref, outer_ref, cutoff_ref,
    v_ref, f_ref, band_ref, rates_ref, cut_ref, v_sem, f_sem, small_sem,
):
    shards, _, held, rows, cells = out_ref.shape
    cols, sensors = v_ref.shape[2:]
    v_copies, f_copies = [], []
    for k in range(held):
        v_copies.append(pltpu.make_async_copy(v_hbm.at[:, k], v_ref.at[:, k], v_sem.at[k]))
        v_copies[k].start()
        for c in range(2):
            copy = pltpu.make_async_copy(f_hbm.at[c, k], f_ref.at[c, k], f_sem.at[2 * k + c])
            f_copies.append(copy)
            copy.start()
    small = []
    for at, (source, target) in enumerate(((band_hbm, band_ref), (rates_hbm, rates_ref), (cut_hbm, cut_ref))):
        small.append(pltpu.make_async_copy(source, target, small_sem.at[at]))
        small[at].start()
    odd = lax.axis_index("cell") % 2
    last = cells - LANES
    inner_at, inner_shift = pl.multiple_of((1 - odd) * last, LANES), (1 - odd) * SWEEPS
    outer_at, outer_shift = pl.multiple_of(odd * last, LANES), odd * SWEEPS
    lane_group = lax.broadcasted_iota(jnp.int32, (ROWS, LANES), 1) // SWEEPS

    def edge(at, block):
        for ref, lanes, shift in ((inner_ref, inner_at, inner_shift), (outer_ref, outer_at, outer_shift)):
            for first in range(0, sensors, ROWS * GROUPS):
                packed = jnp.zeros((ROWS, LANES), jnp.float32)
                for group in range(min(GROUPS, (sensors - first) // ROWS)):
                    rows_at = first + group * ROWS
                    cells_there = block[rows_at : rows_at + ROWS, pl.ds(lanes, LANES)]
                    moved = pltpu.roll(cells_there, group * SWEEPS + shift, 1)
                    packed = jnp.where(lane_group == group, moved, packed)
                ref[at, first // GROUPS : first // GROUPS + ROWS] = packed

    for k in range(held):
        for copy in (v_copies[k], f_copies[2 * k], f_copies[2 * k + 1]):
            copy.wait()
        high, low = split(v_ref[:, k].reshape(2 * cols, sensors))
        parts = jnp.concatenate([high, low], axis=0)
        sums = []
        for c in range(2):
            f_high, f_low = split(f_ref[c, k])
            both = product(parts, f_high, ((1,), (0,)))
            both = both[: 2 * cols] + both[2 * cols :] + product(high, f_low, ((1,), (0,)))
            sums.append(both)
        re = sums[0][:cols] + sums[1][cols:]
        im = sums[0][cols:] - sums[1][:cols]
        out_ref[:, 0, k] = re.reshape(shards, rows, cells)
        out_ref[:, 1, k] = im.reshape(shards, rows, cells)
        for c in range(2):
            edge(c * held + k, f_ref.at[c, k])
    for copy in small:
        copy.wait()
    rates = rates_of(band_ref, rates_ref)
    for ref, at in ((inner_ref, 1 - odd), (outer_ref, odd)):
        facing = jnp.where(at == 0, rates[:, :LANES], rates[:, last:])
        ref[2 * held] = jnp.broadcast_to(facing, ref.shape[1:])
    base = lax.axis_index("freq") * rows
    row = lax.broadcasted_iota(jnp.int32, (rows, LANES), 0)
    cutoff = jnp.zeros((rows, LANES), jnp.int32)
    for r in range(rows):
        cutoff = jnp.where(row == r, cut_ref[base + r], cutoff)
    cutoff_ref[...] = cutoff


def adjoint(columns, blocks, band_index, band_rates, causal_cutoffs, shards):
    _, held, cols, sensors = columns.shape
    cells = blocks.shape[3]
    out = (shards, 2, held, cols // shards, cells)
    packed = -(-sensors // (ROWS * GROUPS)) * ROWS
    edge = jax.ShapeDtypeStruct((2 * held + 1, packed, LANES), jnp.float32)
    return pl.pallas_call(
        adjoint_kernel,
        in_specs=[HBM_SPEC] * 5,
        out_specs=[VMEM_SPEC] * 4,
        out_shape=[
            jax.ShapeDtypeStruct(out, jnp.float32),
            edge,
            edge,
            jax.ShapeDtypeStruct((cols // shards, LANES), jnp.int32),
        ],
        scratch_shapes=[
            pltpu.VMEM(columns.shape, jnp.float32),
            pltpu.VMEM(blocks.shape, jnp.float32),
            pltpu.VMEM((1, cells), jnp.int32),
            pltpu.SMEM(band_rates.shape, jnp.float32),
            pltpu.SMEM(causal_cutoffs.shape, jnp.int32),
            pltpu.SemaphoreType.DMA((held,)),
            pltpu.SemaphoreType.DMA((2 * held,)),
            pltpu.SemaphoreType.DMA((3,)),
        ],
        compiler_params=grant(16),
        cost_estimate=pl.CostEstimate(
            flops=24 * held * cols * sensors * cells, bytes_accessed=8 * held * sensors * cells, transcendentals=0
        ),
        name="adjoint",
    )(columns, blocks, in_hbm(band_index.reshape(1, cells)), in_hbm(band_rates), in_hbm(causal_cutoffs))


def middle_kernel(x_ref, cutoff_ref, out_hbm, out_ref, out_sem):
    shards, _, held, _, cells = x_ref.shape
    freqs = shards * held
    steps = freqs - 1
    half = freqs // 2
    to_cos, to_sin = inverse_table(steps, freqs)
    from_cos, from_sin = forward_table(steps, freqs)
    cutoff = cutoff_ref[...]
    copies = []
    for lane in range(0, cells, LANES):
        at = pl.ds(lane, LANES)
        even, odd = [], []
        for k in range(half):
            a, b = divmod(k, held)
            c, d = divmod(freqs - 1 - k, held)
            re, im = x_ref[a, 0, b, :, at], x_ref[a, 1, b, :, at]
            re2, im2 = x_ref[c, 0, d, :, at], x_ref[c, 1, d, :, at]
            even += [re + re2, im - im2]
            odd += [re - re2, im + im2]
        series = []
        for t in range(steps):
            total = None
            for k in range(half):
                pair = odd if t % 2 else even
                for value, table in ((pair[2 * k], to_cos), (pair[2 * k + 1], to_sin)):
                    term = value * float(table[t, k])
                    total = term if total is None else total + term
            series.append(jnp.where(cutoff > t, total, 0.0))
        for k in range(half):
            a, b = divmod(k, held)
            c, d = divmod(freqs - 1 - k, held)
            sums = []
            for table in (from_cos, from_sin):
                for parity in (0, 1):
                    total = None
                    for t in range(parity, steps, 2):
                        term = series[t] * float(table[k, t])
                        total = term if total is None else total + term
                    sums.append(total)
            out_ref[a, 0, b, :, at] = sums[0] + sums[1]
            out_ref[c, 0, d, :, at] = sums[0] - sums[1]
            out_ref[a, 1, b, :, at] = sums[2] + sums[3]
            out_ref[c, 1, d, :, at] = sums[3] - sums[2]
        source, target = out_ref.at[:, :, :, :, at], out_hbm.at[:, :, :, :, at]
        copy = pltpu.make_async_copy(source, target, out_sem.at[lane // LANES])
        copies.append(copy)
        copy.start()
    for copy in copies:
        copy.wait()


def middle(gathered, cutoff):
    shards, _, held, rows, cells = gathered.shape
    freqs = shards * held
    steps = freqs - 1
    if freqs <= UNROLLED_FREQS and freqs % 2 == 0:
        return pl.pallas_call(
            middle_kernel,
            in_specs=[VMEM_SPEC, VMEM_SPEC],
            out_specs=HBM_SPEC,
            out_shape=pltpu.HBM(gathered.shape, jnp.float32),
            scratch_shapes=[
                pltpu.VMEM(gathered.shape, jnp.float32),
                pltpu.SemaphoreType.DMA((cells // LANES,)),
            ],
            compiler_params=grant(8),
            cost_estimate=pl.CostEstimate(
                flops=8 * freqs * steps * rows * cells, bytes_accessed=16 * freqs * rows * cells, transcendentals=0
            ),
            name="middle",
        )(gathered, cutoff)
    to_time = jnp.asarray(np.concatenate(inverse_table(steps, freqs), axis=1), jnp.float32)
    to_freq = jnp.asarray(np.concatenate(forward_table(steps, freqs), axis=0), jnp.float32)
    x = gathered.transpose(1, 0, 2, 3, 4).reshape(2 * freqs, rows * cells)
    series = jnp.dot(to_time, x, precision=lax.Precision.HIGHEST).reshape(steps, rows, cells)
    moment = lax.broadcasted_iota(jnp.int32, (steps, rows), 0)
    series = jnp.where((moment < cutoff[None, :, 0])[:, :, None], series, 0.0)
    x = jnp.dot(to_freq, series.reshape(steps, rows * cells), precision=lax.Precision.HIGHEST)
    return x.reshape(2, shards, held, rows, cells).transpose(1, 0, 2, 3, 4)


def diagonals_of(rates):
    width = rates.shape[1]
    diagonals = jnp.where(lax.broadcasted_iota(jnp.int32, (2 * ROWS, width), 0) == ROWS, 1.0, 0.0)
    for _ in range(SWEEPS):
        up = pltpu.roll(pltpu.roll(diagonals, 1, 1), 2 * ROWS - 1, 0)
        down = pltpu.roll(pltpu.roll(diagonals, width - 1, 1), 1, 0)
        diagonals = diagonals + rates * (up - 2.0 * diagonals + down)
    return diagonals


def spread(diagonals, offset):
    tile = jnp.zeros(offset.shape, jnp.float32)
    for o in range(-SWEEPS, SWEEPS + 1):
        tile = jnp.where(offset == o, diagonals[ROWS + o : ROWS + o + 1], tile)
    return tile


def smooth_kernel(f_hbm, band_ref, rates_ref, high_ref, low_ref, near_ref, f_ref, a_both, f_sem):
    _, held, _, cells = f_hbm.shape
    copies = []
    for at in range(2 * held):
        c, k = divmod(at, held)
        copies.append(pltpu.make_async_copy(f_hbm.at[c, k], f_ref.at[c, k], f_sem.at[at]))
        copies[at].start()
    diagonals = diagonals_of(jnp.concatenate([rates_of(band_ref, rates_ref), jnp.zeros((1, LANES), jnp.float32)], axis=1))
    for lanes in range(0, cells, LANES):
        column = lax.broadcasted_iota(jnp.int32, (LANES, LANES), 1)
        row = lax.broadcasted_iota(jnp.int32, (LANES, LANES), 0)
        for rows in range(0, cells, LANES):
            high, low = split(spread(diagonals[:, lanes : lanes + LANES], row - column + (rows - lanes)))
            a_both[rows : rows + LANES, lanes : lanes + LANES] = high
            a_both[cells + rows : cells + rows + LANES, lanes : lanes + LANES] = low
    for at in range(2 * held):
        c, k = divmod(at, held)
        copies[at].wait()
        high, low = split(f_ref[c, k])
        both = product(a_both[...], high, ((1,), (1,)))
        total = both[:cells] + both[cells:] + product(a_both[:cells], low, ((1,), (1,)))
        high, low = split(total)
        high_ref[c, k] = high
        low_ref[c, k] = low
        near_ref[c, k, :NEAR] = total[:NEAR]
        near_ref[c, k, NEAR:] = total[cells - NEAR :]


def smooth(blocks, band_index, band_rates):
    _, held, sensors, cells = blocks.shape
    shape = jax.ShapeDtypeStruct((2, held, cells, sensors), jnp.bfloat16)
    return pl.pallas_call(
        smooth_kernel,
        in_specs=[HBM_SPEC, VMEM_SPEC, SMEM_SPEC],
        out_specs=[VMEM_SPEC] * 3,
        out_shape=[shape, shape, jax.ShapeDtypeStruct((2, held, 2 * NEAR, sensors), jnp.float32)],
        scratch_shapes=[
            pltpu.VMEM(blocks.shape, jnp.float32),
            pltpu.VMEM((2 * cells, cells), jnp.bfloat16),
            pltpu.SemaphoreType.DMA((2 * held,)),
        ],
        compiler_params=grant(16),
        cost_estimate=pl.CostEstimate(
            flops=12 * held * sensors * cells * cells, bytes_accessed=16 * held * sensors * cells, transcendentals=0
        ),
        name="smooth",
    )(blocks, band_index.reshape(1, cells), band_rates)


def near_kernel(
    near_ref, own_inner_ref, own_outer_ref, inner_ref, outer_ref, band_ref, rates_ref, high_ref, low_ref, sides
):
    held = near_ref.shape[1]
    sensors = near_ref.shape[3]
    cells = band_ref.shape[1]
    even = lax.axis_index("cell") % 2 == 0
    kinds = 4
    per = kinds * SWEEPS
    pairs = LANES // (2 * per)

    def parts(at, rows):
        own_inner, own_outer = own_inner_ref[at, rows], own_outer_ref[at, rows]
        inner, outer = inner_ref[at, rows], outer_ref[at, rows]
        return (
            jnp.where(even, own_outer, own_inner),
            jnp.where(even, own_inner, own_outer),
            jnp.where(even, inner, outer),
            jnp.where(even, outer, inner),
        )

    lane = lax.broadcasted_iota(jnp.int32, (ROWS, LANES), 1)
    _, _, after, before = parts(2 * held, slice(0, ROWS))
    side = jnp.where(lane < SWEEPS, after, jnp.where(lane >= LANES - SWEEPS, before, 0.0))[:1]
    own = rates_of(band_ref, rates_ref)
    alone = diagonals_of(jnp.concatenate([own, jnp.zeros((1, LANES), jnp.float32)], axis=1))
    full = diagonals_of(jnp.concatenate([own, side], axis=1))
    first = full[:, :LANES] - alone[:, :LANES]
    last = full[:, cells - LANES : cells] - alone[:, cells - LANES : cells]
    beyond = full[:, cells:]
    kind = lax.broadcasted_iota(jnp.int32, (2 * ROWS, LANES), 1) // SWEEPS
    change = jnp.where(kind == 0, first, 0.0)
    change = jnp.where(kind == 1, pltpu.roll(last, 2 * SWEEPS, 1), change)
    change = jnp.where(kind == 2, pltpu.roll(beyond, 2 * SWEEPS, 1), change)
    change = jnp.where(kind == 3, pltpu.roll(beyond, 4 * SWEEPS, 1), change)
    for shift in (per, 2 * per, 4 * per):
        change = change + pltpu.roll(change, shift, 1)
    row = lax.broadcasted_iota(jnp.int32, (2 * NEAR, LANES), 0)
    column = lax.broadcasted_iota(jnp.int32, (2 * NEAR, LANES), 1)
    kind, i = (column // SWEEPS) % kinds, column % SWEEPS
    at_first = jnp.where(kind == 0, row - i, jnp.where(kind == 3, row + SWEEPS - i, LANES))
    end = row - 2 * NEAR
    at_last = jnp.where(kind == 1, end + SWEEPS - i, jnp.where(kind == 2, end - i, LANES))
    matrix = spread(change, jnp.where(row < NEAR, at_first, at_last))
    a_high, a_low = split(matrix)
    owner = column // per
    cell_of = lane // SWEEPS
    for begin_at in range(0, 2 * held, pairs):
        ats = range(begin_at, min(2 * held, begin_at + pairs))
        for begin in range(0, sensors, ROWS * GROUPS):
            packed = slice(begin // GROUPS, begin // GROUPS + ROWS)
            values = [value for at in ats for value in parts(at, packed)]
            values = [pltpu.roll(value, n * SWEEPS, 1) if n else value for n, value in enumerate(values)]
            for group in range(min(GROUPS, (sensors - begin) // ROWS)):
                tile = jnp.zeros((ROWS, LANES), jnp.float32)
                for n, value in enumerate(values):
                    tile = jnp.where(cell_of == (group + n) % GROUPS, value, tile)
                tile = pltpu.roll(tile, (LANES - group * SWEEPS) % LANES, 1)
                rows_at = begin + group * ROWS
                sides[rows_at : rows_at + ROWS] = tile + pltpu.roll(tile, LANES // 2, 1)
        high, low = split(sides[...])
        low_lane = lax.broadcasted_iota(jnp.int32, (sensors, LANES), 1) >= LANES // 2
        operand = jnp.where(low_lane, low.astype(jnp.float32), high.astype(jnp.float32)).astype(jnp.bfloat16)
        left = []
        for p in range(len(ats)):
            left.append(jnp.where(owner % pairs == p, a_high.astype(jnp.float32), 0.0))
            left.append(jnp.where(owner == p, a_low.astype(jnp.float32), 0.0))
        left = jnp.concatenate(left, axis=0).astype(jnp.bfloat16)
        terms = product(left, operand, ((1,), (1,)))
        for p, at in enumerate(ats):
            c, k = divmod(at, held)
            mine = terms[4 * NEAR * p : 4 * NEAR * (p + 1)]
            high, low = split(near_ref[c, k] + mine[: 2 * NEAR] + mine[2 * NEAR :])
            high_ref[c, k] = high
            low_ref[c, k] = low


def near_edges(near, own_inner, own_outer, inner, outer, band_index, band_rates):
    shape = jax.ShapeDtypeStruct(near.shape, jnp.bfloat16)
    held, sensors = near.shape[1], near.shape[3]
    return pl.pallas_call(
        near_kernel,
        in_specs=[VMEM_SPEC] * 6 + [SMEM_SPEC],
        out_specs=[VMEM_SPEC] * 2,
        out_shape=[shape, shape],
        scratch_shapes=[pltpu.VMEM((sensors, LANES), jnp.float32)],
        compiler_params=grant(8),
        cost_estimate=pl.CostEstimate(
            flops=24 * held * sensors * NEAR * LANES, bytes_accessed=8 * near.size, transcendentals=0
        ),
        name="near_edges",
    )(near, own_inner, own_outer, inner, outer, band_index.reshape(1, -1), band_rates)


def forward_kernel(
    steps, chips, wanted, x_ref, high_ref, low_ref, near_high_ref, near_low_ref, away_ref, home_ref
):
    share, sensors = home_ref.shape[3:]
    per = share // ROWS
    cell = lax.axis_index("cell")
    chip, core = cell // 2, cell % 2
    cells = x_ref.shape[4]
    order = []
    for side in (1 - core, core):
        for s in steps:
            order.append((2 * lax.rem(chip + s, chips) + side) * per)
    rows = len(order) * share

    def whole(ref, near, c, k):
        inside = ref[c, k, NEAR : cells - NEAR]
        return jnp.concatenate([near[c, k, :NEAR], inside, near[c, k, NEAR:]], axis=0)

    for at, k in enumerate(wanted):
        parts = []
        for c in range(2):
            for first in order:
                parts.append(x_ref[pl.ds(first, per), c, k].reshape(share, cells))
        high, low = split(jnp.concatenate(parts, axis=0))
        both = jnp.concatenate([high, low], axis=0)
        terms = []
        for c in range(2):
            wide = product(both, whole(high_ref, near_high_ref, c, k), ((1,), (0,)))
            small = product(high, whole(low_ref, near_low_ref, c, k), ((1,), (0,)))
            terms.append(wide[: 2 * rows] + wide[2 * rows :] + small)
        re = (terms[0][:rows] - terms[1][rows:]).reshape(2, len(steps), share, sensors)
        im = (terms[0][rows:] + terms[1][:rows]).reshape(2, len(steps), share, sensors)
        for side, ref in enumerate((away_ref, home_ref)):
            ref[:, 0, at] = re[side]
            ref[:, 1, at] = im[side]


def forward(returned, matrices, steps, chips, wanted):
    shards, _, _, rows, cells = returned.shape
    sensors = matrices[0].shape[3]
    share = shards * rows // (2 * chips)
    shape = jax.ShapeDtypeStruct((len(steps), 2, len(wanted), share, sensors), jnp.float32)
    return pl.pallas_call(
        functools.partial(forward_kernel, steps, chips, wanted),
        in_specs=[VMEM_SPEC] * 5,
        out_specs=[VMEM_SPEC] * 2,
        out_shape=[shape, shape],
        compiler_params=grant(16),
        cost_estimate=pl.CostEstimate(
            flops=48 * len(steps) * len(wanted) * share * sensors * cells,
            bytes_accessed=8 * len(wanted) * sensors * cells,
            transcendentals=0,
        ),
    )(returned, *matrices)


def total_kernel(home_ref, away_ref, *refs):
    out_ref = refs[-1]
    held = out_ref.shape[1]
    for k in range(held):
        total = home_ref[0, :, k] + away_ref[0, :, k]
        for ref in refs[k:-1:held]:
            total += ref[:, 0]
        out_ref[:, k] = total


def on_device(columns, freq_blocks, causal_cutoffs, band_index, band_rates):
    shards, strips = lax.axis_size("freq"), lax.axis_size("cell")
    chips = strips // 2
    held = columns.shape[1]
    columns, blocks = in_hbm(columns), in_hbm(freq_blocks)
    spectrum, own_inner, own_outer, cutoff = adjoint(
        columns, blocks, band_index, band_rates, causal_cutoffs, shards
    )
    gathered = lax.all_to_all(spectrum, "freq", split_axis=0, concat_axis=0, tiled=True)
    spectrum = middle(gathered, cutoff)
    spectrum, own_inner, own_outer, freq_blocks = lax.optimization_barrier(
        (spectrum, own_inner, own_outer, freq_blocks)
    )
    blocks = in_hbm(freq_blocks)
    returned = lax.all_to_all(spectrum, "freq", split_axis=0, concat_axis=0, tiled=True)
    swap = [(i, i ^ 1) for i in range(strips)]
    pairs = [(i, i + 1) for i in range(1, strips - 1, 2)]
    outer = lax.ppermute(own_outer, "cell", pairs + [(j, i) for i, j in pairs])
    inner = lax.ppermute(own_inner, "cell", swap)
    high, low, near = smooth(blocks, band_index, band_rates)
    near = near_edges(near, own_inner, own_outer, inner, outer, band_index, band_rates)
    matrices = (high, low, *near)
    leaving = []
    if chips > 1:
        for k in range(held):
            away, home = forward(returned, matrices, range(1, chips), chips, (k,))
            leaving.append(home + lax.ppermute(away, "cell", swap))
    arrived = []
    for s in range(1, chips):
        pairs = [(i, 2 * ((i // 2 + s) % chips) + i % 2) for i in range(strips)]
        for k in range(held):
            arrived.append(lax.ppermute(leaving[k][s - 1], "cell", pairs))
    away, home = forward(returned, matrices, range(1), chips, range(held))
    away = lax.ppermute(away, "cell", swap)
    share, sensors = home.shape[3:]
    return pl.pallas_call(
        total_kernel,
        in_specs=[VMEM_SPEC] * (2 + len(arrived)),
        out_specs=VMEM_SPEC,
        out_shape=jax.ShapeDtypeStruct((2, held, share, sensors), jnp.float32),
        compiler_params=grant(16),
        name="total",
    )(home, away, *arrived)


def solution(mesh):
    placed = (P(None, "freq", None, None), P(None, "freq", None, "cell"), P(), P("cell"), P())
    return jax.shard_map(
        on_device,
        mesh=mesh,
        in_specs=placed,
        out_specs=P(None, "freq", "cell", None),
        check_vma=False,
    )
```

```python
import functools
import math

import jax
import jax.numpy as jnp
import numpy as np
from jax import lax
from jax.experimental import pallas as pl
from jax.experimental.pallas import tpu as pltpu
from jax.sharding import PartitionSpec as P


SWEEPS = 4
BANDS = 8
ROWS = 8
LANES = 128
UNROLLED_FREQS = 32
GROUPS = LANES // SWEEPS
NEAR = 2 * ROWS


VMEM_SPEC = pl.BlockSpec(memory_space=pltpu.VMEM)
HBM_SPEC = pl.BlockSpec(memory_space=pltpu.HBM)


def grant(mib):
    return pltpu.CompilerParams(vmem_limit_bytes=mib * 2**20)


def in_hbm(x):
    return pltpu.with_memory_space_constraint(x, pltpu.HBM)


def split(x):
    high = x.astype(jnp.bfloat16)
    return high, (x - high.astype(jnp.float32)).astype(jnp.bfloat16)


def product(a, b, contract):
    return lax.dot_general(a, b, (contract, ((), ())), preferred_element_type=jnp.float32)


def inverse_table(steps, freqs):
    cycle = 2 * steps
    turns = np.outer(np.arange(steps), np.arange(freqs)) % cycle
    angle = turns * (2.0 * math.pi / cycle)
    weight = np.where((np.arange(freqs) == 0) | (np.arange(freqs) == freqs - 1), 1.0, 2.0) / cycle
    return weight * np.cos(angle), -weight * np.sin(angle)


def forward_table(steps, freqs):
    cycle = 2 * steps
    turns = np.outer(np.arange(freqs), np.arange(steps)) % cycle
    angle = turns * (2.0 * math.pi / cycle)
    return np.cos(angle), -np.sin(angle)


def rates_of(band_ref, rates_ref):
    band = band_ref[...]
    rates = jnp.zeros(band.shape, jnp.float32)
    for b in range(BANDS):
        rates = jnp.where(band == b, rates_ref[b], rates)
    return rates


def adjoint_kernel(
    v_hbm, f_hbm, band_hbm, rates_hbm, cut_hbm, out_ref, inner_ref, outer_ref, cutoff_ref, spread_ref,
    v_ref, f_ref, band_ref, rates_ref, cut_ref, v_sem, f_sem, small_sem,
):
    shards, _, held, rows, cells = out_ref.shape
    cols, sensors = v_ref.shape[2:]
    v_copies, f_copies = [], []
    for k in range(held):
        v_copies.append(pltpu.make_async_copy(v_hbm.at[:, k], v_ref.at[:, k], v_sem.at[k]))
        v_copies[k].start()
        for c in range(2):
            copy = pltpu.make_async_copy(f_hbm.at[c, k], f_ref.at[c, k], f_sem.at[2 * k + c])
            f_copies.append(copy)
            copy.start()
    small = []
    for at, (source, target) in enumerate(((band_hbm, band_ref), (rates_hbm, rates_ref), (cut_hbm, cut_ref))):
        small.append(pltpu.make_async_copy(source, target, small_sem.at[at]))
        small[at].start()
    odd = lax.axis_index("cell") % 2
    last = cells - LANES
    inner_at, inner_shift = pl.multiple_of((1 - odd) * last, LANES), (1 - odd) * SWEEPS
    outer_at, outer_shift = pl.multiple_of(odd * last, LANES), odd * SWEEPS
    lane_group = lax.broadcasted_iota(jnp.int32, (ROWS, LANES), 1) // SWEEPS

    def edge(at, block):
        for ref, lanes, shift in ((inner_ref, inner_at, inner_shift), (outer_ref, outer_at, outer_shift)):
            for first in range(0, sensors, ROWS * GROUPS):
                packed = jnp.zeros((ROWS, LANES), jnp.float32)
                for group in range(min(GROUPS, (sensors - first) // ROWS)):
                    rows_at = first + group * ROWS
                    cells_there = block[rows_at : rows_at + ROWS, pl.ds(lanes, LANES)]
                    moved = pltpu.roll(cells_there, group * SWEEPS + shift, 1)
                    packed = jnp.where(lane_group == group, moved, packed)
                ref[at, first // GROUPS : first // GROUPS + ROWS] = packed

    for k in range(held):
        for copy in (v_copies[k], f_copies[2 * k], f_copies[2 * k + 1]):
            copy.wait()
        high, low = split(v_ref[:, k].reshape(2 * cols, sensors))
        parts = jnp.concatenate([high, low], axis=0)
        sums = []
        for c in range(2):
            f_high, f_low = split(f_ref[c, k])
            both = product(parts, f_high, ((1,), (0,)))
            both = both[: 2 * cols] + both[2 * cols :] + product(high, f_low, ((1,), (0,)))
            sums.append(both)
        re = sums[0][:cols] + sums[1][cols:]
        im = sums[0][cols:] - sums[1][:cols]
        out_ref[:, 0, k] = re.reshape(shards, rows, cells)
        out_ref[:, 1, k] = im.reshape(shards, rows, cells)
        for c in range(2):
            edge(c * held + k, f_ref.at[c, k])
    for copy in small:
        copy.wait()
    rates = rates_of(band_ref, rates_ref)
    spread_ref[...] = jnp.broadcast_to(rates, spread_ref.shape)
    for ref, at in ((inner_ref, 1 - odd), (outer_ref, odd)):
        facing = jnp.where(at == 0, rates[:, :LANES], rates[:, last:])
        ref[2 * held] = jnp.broadcast_to(facing, ref.shape[1:])
    base = lax.axis_index("freq") * rows
    row = lax.broadcasted_iota(jnp.int32, (rows, LANES), 0)
    cutoff = jnp.zeros((rows, LANES), jnp.int32)
    for r in range(rows):
        cutoff = jnp.where(row == r, cut_ref[base + r], cutoff)
    cutoff_ref[...] = cutoff


def adjoint(columns, blocks, band_index, band_rates, causal_cutoffs, shards):
    _, held, cols, sensors = columns.shape
    cells = blocks.shape[3]
    out = (shards, 2, held, cols // shards, cells)
    packed = -(-sensors // (ROWS * GROUPS)) * ROWS
    edge = jax.ShapeDtypeStruct((2 * held + 1, packed, LANES), jnp.float32)
    return pl.pallas_call(
        adjoint_kernel,
        in_specs=[HBM_SPEC] * 5,
        out_specs=[VMEM_SPEC] * 5,
        out_shape=[
            jax.ShapeDtypeStruct(out, jnp.float32),
            edge,
            edge,
            jax.ShapeDtypeStruct((cols // shards, LANES), jnp.int32),
            jax.ShapeDtypeStruct((ROWS, cells), jnp.float32),
        ],
        scratch_shapes=[
            pltpu.VMEM(columns.shape, jnp.float32),
            pltpu.VMEM(blocks.shape, jnp.float32),
            pltpu.VMEM((1, cells), jnp.int32),
            pltpu.SMEM(band_rates.shape, jnp.float32),
            pltpu.SMEM(causal_cutoffs.shape, jnp.int32),
            pltpu.SemaphoreType.DMA((held,)),
            pltpu.SemaphoreType.DMA((2 * held,)),
            pltpu.SemaphoreType.DMA((3,)),
        ],
        compiler_params=grant(16),
        cost_estimate=pl.CostEstimate(
            flops=24 * held * cols * sensors * cells, bytes_accessed=8 * held * sensors * cells, transcendentals=0
        ),
        name="adjoint",
    )(columns, blocks, in_hbm(band_index.reshape(1, cells)), in_hbm(band_rates), in_hbm(causal_cutoffs))


def middle_kernel(x_ref, cutoff_ref, out_hbm, out_ref, out_sem):
    shards, _, held, _, cells = x_ref.shape
    freqs = shards * held
    steps = freqs - 1
    half = freqs // 2
    to_cos, to_sin = inverse_table(steps, freqs)
    from_cos, from_sin = forward_table(steps, freqs)
    cutoff = cutoff_ref[...]
    copies = []
    for lane in range(0, cells, LANES):
        at = pl.ds(lane, LANES)
        even, odd = [], []
        for k in range(half):
            a, b = divmod(k, held)
            c, d = divmod(freqs - 1 - k, held)
            re, im = x_ref[a, 0, b, :, at], x_ref[a, 1, b, :, at]
            re2, im2 = x_ref[c, 0, d, :, at], x_ref[c, 1, d, :, at]
            even += [re + re2, im - im2]
            odd += [re - re2, im + im2]
        series = []
        for t in range(steps):
            total = None
            for k in range(half):
                pair = odd if t % 2 else even
                for value, table in ((pair[2 * k], to_cos), (pair[2 * k + 1], to_sin)):
                    term = value * float(table[t, k])
                    total = term if total is None else total + term
            series.append(jnp.where(cutoff > t, total, 0.0))
        for k in range(half):
            a, b = divmod(k, held)
            c, d = divmod(freqs - 1 - k, held)
            sums = []
            for table in (from_cos, from_sin):
                for parity in (0, 1):
                    total = None
                    for t in range(parity, steps, 2):
                        term = series[t] * float(table[k, t])
                        total = term if total is None else total + term
                    sums.append(total)
            out_ref[a, 0, b, :, at] = sums[0] + sums[1]
            out_ref[c, 0, d, :, at] = sums[0] - sums[1]
            out_ref[a, 1, b, :, at] = sums[2] + sums[3]
            out_ref[c, 1, d, :, at] = sums[3] - sums[2]
        source, target = out_ref.at[:, :, :, :, at], out_hbm.at[:, :, :, :, at]
        copy = pltpu.make_async_copy(source, target, out_sem.at[lane // LANES])
        copies.append(copy)
        copy.start()
    for copy in copies:
        copy.wait()


def middle(gathered, cutoff):
    shards, _, held, rows, cells = gathered.shape
    freqs = shards * held
    steps = freqs - 1
    if freqs <= UNROLLED_FREQS and freqs % 2 == 0:
        return pl.pallas_call(
            middle_kernel,
            in_specs=[VMEM_SPEC, VMEM_SPEC],
            out_specs=HBM_SPEC,
            out_shape=pltpu.HBM(gathered.shape, jnp.float32),
            scratch_shapes=[
                pltpu.VMEM(gathered.shape, jnp.float32),
                pltpu.SemaphoreType.DMA((cells // LANES,)),
            ],
            compiler_params=grant(8),
            cost_estimate=pl.CostEstimate(
                flops=8 * freqs * steps * rows * cells, bytes_accessed=16 * freqs * rows * cells, transcendentals=0
            ),
            name="middle",
        )(gathered, cutoff)
    to_time = jnp.asarray(np.concatenate(inverse_table(steps, freqs), axis=1), jnp.float32)
    to_freq = jnp.asarray(np.concatenate(forward_table(steps, freqs), axis=0), jnp.float32)
    x = gathered.transpose(1, 0, 2, 3, 4).reshape(2 * freqs, rows * cells)
    series = jnp.dot(to_time, x, precision=lax.Precision.HIGHEST).reshape(steps, rows, cells)
    moment = lax.broadcasted_iota(jnp.int32, (steps, rows), 0)
    series = jnp.where((moment < cutoff[None, :, 0])[:, :, None], series, 0.0)
    x = jnp.dot(to_freq, series.reshape(steps, rows * cells), precision=lax.Precision.HIGHEST)
    return x.reshape(2, shards, held, rows, cells).transpose(1, 0, 2, 3, 4)


def diagonals_of(rates):
    width = rates.shape[1]
    diagonals = jnp.where(lax.broadcasted_iota(jnp.int32, (2 * ROWS, width), 0) == ROWS, 1.0, 0.0)
    for _ in range(SWEEPS):
        up = pltpu.roll(pltpu.roll(diagonals, 1, 1), 2 * ROWS - 1, 0)
        down = pltpu.roll(pltpu.roll(diagonals, width - 1, 1), 1, 0)
        diagonals = diagonals + rates * (up - 2.0 * diagonals + down)
    return diagonals


def spread(diagonals, offset):
    tile = jnp.zeros(offset.shape, jnp.float32)
    for o in range(-SWEEPS, SWEEPS + 1):
        tile = jnp.where(offset == o, diagonals[ROWS + o : ROWS + o + 1], tile)
    return tile


def smooth_kernel(f_hbm, rates_ref, high_ref, low_ref, near_ref, f_ref, a_both, f_sem):
    _, held, _, cells = f_hbm.shape
    copies = []
    for at in range(2 * held):
        c, k = divmod(at, held)
        copies.append(pltpu.make_async_copy(f_hbm.at[c, k], f_ref.at[c, k], f_sem.at[at]))
        copies[at].start()
    diagonals = diagonals_of(jnp.concatenate([rates_ref[:1], jnp.zeros((1, LANES), jnp.float32)], axis=1))
    for lanes in range(0, cells, LANES):
        column = lax.broadcasted_iota(jnp.int32, (LANES, LANES), 1)
        row = lax.broadcasted_iota(jnp.int32, (LANES, LANES), 0)
        for rows in range(0, cells, LANES):
            high, low = split(spread(diagonals[:, lanes : lanes + LANES], row - column + (rows - lanes)))
            a_both[rows : rows + LANES, lanes : lanes + LANES] = high
            a_both[cells + rows : cells + rows + LANES, lanes : lanes + LANES] = low
    for at in range(2 * held):
        c, k = divmod(at, held)
        copies[at].wait()
        high, low = split(f_ref[c, k])
        both = product(a_both[...], high, ((1,), (1,)))
        total = both[:cells] + both[cells:] + product(a_both[:cells], low, ((1,), (1,)))
        high, low = split(total)
        high_ref[c, k] = high
        low_ref[c, k] = low
        near_ref[c, k, :NEAR] = total[:NEAR]
        near_ref[c, k, NEAR:] = total[cells - NEAR :]


def smooth(blocks, rates):
    _, held, sensors, cells = blocks.shape
    shape = jax.ShapeDtypeStruct((2, held, cells, sensors), jnp.bfloat16)
    return pl.pallas_call(
        smooth_kernel,
        in_specs=[HBM_SPEC, VMEM_SPEC],
        out_specs=[VMEM_SPEC] * 3,
        out_shape=[shape, shape, jax.ShapeDtypeStruct((2, held, 2 * NEAR, sensors), jnp.float32)],
        scratch_shapes=[
            pltpu.VMEM(blocks.shape, jnp.float32),
            pltpu.VMEM((2 * cells, cells), jnp.bfloat16),
            pltpu.SemaphoreType.DMA((2 * held,)),
        ],
        compiler_params=grant(16),
        cost_estimate=pl.CostEstimate(
            flops=12 * held * sensors * cells * cells, bytes_accessed=16 * held * sensors * cells, transcendentals=0
        ),
        name="smooth",
    )(blocks, rates)


def near_kernel(
    near_ref, own_inner_ref, own_outer_ref, inner_ref, outer_ref, rates_ref, high_ref, low_ref, sides
):
    held = near_ref.shape[1]
    sensors = near_ref.shape[3]
    cells = rates_ref.shape[1]
    even = lax.axis_index("cell") % 2 == 0
    kinds = 4
    per = kinds * SWEEPS
    pairs = LANES // (2 * per)

    def parts(at, rows):
        own_inner, own_outer = own_inner_ref[at, rows], own_outer_ref[at, rows]
        inner, outer = inner_ref[at, rows], outer_ref[at, rows]
        return (
            jnp.where(even, own_outer, own_inner),
            jnp.where(even, own_inner, own_outer),
            jnp.where(even, inner, outer),
            jnp.where(even, outer, inner),
        )

    lane = lax.broadcasted_iota(jnp.int32, (ROWS, LANES), 1)
    _, _, after, before = parts(2 * held, slice(0, ROWS))
    side = jnp.where(lane < SWEEPS, after, jnp.where(lane >= LANES - SWEEPS, before, 0.0))[:1]
    own = rates_ref[:1]
    alone = diagonals_of(jnp.concatenate([own, jnp.zeros((1, LANES), jnp.float32)], axis=1))
    full = diagonals_of(jnp.concatenate([own, side], axis=1))
    first = full[:, :LANES] - alone[:, :LANES]
    last = full[:, cells - LANES : cells] - alone[:, cells - LANES : cells]
    beyond = full[:, cells:]
    kind = lax.broadcasted_iota(jnp.int32, (2 * ROWS, LANES), 1) // SWEEPS
    change = jnp.where(kind == 0, first, 0.0)
    change = jnp.where(kind == 1, pltpu.roll(last, 2 * SWEEPS, 1), change)
    change = jnp.where(kind == 2, pltpu.roll(beyond, 2 * SWEEPS, 1), change)
    change = jnp.where(kind == 3, pltpu.roll(beyond, 4 * SWEEPS, 1), change)
    for shift in (per, 2 * per, 4 * per):
        change = change + pltpu.roll(change, shift, 1)
    row = lax.broadcasted_iota(jnp.int32, (2 * NEAR, LANES), 0)
    column = lax.broadcasted_iota(jnp.int32, (2 * NEAR, LANES), 1)
    kind, i = (column // SWEEPS) % kinds, column % SWEEPS
    at_first = jnp.where(kind == 0, row - i, jnp.where(kind == 3, row + SWEEPS - i, LANES))
    end = row - 2 * NEAR
    at_last = jnp.where(kind == 1, end + SWEEPS - i, jnp.where(kind == 2, end - i, LANES))
    matrix = spread(change, jnp.where(row < NEAR, at_first, at_last))
    a_high, a_low = split(matrix)
    owner = column // per
    cell_of = lane // SWEEPS
    for begin_at in range(0, 2 * held, pairs):
        ats = range(begin_at, min(2 * held, begin_at + pairs))
        for begin in range(0, sensors, ROWS * GROUPS):
            packed = slice(begin // GROUPS, begin // GROUPS + ROWS)
            values = [value for at in ats for value in parts(at, packed)]
            values = [pltpu.roll(value, n * SWEEPS, 1) if n else value for n, value in enumerate(values)]
            for group in range(min(GROUPS, (sensors - begin) // ROWS)):
                tile = jnp.zeros((ROWS, LANES), jnp.float32)
                for n, value in enumerate(values):
                    tile = jnp.where(cell_of == (group + n) % GROUPS, value, tile)
                tile = pltpu.roll(tile, (LANES - group * SWEEPS) % LANES, 1)
                rows_at = begin + group * ROWS
                sides[rows_at : rows_at + ROWS] = tile + pltpu.roll(tile, LANES // 2, 1)
        high, low = split(sides[...])
        low_lane = lax.broadcasted_iota(jnp.int32, (sensors, LANES), 1) >= LANES // 2
        operand = jnp.where(low_lane, low.astype(jnp.float32), high.astype(jnp.float32)).astype(jnp.bfloat16)
        left = []
        for p in range(len(ats)):
            left.append(jnp.where(owner % pairs == p, a_high.astype(jnp.float32), 0.0))
            left.append(jnp.where(owner == p, a_low.astype(jnp.float32), 0.0))
        left = jnp.concatenate(left, axis=0).astype(jnp.bfloat16)
        terms = product(left, operand, ((1,), (1,)))
        for p, at in enumerate(ats):
            c, k = divmod(at, held)
            mine = terms[4 * NEAR * p : 4 * NEAR * (p + 1)]
            high, low = split(near_ref[c, k] + mine[: 2 * NEAR] + mine[2 * NEAR :])
            high_ref[c, k] = high
            low_ref[c, k] = low


def near_edges(near, own_inner, own_outer, inner, outer, rates):
    shape = jax.ShapeDtypeStruct(near.shape, jnp.bfloat16)
    held, sensors = near.shape[1], near.shape[3]
    return pl.pallas_call(
        near_kernel,
        in_specs=[VMEM_SPEC] * 6,
        out_specs=[VMEM_SPEC] * 2,
        out_shape=[shape, shape],
        scratch_shapes=[pltpu.VMEM((sensors, LANES), jnp.float32)],
        compiler_params=grant(8),
        cost_estimate=pl.CostEstimate(
            flops=24 * held * sensors * NEAR * LANES, bytes_accessed=8 * near.size, transcendentals=0
        ),
        name="near_edges",
    )(near, own_inner, own_outer, inner, outer, rates)


def forward_kernel(
    steps, chips, wanted, x_ref, high_ref, low_ref, near_high_ref, near_low_ref, away_ref, home_ref
):
    share, sensors = home_ref.shape[3:]
    per = share // ROWS
    cell = lax.axis_index("cell")
    chip, core = cell // 2, cell % 2
    cells = x_ref.shape[4]
    order = []
    for side in (1 - core, core):
        for s in steps:
            order.append((2 * lax.rem(chip + s, chips) + side) * per)
    rows = len(order) * share

    def whole(ref, near, c, k):
        inside = ref[c, k, NEAR : cells - NEAR]
        return jnp.concatenate([near[c, k, :NEAR], inside, near[c, k, NEAR:]], axis=0)

    for at, k in enumerate(wanted):
        parts = []
        for c in range(2):
            for first in order:
                parts.append(x_ref[pl.ds(first, per), c, k].reshape(share, cells))
        high, low = split(jnp.concatenate(parts, axis=0))
        both = jnp.concatenate([high, low], axis=0)
        terms = []
        for c in range(2):
            wide = product(both, whole(high_ref, near_high_ref, c, k), ((1,), (0,)))
            small = product(high, whole(low_ref, near_low_ref, c, k), ((1,), (0,)))
            terms.append(wide[: 2 * rows] + wide[2 * rows :] + small)
        re = (terms[0][:rows] - terms[1][rows:]).reshape(2, len(steps), share, sensors)
        im = (terms[0][rows:] + terms[1][:rows]).reshape(2, len(steps), share, sensors)
        for side, ref in enumerate((away_ref, home_ref)):
            ref[:, 0, at] = re[side]
            ref[:, 1, at] = im[side]


def forward(returned, matrices, steps, chips, wanted):
    shards, _, _, rows, cells = returned.shape
    sensors = matrices[0].shape[3]
    share = shards * rows // (2 * chips)
    shape = jax.ShapeDtypeStruct((len(steps), 2, len(wanted), share, sensors), jnp.float32)
    return pl.pallas_call(
        functools.partial(forward_kernel, steps, chips, wanted),
        in_specs=[VMEM_SPEC] * 5,
        out_specs=[VMEM_SPEC] * 2,
        out_shape=[shape, shape],
        compiler_params=grant(16),
        cost_estimate=pl.CostEstimate(
            flops=48 * len(steps) * len(wanted) * share * sensors * cells,
            bytes_accessed=8 * len(wanted) * sensors * cells,
            transcendentals=0,
        ),
    )(returned, *matrices)


def total_kernel(home_ref, away_ref, *refs):
    out_ref = refs[-1]
    held = out_ref.shape[1]
    for k in range(held):
        total = home_ref[0, :, k] + away_ref[0, :, k]
        for ref in refs[k:-1:held]:
            total += ref[:, 0]
        out_ref[:, k] = total


def on_device(columns, freq_blocks, causal_cutoffs, band_index, band_rates):
    shards, strips = lax.axis_size("freq"), lax.axis_size("cell")
    chips = strips // 2
    held = columns.shape[1]
    columns, blocks = in_hbm(columns), in_hbm(freq_blocks)
    spectrum, own_inner, own_outer, cutoff, rates = adjoint(
        columns, blocks, band_index, band_rates, causal_cutoffs, shards
    )
    gathered = lax.all_to_all(spectrum, "freq", split_axis=0, concat_axis=0, tiled=True)
    spectrum = middle(gathered, cutoff)
    spectrum, own_inner, own_outer, freq_blocks = lax.optimization_barrier(
        (spectrum, own_inner, own_outer, freq_blocks)
    )
    blocks = in_hbm(freq_blocks)
    returned = lax.all_to_all(spectrum, "freq", split_axis=0, concat_axis=0, tiled=True)
    swap = [(i, i ^ 1) for i in range(strips)]
    pairs = [(i, i + 1) for i in range(1, strips - 1, 2)]
    outer = lax.ppermute(own_outer, "cell", pairs + [(j, i) for i, j in pairs])
    inner = lax.ppermute(own_inner, "cell", swap)
    high, low, near = smooth(blocks, rates)
    near = near_edges(near, own_inner, own_outer, inner, outer, rates)
    matrices = (high, low, *near)
    leaving = []
    if chips > 1:
        for k in range(held):
            away, home = forward(returned, matrices, range(1, chips), chips, (k,))
            leaving.append(home + lax.ppermute(away, "cell", swap))
    arrived = []
    for s in range(1, chips):
        pairs = [(i, 2 * ((i // 2 + s) % chips) + i % 2) for i in range(strips)]
        for k in range(held):
            arrived.append(lax.ppermute(leaving[k][s - 1], "cell", pairs))
    away, home = forward(returned, matrices, range(1), chips, range(held))
    away = lax.ppermute(away, "cell", swap)
    share, sensors = home.shape[3:]
    return pl.pallas_call(
        total_kernel,
        in_specs=[VMEM_SPEC] * (2 + len(arrived)),
        out_specs=VMEM_SPEC,
        out_shape=jax.ShapeDtypeStruct((2, held, share, sensors), jnp.float32),
        compiler_params=grant(16),
        name="total",
    )(home, away, *arrived)


def solution(mesh):
    placed = (P(None, "freq", None, None), P(None, "freq", None, "cell"), P(), P("cell"), P())
    return jax.shard_map(
        on_device,
        mesh=mesh,
        in_specs=placed,
        out_specs=P(None, "freq", "cell", None),
        check_vma=False,
    )
```

```python
import functools
import math

import jax
import jax.numpy as jnp
import numpy as np
from jax import lax
from jax.experimental import pallas as pl
from jax.experimental.pallas import tpu as pltpu
from jax.sharding import PartitionSpec as P


SWEEPS = 4
BANDS = 8
ROWS = 8
LANES = 128
UNROLLED_FREQS = 32
GROUPS = LANES // SWEEPS
NEAR = 2 * ROWS


VMEM_SPEC = pl.BlockSpec(memory_space=pltpu.VMEM)
HBM_SPEC = pl.BlockSpec(memory_space=pltpu.HBM)


def grant(mib):
    return pltpu.CompilerParams(vmem_limit_bytes=mib * 2**20)


def in_hbm(x):
    return pltpu.with_memory_space_constraint(x, pltpu.HBM)


def split(x):
    high = x.astype(jnp.bfloat16)
    return high, (x - high.astype(jnp.float32)).astype(jnp.bfloat16)


def product(a, b, contract):
    return lax.dot_general(a, b, (contract, ((), ())), preferred_element_type=jnp.float32)


def inverse_table(steps, freqs):
    cycle = 2 * steps
    turns = np.outer(np.arange(steps), np.arange(freqs)) % cycle
    angle = turns * (2.0 * math.pi / cycle)
    weight = np.where((np.arange(freqs) == 0) | (np.arange(freqs) == freqs - 1), 1.0, 2.0) / cycle
    return weight * np.cos(angle), -weight * np.sin(angle)


def forward_table(steps, freqs):
    cycle = 2 * steps
    turns = np.outer(np.arange(freqs), np.arange(steps)) % cycle
    angle = turns * (2.0 * math.pi / cycle)
    return np.cos(angle), -np.sin(angle)


def rates_of(band_ref, rates_ref):
    band = band_ref[...]
    rates = jnp.zeros(band.shape, jnp.float32)
    for b in range(BANDS):
        rates = jnp.where(band == b, rates_ref[b], rates)
    return rates


def packed_of(sensors):
    return -(-sensors // (ROWS * GROUPS)) * ROWS


def adjoint_kernel(
    v_hbm, f_hbm, band_hbm, rates_hbm, cut_hbm, out_ref, inner_ref, outer_ref, cutoff_ref, spread_ref,
    v_ref, f_ref, band_ref, rates_ref, cut_ref, v_sem, f_sem, small_sem,
):
    shards, _, held, rows, cells = out_ref.shape
    cols, sensors = v_ref.shape[2:]
    v_copies, f_copies = [], []
    for k in range(held):
        v_copies.append(pltpu.make_async_copy(v_hbm.at[:, k], v_ref.at[:, k], v_sem.at[k]))
        v_copies[k].start()
        for c in range(2):
            copy = pltpu.make_async_copy(f_hbm.at[c, k], f_ref.at[c, k], f_sem.at[2 * k + c])
            f_copies.append(copy)
            copy.start()
    small = []
    for at, (source, target) in enumerate(((band_hbm, band_ref), (rates_hbm, rates_ref), (cut_hbm, cut_ref))):
        small.append(pltpu.make_async_copy(source, target, small_sem.at[at]))
        small[at].start()
    odd = lax.axis_index("cell") % 2
    last = cells - LANES
    inner_at, inner_shift = pl.multiple_of((1 - odd) * last, LANES), (1 - odd) * SWEEPS
    outer_at, outer_shift = pl.multiple_of(odd * last, LANES), odd * SWEEPS
    lane_group = lax.broadcasted_iota(jnp.int32, (ROWS, LANES), 1) // SWEEPS
    packed_rows = packed_of(sensors)

    def edge(at, block):
        for ref, lanes, shift in ((inner_ref, inner_at, inner_shift), (outer_ref, outer_at, outer_shift)):
            for first in range(0, sensors, ROWS * GROUPS):
                packed = jnp.zeros((ROWS, LANES), jnp.float32)
                for group in range(min(GROUPS, (sensors - first) // ROWS)):
                    rows_at = first + group * ROWS
                    cells_there = block[rows_at : rows_at + ROWS, pl.ds(lanes, LANES)]
                    moved = pltpu.roll(cells_there, group * SWEEPS + shift, 1)
                    packed = jnp.where(lane_group == group, moved, packed)
                place = at * packed_rows + first // GROUPS
                ref[place : place + ROWS] = packed

    for copy in v_copies + f_copies:
        copy.wait()
    for k in range(held):
        high, low = split(v_ref[:, k].reshape(2 * cols, sensors))
        parts = jnp.concatenate([high, low], axis=0)
        sums = []
        for c in range(2):
            f_high, f_low = split(f_ref[c, k])
            both = product(parts, f_high, ((1,), (0,)))
            both = both[: 2 * cols] + both[2 * cols :] + product(high, f_low, ((1,), (0,)))
            sums.append(both)
        re = sums[0][:cols] + sums[1][cols:]
        im = sums[0][cols:] - sums[1][:cols]
        out_ref[:, 0, k] = re.reshape(shards, rows, cells)
        out_ref[:, 1, k] = im.reshape(shards, rows, cells)
        for c in range(2):
            edge(c * held + k, f_ref.at[c, k])
    for copy in small:
        copy.wait()
    rates = rates_of(band_ref, rates_ref)
    spread_ref[...] = jnp.broadcast_to(rates, spread_ref.shape)
    for ref, at in ((inner_ref, 1 - odd), (outer_ref, odd)):
        facing = jnp.where(at == 0, rates[:, :LANES], rates[:, last:])
        ref[2 * held * packed_rows :] = jnp.broadcast_to(facing, (ROWS, LANES))
    base = lax.axis_index("freq") * rows
    row = lax.broadcasted_iota(jnp.int32, (rows, LANES), 0)
    cutoff = jnp.zeros((rows, LANES), jnp.int32)
    for r in range(rows):
        cutoff = jnp.where(row == r, cut_ref[base + r], cutoff)
    cutoff_ref[...] = cutoff


def adjoint(columns, blocks, band_index, band_rates, causal_cutoffs, shards):
    _, held, cols, sensors = columns.shape
    cells = blocks.shape[3]
    out = (shards, 2, held, cols // shards, cells)
    edge = jax.ShapeDtypeStruct((2 * held * packed_of(sensors) + ROWS, LANES), jnp.float32)
    return pl.pallas_call(
        adjoint_kernel,
        in_specs=[HBM_SPEC] * 5,
        out_specs=[VMEM_SPEC] * 5,
        out_shape=[
            jax.ShapeDtypeStruct(out, jnp.float32),
            edge,
            edge,
            jax.ShapeDtypeStruct((cols // shards, LANES), jnp.int32),
            jax.ShapeDtypeStruct((ROWS, cells), jnp.float32),
        ],
        scratch_shapes=[
            pltpu.VMEM(columns.shape, jnp.float32),
            pltpu.VMEM(blocks.shape, jnp.float32),
            pltpu.VMEM((1, cells), jnp.int32),
            pltpu.SMEM(band_rates.shape, jnp.float32),
            pltpu.SMEM(causal_cutoffs.shape, jnp.int32),
            pltpu.SemaphoreType.DMA((held,)),
            pltpu.SemaphoreType.DMA((2 * held,)),
            pltpu.SemaphoreType.DMA((3,)),
        ],
        compiler_params=grant(16),
        cost_estimate=pl.CostEstimate(
            flops=24 * held * cols * sensors * cells, bytes_accessed=8 * held * sensors * cells, transcendentals=0
        ),
        name="adjoint",
    )(columns, blocks, in_hbm(band_index.reshape(1, cells)), in_hbm(band_rates), in_hbm(causal_cutoffs))


def middle_kernel(x_ref, cutoff_ref, out_hbm, out_ref, out_sem):
    shards, _, held, _, cells = x_ref.shape
    freqs = shards * held
    steps = freqs - 1
    half = freqs // 2
    to_cos, to_sin = inverse_table(steps, freqs)
    from_cos, from_sin = forward_table(steps, freqs)
    cutoff = cutoff_ref[...]
    copies = []
    for lane in range(0, cells, LANES):
        at = pl.ds(lane, LANES)
        even, odd = [], []
        for k in range(half):
            a, b = divmod(k, held)
            c, d = divmod(freqs - 1 - k, held)
            re, im = x_ref[a, 0, b, :, at], x_ref[a, 1, b, :, at]
            re2, im2 = x_ref[c, 0, d, :, at], x_ref[c, 1, d, :, at]
            even += [re + re2, im - im2]
            odd += [re - re2, im + im2]
        series = []
        for t in range(steps):
            total = None
            for k in range(half):
                pair = odd if t % 2 else even
                for value, table in ((pair[2 * k], to_cos), (pair[2 * k + 1], to_sin)):
                    term = value * float(table[t, k])
                    total = term if total is None else total + term
            series.append(jnp.where(cutoff > t, total, 0.0))
        for k in range(half):
            a, b = divmod(k, held)
            c, d = divmod(freqs - 1 - k, held)
            sums = []
            for table in (from_cos, from_sin):
                for parity in (0, 1):
                    total = None
                    for t in range(parity, steps, 2):
                        term = series[t] * float(table[k, t])
                        total = term if total is None else total + term
                    sums.append(total)
            out_ref[a, 0, b, :, at] = sums[0] + sums[1]
            out_ref[c, 0, d, :, at] = sums[0] - sums[1]
            out_ref[a, 1, b, :, at] = sums[2] + sums[3]
            out_ref[c, 1, d, :, at] = sums[3] - sums[2]
        source, target = out_ref.at[:, :, :, :, at], out_hbm.at[:, :, :, :, at]
        copy = pltpu.make_async_copy(source, target, out_sem.at[lane // LANES])
        copies.append(copy)
        copy.start()
    for copy in copies:
        copy.wait()


def middle(gathered, cutoff):
    shards, _, held, rows, cells = gathered.shape
    freqs = shards * held
    steps = freqs - 1
    if freqs <= UNROLLED_FREQS and freqs % 2 == 0:
        return pl.pallas_call(
            middle_kernel,
            in_specs=[VMEM_SPEC, VMEM_SPEC],
            out_specs=HBM_SPEC,
            out_shape=pltpu.HBM(gathered.shape, jnp.float32),
            scratch_shapes=[
                pltpu.VMEM(gathered.shape, jnp.float32),
                pltpu.SemaphoreType.DMA((cells // LANES,)),
            ],
            compiler_params=grant(8),
            cost_estimate=pl.CostEstimate(
                flops=8 * freqs * steps * rows * cells, bytes_accessed=16 * freqs * rows * cells, transcendentals=0
            ),
            name="middle",
        )(gathered, cutoff)
    to_time = jnp.asarray(np.concatenate(inverse_table(steps, freqs), axis=1), jnp.float32)
    to_freq = jnp.asarray(np.concatenate(forward_table(steps, freqs), axis=0), jnp.float32)
    x = gathered.transpose(1, 0, 2, 3, 4).reshape(2 * freqs, rows * cells)
    series = jnp.dot(to_time, x, precision=lax.Precision.HIGHEST).reshape(steps, rows, cells)
    moment = lax.broadcasted_iota(jnp.int32, (steps, rows), 0)
    series = jnp.where((moment < cutoff[None, :, 0])[:, :, None], series, 0.0)
    x = jnp.dot(to_freq, series.reshape(steps, rows * cells), precision=lax.Precision.HIGHEST)
    return x.reshape(2, shards, held, rows, cells).transpose(1, 0, 2, 3, 4)


def diagonals_of(rates):
    width = rates.shape[1]
    diagonals = jnp.where(lax.broadcasted_iota(jnp.int32, (2 * ROWS, width), 0) == ROWS, 1.0, 0.0)
    for _ in range(SWEEPS):
        up = pltpu.roll(pltpu.roll(diagonals, 1, 1), 2 * ROWS - 1, 0)
        down = pltpu.roll(pltpu.roll(diagonals, width - 1, 1), 1, 0)
        diagonals = diagonals + rates * (up - 2.0 * diagonals + down)
    return diagonals


def spread(diagonals, offset):
    tile = jnp.zeros(offset.shape, jnp.float32)
    for o in range(-SWEEPS, SWEEPS + 1):
        tile = jnp.where(offset == o, diagonals[ROWS + o : ROWS + o + 1], tile)
    return tile


def smooth_kernel(f_hbm, rates_ref, high_ref, low_ref, near_ref, f_ref, a_both, f_sem):
    _, held, _, cells = f_hbm.shape
    copies = []
    for at in range(2 * held):
        c, k = divmod(at, held)
        copies.append(pltpu.make_async_copy(f_hbm.at[c, k], f_ref.at[c, k], f_sem.at[at]))
        copies[at].start()
    diagonals = diagonals_of(jnp.concatenate([rates_ref[:1], jnp.zeros((1, LANES), jnp.float32)], axis=1))
    for lanes in range(0, cells, LANES):
        column = lax.broadcasted_iota(jnp.int32, (LANES, LANES), 1)
        row = lax.broadcasted_iota(jnp.int32, (LANES, LANES), 0)
        for rows in range(0, cells, LANES):
            high, low = split(spread(diagonals[:, lanes : lanes + LANES], row - column + (rows - lanes)))
            a_both[rows : rows + LANES, lanes : lanes + LANES] = high
            a_both[cells + rows : cells + rows + LANES, lanes : lanes + LANES] = low
    for at in range(2 * held):
        c, k = divmod(at, held)
        copies[at].wait()
        high, low = split(f_ref[c, k])
        both = product(a_both[...], high, ((1,), (1,)))
        total = both[:cells] + both[cells:] + product(a_both[:cells], low, ((1,), (1,)))
        high, low = split(total)
        high_ref[c, k] = high
        low_ref[c, k] = low
        near_ref[c, k, :NEAR] = total[:NEAR]
        near_ref[c, k, NEAR:] = total[cells - NEAR :]


def smooth(blocks, rates):
    _, held, sensors, cells = blocks.shape
    shape = jax.ShapeDtypeStruct((2, held, cells, sensors), jnp.bfloat16)
    return pl.pallas_call(
        smooth_kernel,
        in_specs=[HBM_SPEC, VMEM_SPEC],
        out_specs=[VMEM_SPEC] * 3,
        out_shape=[shape, shape, jax.ShapeDtypeStruct((2, held, 2 * NEAR, sensors), jnp.float32)],
        scratch_shapes=[
            pltpu.VMEM(blocks.shape, jnp.float32),
            pltpu.VMEM((2 * cells, cells), jnp.bfloat16),
            pltpu.SemaphoreType.DMA((2 * held,)),
        ],
        compiler_params=grant(16),
        cost_estimate=pl.CostEstimate(
            flops=12 * held * sensors * cells * cells, bytes_accessed=16 * held * sensors * cells, transcendentals=0
        ),
        name="smooth",
    )(blocks, rates)


def near_kernel(
    near_ref, own_inner_ref, own_outer_ref, inner_ref, outer_ref, rates_ref, high_ref, low_ref, sides
):
    held = near_ref.shape[1]
    sensors = near_ref.shape[3]
    cells = rates_ref.shape[1]
    even = lax.axis_index("cell") % 2 == 0
    kinds = 4
    per = kinds * SWEEPS
    pairs = LANES // (2 * per)

    def parts(first):
        rows = slice(first, first + ROWS)
        own_inner, own_outer = own_inner_ref[rows], own_outer_ref[rows]
        inner, outer = inner_ref[rows], outer_ref[rows]
        return (
            jnp.where(even, own_outer, own_inner),
            jnp.where(even, own_inner, own_outer),
            jnp.where(even, inner, outer),
            jnp.where(even, outer, inner),
        )

    lane = lax.broadcasted_iota(jnp.int32, (ROWS, LANES), 1)
    packed_rows = packed_of(sensors)
    _, _, after, before = parts(2 * held * packed_rows)
    side = jnp.where(lane < SWEEPS, after, jnp.where(lane >= LANES - SWEEPS, before, 0.0))[:1]
    own = rates_ref[:1]
    alone = diagonals_of(jnp.concatenate([own, jnp.zeros((1, LANES), jnp.float32)], axis=1))
    full = diagonals_of(jnp.concatenate([own, side], axis=1))
    first = full[:, :LANES] - alone[:, :LANES]
    last = full[:, cells - LANES : cells] - alone[:, cells - LANES : cells]
    beyond = full[:, cells:]
    kind = lax.broadcasted_iota(jnp.int32, (2 * ROWS, LANES), 1) // SWEEPS
    change = jnp.where(kind == 0, first, 0.0)
    change = jnp.where(kind == 1, pltpu.roll(last, 2 * SWEEPS, 1), change)
    change = jnp.where(kind == 2, pltpu.roll(beyond, 2 * SWEEPS, 1), change)
    change = jnp.where(kind == 3, pltpu.roll(beyond, 4 * SWEEPS, 1), change)
    for shift in (per, 2 * per, 4 * per):
        change = change + pltpu.roll(change, shift, 1)
    row = lax.broadcasted_iota(jnp.int32, (2 * NEAR, LANES), 0)
    column = lax.broadcasted_iota(jnp.int32, (2 * NEAR, LANES), 1)
    kind, i = (column // SWEEPS) % kinds, column % SWEEPS
    at_first = jnp.where(kind == 0, row - i, jnp.where(kind == 3, row + SWEEPS - i, LANES))
    end = row - 2 * NEAR
    at_last = jnp.where(kind == 1, end + SWEEPS - i, jnp.where(kind == 2, end - i, LANES))
    matrix = spread(change, jnp.where(row < NEAR, at_first, at_last))
    a_high, a_low = split(matrix)
    owner = column // per
    cell_of = lane // SWEEPS
    for begin_at in range(0, 2 * held, pairs):
        ats = range(begin_at, min(2 * held, begin_at + pairs))
        for begin in range(0, sensors, ROWS * GROUPS):
            values = [value for at in ats for value in parts(at * packed_rows + begin // GROUPS)]
            values = [pltpu.roll(value, n * SWEEPS, 1) if n else value for n, value in enumerate(values)]
            for group in range(min(GROUPS, (sensors - begin) // ROWS)):
                tile = jnp.zeros((ROWS, LANES), jnp.float32)
                for n, value in enumerate(values):
                    tile = jnp.where(cell_of == (group + n) % GROUPS, value, tile)
                tile = pltpu.roll(tile, (LANES - group * SWEEPS) % LANES, 1)
                rows_at = begin + group * ROWS
                sides[rows_at : rows_at + ROWS] = tile + pltpu.roll(tile, LANES // 2, 1)
        high, low = split(sides[...])
        low_lane = lax.broadcasted_iota(jnp.int32, (sensors, LANES), 1) >= LANES // 2
        operand = jnp.where(low_lane, low.astype(jnp.float32), high.astype(jnp.float32)).astype(jnp.bfloat16)
        left = []
        for p in range(len(ats)):
            left.append(jnp.where(owner % pairs == p, a_high.astype(jnp.float32), 0.0))
            left.append(jnp.where(owner == p, a_low.astype(jnp.float32), 0.0))
        left = jnp.concatenate(left, axis=0).astype(jnp.bfloat16)
        terms = product(left, operand, ((1,), (1,)))
        for p, at in enumerate(ats):
            c, k = divmod(at, held)
            mine = terms[4 * NEAR * p : 4 * NEAR * (p + 1)]
            high, low = split(near_ref[c, k] + mine[: 2 * NEAR] + mine[2 * NEAR :])
            high_ref[c, k] = high
            low_ref[c, k] = low


def near_edges(near, own_inner, own_outer, inner, outer, rates):
    shape = jax.ShapeDtypeStruct(near.shape, jnp.bfloat16)
    held, sensors = near.shape[1], near.shape[3]
    return pl.pallas_call(
        near_kernel,
        in_specs=[VMEM_SPEC] * 6,
        out_specs=[VMEM_SPEC] * 2,
        out_shape=[shape, shape],
        scratch_shapes=[pltpu.VMEM((sensors, LANES), jnp.float32)],
        compiler_params=grant(8),
        cost_estimate=pl.CostEstimate(
            flops=24 * held * sensors * NEAR * LANES, bytes_accessed=8 * near.size, transcendentals=0
        ),
        name="near_edges",
    )(near, own_inner, own_outer, inner, outer, rates)


def forward_kernel(
    steps, chips, wanted, x_ref, high_ref, low_ref, near_high_ref, near_low_ref, away_ref, home_ref
):
    share, sensors = home_ref.shape[3:]
    per = share // ROWS
    cell = lax.axis_index("cell")
    chip, core = cell // 2, cell % 2
    cells = x_ref.shape[4]
    order = []
    for side in (1 - core, core):
        for s in steps:
            order.append((2 * lax.rem(chip + s, chips) + side) * per)
    rows = len(order) * share

    def whole(ref, near, c, k):
        inside = ref[c, k, NEAR : cells - NEAR]
        return jnp.concatenate([near[c, k, :NEAR], inside, near[c, k, NEAR:]], axis=0)

    for at, k in enumerate(wanted):
        parts = []
        for c in range(2):
            for first in order:
                parts.append(x_ref[pl.ds(first, per), c, k].reshape(share, cells))
        high, low = split(jnp.concatenate(parts, axis=0))
        both = jnp.concatenate([high, low], axis=0)
        terms = []
        for c in range(2):
            wide = product(both, whole(high_ref, near_high_ref, c, k), ((1,), (0,)))
            small = product(high, whole(low_ref, near_low_ref, c, k), ((1,), (0,)))
            terms.append(wide[: 2 * rows] + wide[2 * rows :] + small)
        re = (terms[0][:rows] - terms[1][rows:]).reshape(2, len(steps), share, sensors)
        im = (terms[0][rows:] + terms[1][:rows]).reshape(2, len(steps), share, sensors)
        for side, ref in enumerate((away_ref, home_ref)):
            ref[:, 0, at] = re[side]
            ref[:, 1, at] = im[side]


def forward(returned, matrices, steps, chips, wanted):
    shards, _, _, rows, cells = returned.shape
    sensors = matrices[0].shape[3]
    share = shards * rows // (2 * chips)
    shape = jax.ShapeDtypeStruct((len(steps), 2, len(wanted), share, sensors), jnp.float32)
    return pl.pallas_call(
        functools.partial(forward_kernel, steps, chips, wanted),
        in_specs=[VMEM_SPEC] * 5,
        out_specs=[VMEM_SPEC] * 2,
        out_shape=[shape, shape],
        compiler_params=grant(16),
        cost_estimate=pl.CostEstimate(
            flops=48 * len(steps) * len(wanted) * share * sensors * cells,
            bytes_accessed=8 * len(wanted) * sensors * cells,
            transcendentals=0,
        ),
    )(returned, *matrices)


def total_kernel(home_ref, away_ref, *refs):
    out_ref = refs[-1]
    held = out_ref.shape[1]
    for k in range(held):
        total = home_ref[0, :, k] + away_ref[0, :, k]
        for ref in refs[k:-1:held]:
            total += ref[:, 0]
        out_ref[:, k] = total


def on_device(columns, freq_blocks, causal_cutoffs, band_index, band_rates):
    shards, strips = lax.axis_size("freq"), lax.axis_size("cell")
    chips = strips // 2
    held = columns.shape[1]
    columns, blocks = in_hbm(columns), in_hbm(freq_blocks)
    spectrum, own_inner, own_outer, cutoff, rates = adjoint(
        columns, blocks, band_index, band_rates, causal_cutoffs, shards
    )
    gathered = lax.all_to_all(spectrum, "freq", split_axis=0, concat_axis=0, tiled=True)
    spectrum = middle(gathered, cutoff)
    spectrum, own_inner, own_outer, freq_blocks = lax.optimization_barrier(
        (spectrum, own_inner, own_outer, freq_blocks)
    )
    blocks = in_hbm(freq_blocks)
    returned = lax.all_to_all(spectrum, "freq", split_axis=0, concat_axis=0, tiled=True)
    swap = [(i, i ^ 1) for i in range(strips)]
    pairs = [(i, i + 1) for i in range(1, strips - 1, 2)]
    outer = lax.ppermute(own_outer, "cell", pairs + [(j, i) for i, j in pairs])
    inner = lax.ppermute(own_inner, "cell", swap)
    high, low, near = smooth(blocks, rates)
    near = near_edges(near, own_inner, own_outer, inner, outer, rates)
    matrices = (high, low, *near)
    leaving = []
    if chips > 1:
        for k in range(held):
            away, home = forward(returned, matrices, range(1, chips), chips, (k,))
            leaving.append(home + lax.ppermute(away, "cell", swap))
    arrived = []
    for s in range(1, chips):
        pairs = [(i, 2 * ((i // 2 + s) % chips) + i % 2) for i in range(strips)]
        for k in range(held):
            arrived.append(lax.ppermute(leaving[k][s - 1], "cell", pairs))
    away, home = forward(returned, matrices, range(1), chips, range(held))
    away = lax.ppermute(away, "cell", swap)
    share, sensors = home.shape[3:]
    return pl.pallas_call(
        total_kernel,
        in_specs=[VMEM_SPEC] * (2 + len(arrived)),
        out_specs=VMEM_SPEC,
        out_shape=jax.ShapeDtypeStruct((2, held, share, sensors), jnp.float32),
        compiler_params=grant(16),
        name="total",
    )(home, away, *arrived)


def solution(mesh):
    placed = (P(None, "freq", None, None), P(None, "freq", None, "cell"), P(), P("cell"), P())
    return jax.shard_map(
        on_device,
        mesh=mesh,
        in_specs=placed,
        out_specs=P(None, "freq", "cell", None),
        check_vma=False,
    )
```

```python
import functools
import math

import jax
import jax.numpy as jnp
import numpy as np
from jax import lax
from jax.experimental import pallas as pl
from jax.experimental.pallas import tpu as pltpu
from jax.sharding import PartitionSpec as P


SWEEPS = 4
BANDS = 8
ROWS = 8
LANES = 128
UNROLLED_FREQS = 32
GROUPS = LANES // SWEEPS
NEAR = 2 * ROWS


VMEM_SPEC = pl.BlockSpec(memory_space=pltpu.VMEM)
HBM_SPEC = pl.BlockSpec(memory_space=pltpu.HBM)


def grant(mib):
    return pltpu.CompilerParams(vmem_limit_bytes=mib * 2**20)


def in_hbm(x):
    return pltpu.with_memory_space_constraint(x, pltpu.HBM)


def split(x):
    high = x.astype(jnp.bfloat16)
    return high, (x - high.astype(jnp.float32)).astype(jnp.bfloat16)


def product(a, b, contract):
    return lax.dot_general(a, b, (contract, ((), ())), preferred_element_type=jnp.float32)


def inverse_table(steps, freqs):
    cycle = 2 * steps
    turns = np.outer(np.arange(steps), np.arange(freqs)) % cycle
    angle = turns * (2.0 * math.pi / cycle)
    weight = np.where((np.arange(freqs) == 0) | (np.arange(freqs) == freqs - 1), 1.0, 2.0) / cycle
    return weight * np.cos(angle), -weight * np.sin(angle)


def forward_table(steps, freqs):
    cycle = 2 * steps
    turns = np.outer(np.arange(freqs), np.arange(steps)) % cycle
    angle = turns * (2.0 * math.pi / cycle)
    return np.cos(angle), -np.sin(angle)


def rates_of(band_ref, rates_ref):
    band = band_ref[...]
    rates = jnp.zeros(band.shape, jnp.float32)
    for b in range(BANDS):
        rates = jnp.where(band == b, rates_ref[b], rates)
    return rates


def packed_of(sensors):
    return -(-sensors // (ROWS * GROUPS)) * ROWS


def adjoint_kernel(
    v_hbm, f_hbm, band_hbm, rates_hbm, cut_hbm, out_ref, inner_ref, outer_ref, cutoff_ref, spread_ref,
    v_ref, f_ref, band_ref, rates_ref, cut_ref, tail_v, tail_f, v_sem, f_sem, small_sem,
):
    shards, _, held, rows, cells = out_ref.shape
    cols, sensors = v_ref.shape[2:]
    copies = [pltpu.make_async_copy(f_hbm, f_ref, f_sem), pltpu.make_async_copy(v_hbm, v_ref, v_sem)]
    for copy in copies:
        copy.start()
    small = []
    for at, (source, target) in enumerate(((band_hbm, band_ref), (rates_hbm, rates_ref), (cut_hbm, cut_ref))):
        small.append(pltpu.make_async_copy(source, target, small_sem.at[at]))
        small[at].start()
    odd = lax.axis_index("cell") % 2
    last = cells - LANES
    inner_at, inner_shift = pl.multiple_of((1 - odd) * last, LANES), (1 - odd) * SWEEPS
    outer_at, outer_shift = pl.multiple_of(odd * last, LANES), odd * SWEEPS
    lane_group = lax.broadcasted_iota(jnp.int32, (ROWS, LANES), 1) // SWEEPS
    packed_rows = packed_of(sensors)

    def edge(at, block):
        for ref, lanes, shift in ((inner_ref, inner_at, inner_shift), (outer_ref, outer_at, outer_shift)):
            for first in range(0, sensors, ROWS * GROUPS):
                packed = jnp.zeros((ROWS, LANES), jnp.float32)
                for group in range(min(GROUPS, (sensors - first) // ROWS)):
                    rows_at = first + group * ROWS
                    cells_there = block[rows_at : rows_at + ROWS, pl.ds(lanes, LANES)]
                    moved = pltpu.roll(cells_there, group * SWEEPS + shift, 1)
                    packed = jnp.where(lane_group == group, moved, packed)
                place = at * packed_rows + first // GROUPS
                ref[place : place + ROWS] = packed

    tail_v[...] = jnp.zeros_like(tail_v)
    tail_f[...] = jnp.zeros_like(tail_f)
    for copy in copies:
        copy.wait()
    for k in range(held):
        high, low = split(v_ref[:, k].reshape(2 * cols, sensors))
        parts = jnp.concatenate([high, low], axis=0)
        body = sensors // (2 * LANES) * (2 * LANES)
        rest = sensors - body
        tail_v[: 4 * cols, :rest] = parts[:, body:]
        tail_v[: 2 * cols, LANES : LANES + rest] = high[:, body:]
        sums = []
        for c in range(2):
            f_high, f_low = split(f_ref[c, k])
            tail_f[c, :rest] = f_high[body:]
            tail_f[c, LANES : LANES + rest] = f_low[body:]
            both = product(parts[:, :body], f_high[:body], ((1,), (0,)))
            both += product(tail_v[...], tail_f[c], ((1,), (0,)))
            both = both[: 2 * cols] + both[2 * cols :] + product(high[:, :body], f_low[:body], ((1,), (0,)))
            sums.append(both)
        re = sums[0][:cols] + sums[1][cols:]
        im = sums[0][cols:] - sums[1][:cols]
        out_ref[:, 0, k] = re.reshape(shards, rows, cells)
        out_ref[:, 1, k] = im.reshape(shards, rows, cells)
        for c in range(2):
            edge(c * held + k, f_ref.at[c, k])
    for copy in small:
        copy.wait()
    rates = rates_of(band_ref, rates_ref)
    spread_ref[...] = jnp.broadcast_to(rates, spread_ref.shape)
    for ref, at in ((inner_ref, 1 - odd), (outer_ref, odd)):
        facing = jnp.where(at == 0, rates[:, :LANES], rates[:, last:])
        ref[2 * held * packed_rows :] = jnp.broadcast_to(facing, (ROWS, LANES))
    base = lax.axis_index("freq") * rows
    row = lax.broadcasted_iota(jnp.int32, (rows, LANES), 0)
    cutoff = jnp.zeros((rows, LANES), jnp.int32)
    for r in range(rows):
        cutoff = jnp.where(row == r, cut_ref[base + r], cutoff)
    cutoff_ref[...] = cutoff


def adjoint(columns, blocks, band_index, band_rates, causal_cutoffs, shards):
    _, held, cols, sensors = columns.shape
    cells = blocks.shape[3]
    out = (shards, 2, held, cols // shards, cells)
    edge = jax.ShapeDtypeStruct((2 * held * packed_of(sensors) + ROWS, LANES), jnp.float32)
    return pl.pallas_call(
        adjoint_kernel,
        in_specs=[HBM_SPEC] * 5,
        out_specs=[VMEM_SPEC] * 5,
        out_shape=[
            jax.ShapeDtypeStruct(out, jnp.float32),
            edge,
            edge,
            jax.ShapeDtypeStruct((cols // shards, LANES), jnp.int32),
            jax.ShapeDtypeStruct((ROWS, cells), jnp.float32),
        ],
        scratch_shapes=[
            pltpu.VMEM(columns.shape, jnp.float32),
            pltpu.VMEM(blocks.shape, jnp.float32),
            pltpu.VMEM((1, cells), jnp.int32),
            pltpu.SMEM(band_rates.shape, jnp.float32),
            pltpu.SMEM(causal_cutoffs.shape, jnp.int32),
            pltpu.VMEM((4 * cols, 2 * LANES), jnp.bfloat16),
            pltpu.VMEM((2, 2 * LANES, cells), jnp.bfloat16),
            pltpu.SemaphoreType.DMA,
            pltpu.SemaphoreType.DMA,
            pltpu.SemaphoreType.DMA((3,)),
        ],
        compiler_params=grant(16),
        cost_estimate=pl.CostEstimate(
            flops=24 * held * cols * sensors * cells, bytes_accessed=8 * held * sensors * cells, transcendentals=0
        ),
        name="adjoint",
    )(columns, blocks, in_hbm(band_index.reshape(1, cells)), in_hbm(band_rates), in_hbm(causal_cutoffs))


def middle_kernel(x_ref, cutoff_ref, out_hbm, out_ref, out_sem):
    shards, _, held, _, cells = x_ref.shape
    freqs = shards * held
    steps = freqs - 1
    half = freqs // 2
    to_cos, to_sin = inverse_table(steps, freqs)
    from_cos, from_sin = forward_table(steps, freqs)
    cutoff = cutoff_ref[...]
    copies = []
    for lane in range(0, cells, LANES):
        at = pl.ds(lane, LANES)
        even, odd = [], []
        for k in range(half):
            a, b = divmod(k, held)
            c, d = divmod(freqs - 1 - k, held)
            re, im = x_ref[a, 0, b, :, at], x_ref[a, 1, b, :, at]
            re2, im2 = x_ref[c, 0, d, :, at], x_ref[c, 1, d, :, at]
            even += [re + re2, im - im2]
            odd += [re - re2, im + im2]
        series = []
        for t in range(steps):
            total = None
            for k in range(half):
                pair = odd if t % 2 else even
                for value, table in ((pair[2 * k], to_cos), (pair[2 * k + 1], to_sin)):
                    term = value * float(table[t, k])
                    total = term if total is None else total + term
            series.append(jnp.where(cutoff > t, total, 0.0))
        for k in range(half):
            a, b = divmod(k, held)
            c, d = divmod(freqs - 1 - k, held)
            sums = []
            for table in (from_cos, from_sin):
                for parity in (0, 1):
                    total = None
                    for t in range(parity, steps, 2):
                        term = series[t] * float(table[k, t])
                        total = term if total is None else total + term
                    sums.append(total)
            out_ref[a, 0, b, :, at] = sums[0] + sums[1]
            out_ref[c, 0, d, :, at] = sums[0] - sums[1]
            out_ref[a, 1, b, :, at] = sums[2] + sums[3]
            out_ref[c, 1, d, :, at] = sums[3] - sums[2]
        source, target = out_ref.at[:, :, :, :, at], out_hbm.at[:, :, :, :, at]
        copy = pltpu.make_async_copy(source, target, out_sem.at[lane // LANES])
        copies.append(copy)
        copy.start()
    for copy in copies:
        copy.wait()


def middle(gathered, cutoff):
    shards, _, held, rows, cells = gathered.shape
    freqs = shards * held
    steps = freqs - 1
    if freqs <= UNROLLED_FREQS and freqs % 2 == 0:
        return pl.pallas_call(
            middle_kernel,
            in_specs=[VMEM_SPEC, VMEM_SPEC],
            out_specs=HBM_SPEC,
            out_shape=pltpu.HBM(gathered.shape, jnp.float32),
            scratch_shapes=[
                pltpu.VMEM(gathered.shape, jnp.float32),
                pltpu.SemaphoreType.DMA((cells // LANES,)),
            ],
            compiler_params=grant(8),
            cost_estimate=pl.CostEstimate(
                flops=8 * freqs * steps * rows * cells, bytes_accessed=16 * freqs * rows * cells, transcendentals=0
            ),
            name="middle",
        )(gathered, cutoff)
    to_time = jnp.asarray(np.concatenate(inverse_table(steps, freqs), axis=1), jnp.float32)
    to_freq = jnp.asarray(np.concatenate(forward_table(steps, freqs), axis=0), jnp.float32)
    x = gathered.transpose(1, 0, 2, 3, 4).reshape(2 * freqs, rows * cells)
    series = jnp.dot(to_time, x, precision=lax.Precision.HIGHEST).reshape(steps, rows, cells)
    moment = lax.broadcasted_iota(jnp.int32, (steps, rows), 0)
    series = jnp.where((moment < cutoff[None, :, 0])[:, :, None], series, 0.0)
    x = jnp.dot(to_freq, series.reshape(steps, rows * cells), precision=lax.Precision.HIGHEST)
    return x.reshape(2, shards, held, rows, cells).transpose(1, 0, 2, 3, 4)


def diagonals_of(rates):
    width = rates.shape[1]
    diagonals = jnp.where(lax.broadcasted_iota(jnp.int32, (2 * ROWS, width), 0) == ROWS, 1.0, 0.0)
    for _ in range(SWEEPS):
        up = pltpu.roll(pltpu.roll(diagonals, 1, 1), 2 * ROWS - 1, 0)
        down = pltpu.roll(pltpu.roll(diagonals, width - 1, 1), 1, 0)
        diagonals = diagonals + rates * (up - 2.0 * diagonals + down)
    return diagonals


def spread(diagonals, offset):
    tile = jnp.zeros(offset.shape, jnp.float32)
    for o in range(-SWEEPS, SWEEPS + 1):
        tile = jnp.where(offset == o, diagonals[ROWS + o : ROWS + o + 1], tile)
    return tile


def smooth_kernel(f_hbm, rates_ref, high_ref, low_ref, near_ref, f_ref, a_both, f_sem):
    _, held, _, cells = f_hbm.shape
    copies = []
    for at in range(2 * held):
        c, k = divmod(at, held)
        copies.append(pltpu.make_async_copy(f_hbm.at[c, k], f_ref.at[c, k], f_sem.at[at]))
        copies[at].start()
    diagonals = diagonals_of(jnp.concatenate([rates_ref[:1], jnp.zeros((1, LANES), jnp.float32)], axis=1))
    for lanes in range(0, cells, LANES):
        column = lax.broadcasted_iota(jnp.int32, (LANES, LANES), 1)
        row = lax.broadcasted_iota(jnp.int32, (LANES, LANES), 0)
        for rows in range(0, cells, LANES):
            high, low = split(spread(diagonals[:, lanes : lanes + LANES], row - column + (rows - lanes)))
            a_both[rows : rows + LANES, lanes : lanes + LANES] = high
            a_both[cells + rows : cells + rows + LANES, lanes : lanes + LANES] = low
    for at in range(2 * held):
        c, k = divmod(at, held)
        copies[at].wait()
        high, low = split(f_ref[c, k])
        both = product(a_both[...], high, ((1,), (1,)))
        total = both[:cells] + both[cells:] + product(a_both[:cells], low, ((1,), (1,)))
        high, low = split(total)
        high_ref[c, k] = high
        low_ref[c, k] = low
        near_ref[c, k, :NEAR] = total[:NEAR]
        near_ref[c, k, NEAR:] = total[cells - NEAR :]


def smooth(blocks, rates):
    _, held, sensors, cells = blocks.shape
    shape = jax.ShapeDtypeStruct((2, held, cells, sensors), jnp.bfloat16)
    return pl.pallas_call(
        smooth_kernel,
        in_specs=[HBM_SPEC, VMEM_SPEC],
        out_specs=[VMEM_SPEC] * 3,
        out_shape=[shape, shape, jax.ShapeDtypeStruct((2, held, 2 * NEAR, sensors), jnp.float32)],
        scratch_shapes=[
            pltpu.VMEM(blocks.shape, jnp.float32),
            pltpu.VMEM((2 * cells, cells), jnp.bfloat16),
            pltpu.SemaphoreType.DMA((2 * held,)),
        ],
        compiler_params=grant(16),
        cost_estimate=pl.CostEstimate(
            flops=12 * held * sensors * cells * cells, bytes_accessed=16 * held * sensors * cells, transcendentals=0
        ),
        name="smooth",
    )(blocks, rates)


def near_kernel(
    near_ref, own_inner_ref, own_outer_ref, inner_ref, outer_ref, rates_ref, high_ref, low_ref, sides
):
    held = near_ref.shape[1]
    sensors = near_ref.shape[3]
    cells = rates_ref.shape[1]
    even = lax.axis_index("cell") % 2 == 0
    kinds = 4
    per = kinds * SWEEPS
    pairs = LANES // (2 * per)

    def parts(first):
        rows = slice(first, first + ROWS)
        own_inner, own_outer = own_inner_ref[rows], own_outer_ref[rows]
        inner, outer = inner_ref[rows], outer_ref[rows]
        return (
            jnp.where(even, own_outer, own_inner),
            jnp.where(even, own_inner, own_outer),
            jnp.where(even, inner, outer),
            jnp.where(even, outer, inner),
        )

    lane = lax.broadcasted_iota(jnp.int32, (ROWS, LANES), 1)
    packed_rows = packed_of(sensors)
    _, _, after, before = parts(2 * held * packed_rows)
    side = jnp.where(lane < SWEEPS, after, jnp.where(lane >= LANES - SWEEPS, before, 0.0))[:1]
    own = rates_ref[:1]
    alone = diagonals_of(jnp.concatenate([own, jnp.zeros((1, LANES), jnp.float32)], axis=1))
    full = diagonals_of(jnp.concatenate([own, side], axis=1))
    first = full[:, :LANES] - alone[:, :LANES]
    last = full[:, cells - LANES : cells] - alone[:, cells - LANES : cells]
    beyond = full[:, cells:]
    kind = lax.broadcasted_iota(jnp.int32, (2 * ROWS, LANES), 1) // SWEEPS
    change = jnp.where(kind == 0, first, 0.0)
    change = jnp.where(kind == 1, pltpu.roll(last, 2 * SWEEPS, 1), change)
    change = jnp.where(kind == 2, pltpu.roll(beyond, 2 * SWEEPS, 1), change)
    change = jnp.where(kind == 3, pltpu.roll(beyond, 4 * SWEEPS, 1), change)
    for shift in (per, 2 * per, 4 * per):
        change = change + pltpu.roll(change, shift, 1)
    row = lax.broadcasted_iota(jnp.int32, (2 * NEAR, LANES), 0)
    column = lax.broadcasted_iota(jnp.int32, (2 * NEAR, LANES), 1)
    kind, i = (column // SWEEPS) % kinds, column % SWEEPS
    at_first = jnp.where(kind == 0, row - i, jnp.where(kind == 3, row + SWEEPS - i, LANES))
    end = row - 2 * NEAR
    at_last = jnp.where(kind == 1, end + SWEEPS - i, jnp.where(kind == 2, end - i, LANES))
    matrix = spread(change, jnp.where(row < NEAR, at_first, at_last))
    a_high, a_low = split(matrix)
    owner = column // per
    cell_of = lane // SWEEPS
    for begin_at in range(0, 2 * held, pairs):
        ats = range(begin_at, min(2 * held, begin_at + pairs))
        for begin in range(0, sensors, ROWS * GROUPS):
            values = [value for at in ats for value in parts(at * packed_rows + begin // GROUPS)]
            values = [pltpu.roll(value, n * SWEEPS, 1) if n else value for n, value in enumerate(values)]
            for group in range(min(GROUPS, (sensors - begin) // ROWS)):
                tile = jnp.zeros((ROWS, LANES), jnp.float32)
                for n, value in enumerate(values):
                    tile = jnp.where(cell_of == (group + n) % GROUPS, value, tile)
                tile = pltpu.roll(tile, (LANES - group * SWEEPS) % LANES, 1)
                rows_at = begin + group * ROWS
                sides[rows_at : rows_at + ROWS] = tile + pltpu.roll(tile, LANES // 2, 1)
        high, low = split(sides[...])
        low_lane = lax.broadcasted_iota(jnp.int32, (sensors, LANES), 1) >= LANES // 2
        operand = jnp.where(low_lane, low.astype(jnp.float32), high.astype(jnp.float32)).astype(jnp.bfloat16)
        left = []
        for p in range(len(ats)):
            left.append(jnp.where(owner % pairs == p, a_high.astype(jnp.float32), 0.0))
            left.append(jnp.where(owner == p, a_low.astype(jnp.float32), 0.0))
        left = jnp.concatenate(left, axis=0).astype(jnp.bfloat16)
        terms = product(left, operand, ((1,), (1,)))
        for p, at in enumerate(ats):
            c, k = divmod(at, held)
            mine = terms[4 * NEAR * p : 4 * NEAR * (p + 1)]
            high, low = split(near_ref[c, k] + mine[: 2 * NEAR] + mine[2 * NEAR :])
            high_ref[c, k] = high
            low_ref[c, k] = low


def near_edges(near, own_inner, own_outer, inner, outer, rates):
    shape = jax.ShapeDtypeStruct(near.shape, jnp.bfloat16)
    held, sensors = near.shape[1], near.shape[3]
    return pl.pallas_call(
        near_kernel,
        in_specs=[VMEM_SPEC] * 6,
        out_specs=[VMEM_SPEC] * 2,
        out_shape=[shape, shape],
        scratch_shapes=[pltpu.VMEM((sensors, LANES), jnp.float32)],
        compiler_params=grant(8),
        cost_estimate=pl.CostEstimate(
            flops=24 * held * sensors * NEAR * LANES, bytes_accessed=8 * near.size, transcendentals=0
        ),
        name="near_edges",
    )(near, own_inner, own_outer, inner, outer, rates)


def forward_kernel(
    steps, chips, wanted, x_ref, high_ref, low_ref, near_high_ref, near_low_ref, away_ref, home_ref
):
    share, sensors = home_ref.shape[3:]
    per = share // ROWS
    cell = lax.axis_index("cell")
    chip, core = cell // 2, cell % 2
    cells = x_ref.shape[4]
    order = []
    for side in (1 - core, core):
        for s in steps:
            order.append((2 * lax.rem(chip + s, chips) + side) * per)
    rows = len(order) * share

    def whole(ref, near, c, k):
        inside = ref[c, k, NEAR : cells - NEAR]
        return jnp.concatenate([near[c, k, :NEAR], inside, near[c, k, NEAR:]], axis=0)

    for at, k in enumerate(wanted):
        parts = []
        for c in range(2):
            for first in order:
                parts.append(x_ref[pl.ds(first, per), c, k].reshape(share, cells))
        high, low = split(jnp.concatenate(parts, axis=0))
        both = jnp.concatenate([high, low], axis=0)
        terms = []
        for c in range(2):
            wide = product(both, whole(high_ref, near_high_ref, c, k), ((1,), (0,)))
            small = product(high, whole(low_ref, near_low_ref, c, k), ((1,), (0,)))
            terms.append(wide[: 2 * rows] + wide[2 * rows :] + small)
        re = (terms[0][:rows] - terms[1][rows:]).reshape(2, len(steps), share, sensors)
        im = (terms[0][rows:] + terms[1][:rows]).reshape(2, len(steps), share, sensors)
        for side, ref in enumerate((away_ref, home_ref)):
            ref[:, 0, at] = re[side]
            ref[:, 1, at] = im[side]


def forward(returned, matrices, steps, chips, wanted):
    shards, _, _, rows, cells = returned.shape
    sensors = matrices[0].shape[3]
    share = shards * rows // (2 * chips)
    shape = jax.ShapeDtypeStruct((len(steps), 2, len(wanted), share, sensors), jnp.float32)
    return pl.pallas_call(
        functools.partial(forward_kernel, steps, chips, wanted),
        in_specs=[VMEM_SPEC] * 5,
        out_specs=[VMEM_SPEC] * 2,
        out_shape=[shape, shape],
        compiler_params=grant(16),
        cost_estimate=pl.CostEstimate(
            flops=48 * len(steps) * len(wanted) * share * sensors * cells,
            bytes_accessed=8 * len(wanted) * sensors * cells,
            transcendentals=0,
        ),
    )(returned, *matrices)


def total_kernel(home_ref, away_ref, *refs):
    out_ref = refs[-1]
    held = out_ref.shape[1]
    for k in range(held):
        total = home_ref[0, :, k] + away_ref[0, :, k]
        for ref in refs[k:-1:held]:
            total += ref[:, 0]
        out_ref[:, k] = total


def on_device(columns, freq_blocks, causal_cutoffs, band_index, band_rates):
    shards, strips = lax.axis_size("freq"), lax.axis_size("cell")
    chips = strips // 2
    held = columns.shape[1]
    columns, blocks = in_hbm(columns), in_hbm(freq_blocks)
    spectrum, own_inner, own_outer, cutoff, rates = adjoint(
        columns, blocks, band_index, band_rates, causal_cutoffs, shards
    )
    gathered = lax.all_to_all(spectrum, "freq", split_axis=0, concat_axis=0, tiled=True)
    spectrum = middle(gathered, cutoff)
    spectrum, own_inner, own_outer, freq_blocks = lax.optimization_barrier(
        (spectrum, own_inner, own_outer, freq_blocks)
    )
    blocks = in_hbm(freq_blocks)
    returned = lax.all_to_all(spectrum, "freq", split_axis=0, concat_axis=0, tiled=True)
    swap = [(i, i ^ 1) for i in range(strips)]
    pairs = [(i, i + 1) for i in range(1, strips - 1, 2)]
    outer = lax.ppermute(own_outer, "cell", pairs + [(j, i) for i, j in pairs])
    inner = lax.ppermute(own_inner, "cell", swap)
    high, low, near = smooth(blocks, rates)
    near = near_edges(near, own_inner, own_outer, inner, outer, rates)
    matrices = (high, low, *near)
    leaving = []
    if chips > 1:
        for k in range(held):
            away, home = forward(returned, matrices, range(1, chips), chips, (k,))
            leaving.append(home + lax.ppermute(away, "cell", swap))
    arrived = []
    for s in range(1, chips):
        pairs = [(i, 2 * ((i // 2 + s) % chips) + i % 2) for i in range(strips)]
        for k in range(held):
            arrived.append(lax.ppermute(leaving[k][s - 1], "cell", pairs))
    away, home = forward(returned, matrices, range(1), chips, range(held))
    away = lax.ppermute(away, "cell", swap)
    share, sensors = home.shape[3:]
    return pl.pallas_call(
        total_kernel,
        in_specs=[VMEM_SPEC] * (2 + len(arrived)),
        out_specs=VMEM_SPEC,
        out_shape=jax.ShapeDtypeStruct((2, held, share, sensors), jnp.float32),
        compiler_params=grant(16),
        name="total",
    )(home, away, *arrived)


def solution(mesh):
    placed = (P(None, "freq", None, None), P(None, "freq", None, "cell"), P(), P("cell"), P())
    return jax.shard_map(
        on_device,
        mesh=mesh,
        in_specs=placed,
        out_specs=P(None, "freq", "cell", None),
        check_vma=False,
    )
```

```python
import functools
import math

import jax
import jax.numpy as jnp
import numpy as np
from jax import lax
from jax.experimental import pallas as pl
from jax.experimental.pallas import tpu as pltpu
from jax.sharding import PartitionSpec as P


SWEEPS = 4
BANDS = 8
ROWS = 8
LANES = 128
UNROLLED_FREQS = 32
GROUPS = LANES // SWEEPS
NEAR = 2 * ROWS


VMEM_SPEC = pl.BlockSpec(memory_space=pltpu.VMEM)
HBM_SPEC = pl.BlockSpec(memory_space=pltpu.HBM)


def grant(mib):
    return pltpu.CompilerParams(vmem_limit_bytes=mib * 2**20)


def in_hbm(x):
    return pltpu.with_memory_space_constraint(x, pltpu.HBM)


def split(x):
    high = x.astype(jnp.bfloat16)
    return high, (x - high.astype(jnp.float32)).astype(jnp.bfloat16)


def product(a, b, contract):
    return lax.dot_general(a, b, (contract, ((), ())), preferred_element_type=jnp.float32)


def inverse_table(steps, freqs):
    cycle = 2 * steps
    turns = np.outer(np.arange(steps), np.arange(freqs)) % cycle
    angle = turns * (2.0 * math.pi / cycle)
    weight = np.where((np.arange(freqs) == 0) | (np.arange(freqs) == freqs - 1), 1.0, 2.0) / cycle
    return weight * np.cos(angle), -weight * np.sin(angle)


def forward_table(steps, freqs):
    cycle = 2 * steps
    turns = np.outer(np.arange(freqs), np.arange(steps)) % cycle
    angle = turns * (2.0 * math.pi / cycle)
    return np.cos(angle), -np.sin(angle)


def rates_of(band_ref, rates_ref):
    band = band_ref[...]
    rates = jnp.zeros(band.shape, jnp.float32)
    for b in range(BANDS):
        rates = jnp.where(band == b, rates_ref[b], rates)
    return rates


def packed_of(sensors):
    return -(-sensors // (ROWS * GROUPS)) * ROWS


def adjoint_kernel(
    v_hbm, f_hbm, band_hbm, rates_hbm, cut_hbm, out_ref, inner_ref, outer_ref, cutoff_ref, spread_ref,
    v_ref, f_ref, band_ref, rates_ref, cut_ref, tail_v, tail_f, v_sem, f_sem, small_sem,
):
    shards, _, held, rows, cells = out_ref.shape
    cols, sensors = v_ref.shape[2:]
    copies = [pltpu.make_async_copy(f_hbm, f_ref, f_sem), pltpu.make_async_copy(v_hbm, v_ref, v_sem)]
    for copy in copies:
        copy.start()
    small = []
    for at, (source, target) in enumerate(((band_hbm, band_ref), (rates_hbm, rates_ref), (cut_hbm, cut_ref))):
        small.append(pltpu.make_async_copy(source, target, small_sem.at[at]))
        small[at].start()
    odd = lax.axis_index("cell") % 2
    last = cells - LANES
    inner_at, inner_shift = pl.multiple_of((1 - odd) * last, LANES), (1 - odd) * SWEEPS
    outer_at, outer_shift = pl.multiple_of(odd * last, LANES), odd * SWEEPS
    lane_group = lax.broadcasted_iota(jnp.int32, (ROWS, LANES), 1) // SWEEPS
    packed_rows = packed_of(sensors)

    def edge(at, block):
        for ref, lanes, shift in ((inner_ref, inner_at, inner_shift), (outer_ref, outer_at, outer_shift)):
            for first in range(0, sensors, ROWS * GROUPS):
                packed = jnp.zeros((ROWS, LANES), jnp.float32)
                for group in range(min(GROUPS, (sensors - first) // ROWS)):
                    rows_at = first + group * ROWS
                    cells_there = block[rows_at : rows_at + ROWS, pl.ds(lanes, LANES)]
                    moved = pltpu.roll(cells_there, group * SWEEPS + shift, 1)
                    packed = jnp.where(lane_group == group, moved, packed)
                place = at * packed_rows + first // GROUPS
                ref[place : place + ROWS] = packed

    tail_v[...] = jnp.zeros_like(tail_v)
    tail_f[...] = jnp.zeros_like(tail_f)
    for copy in copies:
        copy.wait()
    for k in range(held):
        high, low = split(v_ref[:, k].reshape(2 * cols, sensors))
        parts = jnp.concatenate([high, low], axis=0)
        body = sensors // (2 * LANES) * (2 * LANES)
        rest = sensors - body
        tail_v[: 4 * cols, :rest] = parts[:, body:]
        tail_v[: 2 * cols, LANES : LANES + rest] = high[:, body:]
        sums = []
        for c in range(2):
            f_high, f_low = split(f_ref[c, k])
            tail_f[c, :rest] = f_high[body:]
            tail_f[c, LANES : LANES + rest] = f_low[body:]
            both = product(parts[:, :body], f_high[:body], ((1,), (0,)))
            both += product(tail_v[...], tail_f[c], ((1,), (0,)))
            both = both[: 2 * cols] + both[2 * cols :] + product(high[:, :body], f_low[:body], ((1,), (0,)))
            sums.append(both)
        re = sums[0][:cols] + sums[1][cols:]
        im = sums[0][cols:] - sums[1][:cols]
        out_ref[:, 0, k] = re.reshape(shards, rows, cells)
        out_ref[:, 1, k] = im.reshape(shards, rows, cells)
        for c in range(2):
            edge(c * held + k, f_ref.at[c, k])
    for copy in small:
        copy.wait()
    rates = rates_of(band_ref, rates_ref)
    spread_ref[...] = jnp.broadcast_to(rates, spread_ref.shape)
    for ref, at in ((inner_ref, 1 - odd), (outer_ref, odd)):
        facing = jnp.where(at == 0, rates[:, :LANES], rates[:, last:])
        ref[2 * held * packed_rows :] = jnp.broadcast_to(facing, (ROWS, LANES))
    base = lax.axis_index("freq") * rows
    row = lax.broadcasted_iota(jnp.int32, (rows, LANES), 0)
    cutoff = jnp.zeros((rows, LANES), jnp.int32)
    for r in range(rows):
        cutoff = jnp.where(row == r, cut_ref[base + r], cutoff)
    cutoff_ref[...] = cutoff


def adjoint(columns, blocks, band_index, band_rates, causal_cutoffs, shards):
    _, held, cols, sensors = columns.shape
    cells = blocks.shape[3]
    out = (shards, 2, held, cols // shards, cells)
    edge = jax.ShapeDtypeStruct((2 * held * packed_of(sensors) + ROWS, LANES), jnp.float32)
    return pl.pallas_call(
        adjoint_kernel,
        in_specs=[HBM_SPEC] * 5,
        out_specs=[VMEM_SPEC] * 5,
        out_shape=[
            jax.ShapeDtypeStruct(out, jnp.float32),
            edge,
            edge,
            jax.ShapeDtypeStruct((cols // shards, LANES), jnp.int32),
            jax.ShapeDtypeStruct((ROWS, cells), jnp.float32),
        ],
        scratch_shapes=[
            pltpu.VMEM(columns.shape, jnp.float32),
            pltpu.VMEM(blocks.shape, jnp.float32),
            pltpu.VMEM((1, cells), jnp.int32),
            pltpu.SMEM(band_rates.shape, jnp.float32),
            pltpu.SMEM(causal_cutoffs.shape, jnp.int32),
            pltpu.VMEM((4 * cols, 2 * LANES), jnp.bfloat16),
            pltpu.VMEM((2, 2 * LANES, cells), jnp.bfloat16),
            pltpu.SemaphoreType.DMA,
            pltpu.SemaphoreType.DMA,
            pltpu.SemaphoreType.DMA((3,)),
        ],
        compiler_params=grant(16),
        cost_estimate=pl.CostEstimate(
            flops=24 * held * cols * sensors * cells, bytes_accessed=8 * held * sensors * cells, transcendentals=0
        ),
        name="adjoint",
    )(columns, blocks, in_hbm(band_index.reshape(1, cells)), in_hbm(band_rates), in_hbm(causal_cutoffs))


def middle_kernel(x_ref, cutoff_ref, out_hbm, out_ref, out_sem):
    shards, _, held, _, cells = x_ref.shape
    freqs = shards * held
    steps = freqs - 1
    half = freqs // 2
    to_cos, to_sin = inverse_table(steps, freqs)
    from_cos, from_sin = forward_table(steps, freqs)
    cutoff = cutoff_ref[...]
    copies = []
    for lane in range(0, cells, LANES):
        at = pl.ds(lane, LANES)
        even, odd = [], []
        for k in range(half):
            a, b = divmod(k, held)
            c, d = divmod(freqs - 1 - k, held)
            re, im = x_ref[a, 0, b, :, at], x_ref[a, 1, b, :, at]
            re2, im2 = x_ref[c, 0, d, :, at], x_ref[c, 1, d, :, at]
            even += [re + re2, im - im2]
            odd += [re - re2, im + im2]
        series = []
        for t in range(steps):
            total = None
            for k in range(half):
                pair = odd if t % 2 else even
                for value, table in ((pair[2 * k], to_cos), (pair[2 * k + 1], to_sin)):
                    term = value * float(table[t, k])
                    total = term if total is None else total + term
            series.append(jnp.where(cutoff > t, total, 0.0))
        for k in range(half):
            a, b = divmod(k, held)
            c, d = divmod(freqs - 1 - k, held)
            sums = []
            for table in (from_cos, from_sin):
                for parity in (0, 1):
                    total = None
                    for t in range(parity, steps, 2):
                        term = series[t] * float(table[k, t])
                        total = term if total is None else total + term
                    sums.append(total)
            out_ref[a, 0, b, :, at] = sums[0] + sums[1]
            out_ref[c, 0, d, :, at] = sums[0] - sums[1]
            out_ref[a, 1, b, :, at] = sums[2] + sums[3]
            out_ref[c, 1, d, :, at] = sums[3] - sums[2]
        source, target = out_ref.at[:, :, :, :, at], out_hbm.at[:, :, :, :, at]
        copy = pltpu.make_async_copy(source, target, out_sem.at[lane // LANES])
        copies.append(copy)
        copy.start()
    for copy in copies:
        copy.wait()


def middle(gathered, cutoff):
    shards, _, held, rows, cells = gathered.shape
    freqs = shards * held
    steps = freqs - 1
    if freqs <= UNROLLED_FREQS and freqs % 2 == 0:
        return pl.pallas_call(
            middle_kernel,
            in_specs=[VMEM_SPEC, VMEM_SPEC],
            out_specs=HBM_SPEC,
            out_shape=pltpu.HBM(gathered.shape, jnp.float32),
            scratch_shapes=[
                pltpu.VMEM(gathered.shape, jnp.float32),
                pltpu.SemaphoreType.DMA((cells // LANES,)),
            ],
            compiler_params=grant(8),
            cost_estimate=pl.CostEstimate(
                flops=8 * freqs * steps * rows * cells, bytes_accessed=16 * freqs * rows * cells, transcendentals=0
            ),
            name="middle",
        )(gathered, cutoff)
    to_time = jnp.asarray(np.concatenate(inverse_table(steps, freqs), axis=1), jnp.float32)
    to_freq = jnp.asarray(np.concatenate(forward_table(steps, freqs), axis=0), jnp.float32)
    x = gathered.transpose(1, 0, 2, 3, 4).reshape(2 * freqs, rows * cells)
    series = jnp.dot(to_time, x, precision=lax.Precision.HIGHEST).reshape(steps, rows, cells)
    moment = lax.broadcasted_iota(jnp.int32, (steps, rows), 0)
    series = jnp.where((moment < cutoff[None, :, 0])[:, :, None], series, 0.0)
    x = jnp.dot(to_freq, series.reshape(steps, rows * cells), precision=lax.Precision.HIGHEST)
    return x.reshape(2, shards, held, rows, cells).transpose(1, 0, 2, 3, 4)


def diagonals_of(rates):
    width = rates.shape[1]
    diagonals = jnp.where(lax.broadcasted_iota(jnp.int32, (2 * ROWS, width), 0) == ROWS, 1.0, 0.0)
    for _ in range(SWEEPS):
        up = pltpu.roll(pltpu.roll(diagonals, 1, 1), 2 * ROWS - 1, 0)
        down = pltpu.roll(pltpu.roll(diagonals, width - 1, 1), 1, 0)
        diagonals = diagonals + rates * (up - 2.0 * diagonals + down)
    return diagonals


def spread(diagonals, offset):
    tile = jnp.zeros(offset.shape, jnp.float32)
    for o in range(-SWEEPS, SWEEPS + 1):
        tile = jnp.where(offset == o, diagonals[ROWS + o : ROWS + o + 1], tile)
    return tile


def smooth_kernel(f_hbm, rates_ref, high_ref, low_ref, near_ref, f_ref, a_both, f_sem):
    _, held, _, cells = f_hbm.shape
    copies = []
    for at in range(2 * held):
        c, k = divmod(at, held)
        copies.append(pltpu.make_async_copy(f_hbm.at[c, k], f_ref.at[c, k], f_sem.at[at]))
        copies[at].start()
    diagonals = diagonals_of(jnp.concatenate([rates_ref[:1], jnp.zeros((1, LANES), jnp.float32)], axis=1))
    for lanes in range(0, cells, LANES):
        column = lax.broadcasted_iota(jnp.int32, (LANES, LANES), 1)
        row = lax.broadcasted_iota(jnp.int32, (LANES, LANES), 0)
        for rows in range(0, cells, LANES):
            high, low = split(spread(diagonals[:, lanes : lanes + LANES], row - column + (rows - lanes)))
            a_both[rows : rows + LANES, lanes : lanes + LANES] = high
            a_both[cells + rows : cells + rows + LANES, lanes : lanes + LANES] = low
    for at in range(2 * held):
        c, k = divmod(at, held)
        copies[at].wait()
        high, low = split(f_ref[c, k])
        both = product(a_both[...], high, ((1,), (1,)))
        total = both[:cells] + both[cells:] + product(a_both[:cells], low, ((1,), (1,)))
        high, low = split(total)
        high_ref[c, k] = high
        low_ref[c, k] = low
        near_ref[c, k, :NEAR] = total[:NEAR]
        near_ref[c, k, NEAR:] = total[cells - NEAR :]


def smooth(blocks, rates):
    _, held, sensors, cells = blocks.shape
    shape = jax.ShapeDtypeStruct((2, held, cells, sensors), jnp.bfloat16)
    return pl.pallas_call(
        smooth_kernel,
        in_specs=[HBM_SPEC, VMEM_SPEC],
        out_specs=[VMEM_SPEC] * 3,
        out_shape=[shape, shape, jax.ShapeDtypeStruct((2, held, 2 * NEAR, sensors), jnp.float32)],
        scratch_shapes=[
            pltpu.VMEM(blocks.shape, jnp.float32),
            pltpu.VMEM((2 * cells, cells), jnp.bfloat16),
            pltpu.SemaphoreType.DMA((2 * held,)),
        ],
        compiler_params=grant(16),
        cost_estimate=pl.CostEstimate(
            flops=12 * held * sensors * cells * cells, bytes_accessed=16 * held * sensors * cells, transcendentals=0
        ),
        name="smooth",
    )(blocks, rates)


def near_kernel(
    near_ref, own_inner_ref, own_outer_ref, inner_ref, outer_ref, rates_ref, high_ref, low_ref, sides
):
    held = near_ref.shape[1]
    sensors = near_ref.shape[3]
    cells = rates_ref.shape[1]
    even = lax.axis_index("cell") % 2 == 0
    kinds = 4
    per = kinds * SWEEPS
    pairs = LANES // (2 * per)

    def parts(first):
        rows = slice(first, first + ROWS)
        own_inner, own_outer = own_inner_ref[rows], own_outer_ref[rows]
        inner, outer = inner_ref[rows], outer_ref[rows]
        return (
            jnp.where(even, own_outer, own_inner),
            jnp.where(even, own_inner, own_outer),
            jnp.where(even, inner, outer),
            jnp.where(even, outer, inner),
        )

    lane = lax.broadcasted_iota(jnp.int32, (ROWS, LANES), 1)
    packed_rows = packed_of(sensors)
    _, _, after, before = parts(2 * held * packed_rows)
    side = jnp.where(lane < SWEEPS, after, jnp.where(lane >= LANES - SWEEPS, before, 0.0))[:1]
    own = rates_ref[:1]
    alone = diagonals_of(jnp.concatenate([own, jnp.zeros((1, LANES), jnp.float32)], axis=1))
    full = diagonals_of(jnp.concatenate([own, side], axis=1))
    first = full[:, :LANES] - alone[:, :LANES]
    last = full[:, cells - LANES : cells] - alone[:, cells - LANES : cells]
    beyond = full[:, cells:]
    kind = lax.broadcasted_iota(jnp.int32, (2 * ROWS, LANES), 1) // SWEEPS
    change = jnp.where(kind == 0, first, 0.0)
    change = jnp.where(kind == 1, pltpu.roll(last, 2 * SWEEPS, 1), change)
    change = jnp.where(kind == 2, pltpu.roll(beyond, 2 * SWEEPS, 1), change)
    change = jnp.where(kind == 3, pltpu.roll(beyond, 4 * SWEEPS, 1), change)
    for shift in (per, 2 * per, 4 * per):
        change = change + pltpu.roll(change, shift, 1)
    row = lax.broadcasted_iota(jnp.int32, (2 * NEAR, LANES), 0)
    column = lax.broadcasted_iota(jnp.int32, (2 * NEAR, LANES), 1)
    kind, i = (column // SWEEPS) % kinds, column % SWEEPS
    at_first = jnp.where(kind == 0, row - i, jnp.where(kind == 3, row + SWEEPS - i, LANES))
    end = row - 2 * NEAR
    at_last = jnp.where(kind == 1, end + SWEEPS - i, jnp.where(kind == 2, end - i, LANES))
    matrix = spread(change, jnp.where(row < NEAR, at_first, at_last))
    a_high, a_low = split(matrix)
    owner = column // per
    cell_of = lane // SWEEPS
    for begin_at in range(0, 2 * held, pairs):
        ats = range(begin_at, min(2 * held, begin_at + pairs))
        for begin in range(0, sensors, ROWS * GROUPS):
            values = [value for at in ats for value in parts(at * packed_rows + begin // GROUPS)]
            values = [pltpu.roll(value, n * SWEEPS, 1) if n else value for n, value in enumerate(values)]
            for group in range(min(GROUPS, (sensors - begin) // ROWS)):
                tile = jnp.zeros((ROWS, LANES), jnp.float32)
                for n, value in enumerate(values):
                    tile = jnp.where(cell_of == (group + n) % GROUPS, value, tile)
                tile = pltpu.roll(tile, (LANES - group * SWEEPS) % LANES, 1)
                rows_at = begin + group * ROWS
                sides[rows_at : rows_at + ROWS] = tile + pltpu.roll(tile, LANES // 2, 1)
        high, low = split(sides[...])
        low_lane = lax.broadcasted_iota(jnp.int32, (sensors, LANES), 1) >= LANES // 2
        operand = jnp.where(low_lane, low.astype(jnp.float32), high.astype(jnp.float32)).astype(jnp.bfloat16)
        left = []
        for p in range(len(ats)):
            left.append(jnp.where(owner % pairs == p, a_high.astype(jnp.float32), 0.0))
            left.append(jnp.where(owner == p, a_low.astype(jnp.float32), 0.0))
        left = jnp.concatenate(left, axis=0).astype(jnp.bfloat16)
        terms = product(left, operand, ((1,), (1,)))
        for p, at in enumerate(ats):
            c, k = divmod(at, held)
            mine = terms[4 * NEAR * p : 4 * NEAR * (p + 1)]
            high, low = split(near_ref[c, k] + mine[: 2 * NEAR] + mine[2 * NEAR :])
            high_ref[c, k] = high
            low_ref[c, k] = low


def near_edges(near, own_inner, own_outer, inner, outer, rates):
    shape = jax.ShapeDtypeStruct(near.shape, jnp.bfloat16)
    held, sensors = near.shape[1], near.shape[3]
    return pl.pallas_call(
        near_kernel,
        in_specs=[VMEM_SPEC] * 6,
        out_specs=[VMEM_SPEC] * 2,
        out_shape=[shape, shape],
        scratch_shapes=[pltpu.VMEM((sensors, LANES), jnp.float32)],
        compiler_params=grant(8),
        cost_estimate=pl.CostEstimate(
            flops=24 * held * sensors * NEAR * LANES, bytes_accessed=8 * near.size, transcendentals=0
        ),
        name="near_edges",
    )(near, own_inner, own_outer, inner, outer, rates)


def pack(ref, s, values, pad_ref):
    rows, sensors = values[0].shape
    tiles, rest = divmod(sensors, LANES)
    for p, value in enumerate(values):
        for t in range(tiles):
            place = (p * tiles + t) * rows
            ref[s, place : place + rows] = value[:, t * LANES : (t + 1) * LANES]
        pad_ref[p, :, :rest] = value[:, tiles * LANES :]
    lane = lax.broadcasted_iota(jnp.int32, (rows, LANES), 1)
    second = pltpu.roll(pad_ref[1], rest, 1)
    place = 2 * tiles * rows
    ref[s, place : place + rows] = jnp.where(lane < rest, pad_ref[0], second)
    half = rows // 2
    moved = pltpu.roll(second, LANES // 2, 1)
    ref[s, place + rows :] = jnp.where(lane[:half] < LANES // 2, second[:half], moved[half:])


def unpack(ref, rows, sensors):
    tiles, rest = divmod(sensors, LANES)
    parts = []
    place = 2 * tiles * rows
    lane = lax.broadcasted_iota(jnp.int32, (rows, LANES), 1)
    first, last = ref[place : place + rows], ref[place + rows :]
    second = jnp.concatenate([last, pltpu.roll(last, LANES // 2, 1)], axis=0)
    second = pltpu.roll(jnp.where(lane < rest, second, first), LANES - rest, 1)
    for p, tail in enumerate((first, second)):
        tile = [ref[(p * tiles + t) * rows : (p * tiles + t + 1) * rows] for t in range(tiles)]
        parts.append(jnp.concatenate(tile + [tail], axis=1)[:, :sensors])
    return parts


def forward_kernel(
    steps, chips, wanted, share, x_ref, high_ref, low_ref, near_high_ref, near_low_ref, away_ref, home_ref, pad_ref
):
    sensors = high_ref.shape[3]
    per = share // ROWS
    cell = lax.axis_index("cell")
    chip, core = cell // 2, cell % 2
    cells = x_ref.shape[4]
    order = []
    for side in (1 - core, core):
        for s in steps:
            order.append((2 * lax.rem(chip + s, chips) + side) * per)
    rows = len(order) * share

    def whole(ref, near, c, k):
        inside = ref[c, k, NEAR : cells - NEAR]
        return jnp.concatenate([near[c, k, :NEAR], inside, near[c, k, NEAR:]], axis=0)

    for at, k in enumerate(wanted):
        parts = []
        for c in range(2):
            for first in order:
                parts.append(x_ref[pl.ds(first, per), c, k].reshape(share, cells))
        high, low = split(jnp.concatenate(parts, axis=0))
        both = jnp.concatenate([high, low], axis=0)
        terms = []
        for c in range(2):
            wide = product(both, whole(high_ref, near_high_ref, c, k), ((1,), (0,)))
            small = product(high, whole(low_ref, near_low_ref, c, k), ((1,), (0,)))
            terms.append(wide[: 2 * rows] + wide[2 * rows :] + small)
        re = (terms[0][:rows] - terms[1][rows:]).reshape(2, len(steps), share, sensors)
        im = (terms[0][rows:] + terms[1][:rows]).reshape(2, len(steps), share, sensors)
        for side, ref in enumerate((away_ref, home_ref)):
            if len(ref.shape) == 3:
                for s in range(len(steps)):
                    pack(ref, s, (re[side, s], im[side, s]), pad_ref)
            else:
                ref[:, 0, at] = re[side]
                ref[:, 1, at] = im[side]


def forward(returned, matrices, steps, chips, wanted, packed):
    shards, _, _, rows, cells = returned.shape
    sensors = matrices[0].shape[3]
    share = shards * rows // (2 * chips)
    if packed:
        rows = 2 * (sensors // LANES) * share + share + share // 2
        shape = jax.ShapeDtypeStruct((len(steps), rows, LANES), jnp.float32)
    else:
        shape = jax.ShapeDtypeStruct((len(steps), 2, len(wanted), share, sensors), jnp.float32)
    return pl.pallas_call(
        functools.partial(forward_kernel, steps, chips, wanted, share),
        in_specs=[VMEM_SPEC] * 5,
        out_specs=[VMEM_SPEC] * 2,
        out_shape=[shape, shape],
        scratch_shapes=[pltpu.VMEM((2, share, LANES), jnp.float32)],
        compiler_params=grant(16),
        cost_estimate=pl.CostEstimate(
            flops=48 * len(steps) * len(wanted) * share * sensors * cells,
            bytes_accessed=8 * len(wanted) * sensors * cells,
            transcendentals=0,
        ),
    )(returned, *matrices)


def total_kernel(home_ref, away_ref, *refs):
    out_ref = refs[-1]
    held = out_ref.shape[1]
    for k in range(held):
        arrived = [unpack(ref, *out_ref.shape[2:]) for ref in refs[k:-1:held]]
        for c in range(2):
            total = home_ref[0, c, k] + away_ref[0, c, k]
            for parts in arrived:
                total += parts[c]
            out_ref[c, k] = total


def on_device(columns, freq_blocks, causal_cutoffs, band_index, band_rates):
    shards, strips = lax.axis_size("freq"), lax.axis_size("cell")
    chips = strips // 2
    held = columns.shape[1]
    columns, blocks = in_hbm(columns), in_hbm(freq_blocks)
    spectrum, own_inner, own_outer, cutoff, rates = adjoint(
        columns, blocks, band_index, band_rates, causal_cutoffs, shards
    )
    gathered = lax.all_to_all(spectrum, "freq", split_axis=0, concat_axis=0, tiled=True)
    spectrum = middle(gathered, cutoff)
    spectrum, own_inner, own_outer, freq_blocks = lax.optimization_barrier(
        (spectrum, own_inner, own_outer, freq_blocks)
    )
    blocks = in_hbm(freq_blocks)
    returned = lax.all_to_all(spectrum, "freq", split_axis=0, concat_axis=0, tiled=True)
    swap = [(i, i ^ 1) for i in range(strips)]
    pairs = [(i, i + 1) for i in range(1, strips - 1, 2)]
    outer = lax.ppermute(own_outer, "cell", pairs + [(j, i) for i, j in pairs])
    inner = lax.ppermute(own_inner, "cell", swap)
    high, low, near = smooth(blocks, rates)
    near = near_edges(near, own_inner, own_outer, inner, outer, rates)
    matrices = (high, low, *near)
    leaving = []
    if chips > 1:
        for k in range(held):
            away, home = forward(returned, matrices, range(1, chips), chips, (k,), True)
            leaving.append(home + lax.ppermute(away, "cell", swap))
    arrived = []
    for s in range(1, chips):
        pairs = [(i, 2 * ((i // 2 + s) % chips) + i % 2) for i in range(strips)]
        for k in range(held):
            arrived.append(lax.ppermute(leaving[k][s - 1], "cell", pairs))
    away, home = forward(returned, matrices, range(1), chips, range(held), False)
    away = lax.ppermute(away, "cell", swap)
    share, sensors = home.shape[3:]
    return pl.pallas_call(
        total_kernel,
        in_specs=[VMEM_SPEC] * (2 + len(arrived)),
        out_specs=VMEM_SPEC,
        out_shape=jax.ShapeDtypeStruct((2, held, share, sensors), jnp.float32),
        compiler_params=grant(16),
        name="total",
    )(home, away, *arrived)


def solution(mesh):
    placed = (P(None, "freq", None, None), P(None, "freq", None, "cell"), P(), P("cell"), P())
    return jax.shard_map(
        on_device,
        mesh=mesh,
        in_specs=placed,
        out_specs=P(None, "freq", "cell", None),
        check_vma=False,
    )
```

```python
import functools
import math

import jax
import jax.numpy as jnp
import numpy as np
from jax import lax
from jax.experimental import pallas as pl
from jax.experimental.pallas import tpu as pltpu
from jax.sharding import PartitionSpec as P


SWEEPS = 4
BANDS = 8
ROWS = 8
LANES = 128
UNROLLED_FREQS = 32
GROUPS = LANES // SWEEPS
NEAR = 2 * ROWS


VMEM_SPEC = pl.BlockSpec(memory_space=pltpu.VMEM)
HBM_SPEC = pl.BlockSpec(memory_space=pltpu.HBM)


def grant(mib):
    return pltpu.CompilerParams(vmem_limit_bytes=mib * 2**20)


def in_hbm(x):
    return pltpu.with_memory_space_constraint(x, pltpu.HBM)


def split(x):
    high = x.astype(jnp.bfloat16)
    return high, (x - high.astype(jnp.float32)).astype(jnp.bfloat16)


def product(a, b, contract):
    return lax.dot_general(a, b, (contract, ((), ())), preferred_element_type=jnp.float32)


def inverse_table(steps, freqs):
    cycle = 2 * steps
    turns = np.outer(np.arange(steps), np.arange(freqs)) % cycle
    angle = turns * (2.0 * math.pi / cycle)
    weight = np.where((np.arange(freqs) == 0) | (np.arange(freqs) == freqs - 1), 1.0, 2.0) / cycle
    return weight * np.cos(angle), -weight * np.sin(angle)


def forward_table(steps, freqs):
    cycle = 2 * steps
    turns = np.outer(np.arange(freqs), np.arange(steps)) % cycle
    angle = turns * (2.0 * math.pi / cycle)
    return np.cos(angle), -np.sin(angle)


def rates_of(band_ref, rates_ref):
    band = band_ref[...]
    rates = jnp.zeros(band.shape, jnp.float32)
    for b in range(BANDS):
        rates = jnp.where(band == b, rates_ref[b], rates)
    return rates


def packed_of(sensors):
    return -(-sensors // (ROWS * GROUPS)) * ROWS


def adjoint_kernel(
    v_hbm, f_hbm, band_hbm, rates_hbm, cut_hbm, out_ref, inner_ref, outer_ref, cutoff_ref, spread_ref,
    v_ref, f_ref, band_ref, rates_ref, cut_ref, v_sem, f_sem, small_sem,
):
    shards, _, held, rows, cells = out_ref.shape
    cols, sensors = v_ref.shape[2:]
    v_copies, f_copies = [], []
    for k in range(held):
        v_copies.append(pltpu.make_async_copy(v_hbm.at[:, k], v_ref.at[:, k], v_sem.at[k]))
        v_copies[k].start()
        for c in range(2):
            copy = pltpu.make_async_copy(f_hbm.at[c, k], f_ref.at[c, k], f_sem.at[2 * k + c])
            f_copies.append(copy)
            copy.start()
    small = []
    for at, (source, target) in enumerate(((band_hbm, band_ref), (rates_hbm, rates_ref), (cut_hbm, cut_ref))):
        small.append(pltpu.make_async_copy(source, target, small_sem.at[at]))
        small[at].start()
    odd = lax.axis_index("cell") % 2
    last = cells - LANES
    inner_at, inner_shift = pl.multiple_of((1 - odd) * last, LANES), (1 - odd) * SWEEPS
    outer_at, outer_shift = pl.multiple_of(odd * last, LANES), odd * SWEEPS
    lane_group = lax.broadcasted_iota(jnp.int32, (ROWS, LANES), 1) // SWEEPS
    packed_rows = packed_of(sensors)

    def edge(at, block):
        for ref, lanes, shift in ((inner_ref, inner_at, inner_shift), (outer_ref, outer_at, outer_shift)):
            for first in range(0, sensors, ROWS * GROUPS):
                packed = jnp.zeros((ROWS, LANES), jnp.float32)
                for group in range(min(GROUPS, (sensors - first) // ROWS)):
                    rows_at = first + group * ROWS
                    cells_there = block[rows_at : rows_at + ROWS, pl.ds(lanes, LANES)]
                    moved = pltpu.roll(cells_there, group * SWEEPS + shift, 1)
                    packed = jnp.where(lane_group == group, moved, packed)
                place = at * packed_rows + first // GROUPS
                ref[place : place + ROWS] = packed

    for copy in v_copies + f_copies:
        copy.wait()
    for k in range(held):
        high, low = split(v_ref[:, k].reshape(2 * cols, sensors))
        parts = jnp.concatenate([high, low], axis=0)
        sums = []
        for c in range(2):
            f_high, f_low = split(f_ref[c, k])
            both = product(parts, f_high, ((1,), (0,)))
            both = both[: 2 * cols] + both[2 * cols :] + product(high, f_low, ((1,), (0,)))
            sums.append(both)
        re = sums[0][:cols] + sums[1][cols:]
        im = sums[0][cols:] - sums[1][:cols]
        out_ref[:, 0, k] = re.reshape(shards, rows, cells)
        out_ref[:, 1, k] = im.reshape(shards, rows, cells)
        for c in range(2):
            edge(c * held + k, f_ref.at[c, k])
    for copy in small:
        copy.wait()
    rates = rates_of(band_ref, rates_ref)
    spread_ref[...] = jnp.broadcast_to(rates, spread_ref.shape)
    for ref, at in ((inner_ref, 1 - odd), (outer_ref, odd)):
        facing = jnp.where(at == 0, rates[:, :LANES], rates[:, last:])
        ref[2 * held * packed_rows :] = jnp.broadcast_to(facing, (ROWS, LANES))
    base = lax.axis_index("freq") * rows
    row = lax.broadcasted_iota(jnp.int32, (rows, LANES), 0)
    cutoff = jnp.zeros((rows, LANES), jnp.int32)
    for r in range(rows):
        cutoff = jnp.where(row == r, cut_ref[base + r], cutoff)
    cutoff_ref[...] = cutoff


def adjoint(columns, blocks, band_index, band_rates, causal_cutoffs, shards):
    _, held, cols, sensors = columns.shape
    cells = blocks.shape[3]
    out = (shards, 2, held, cols // shards, cells)
    edge = jax.ShapeDtypeStruct((2 * held * packed_of(sensors) + ROWS, LANES), jnp.float32)
    return pl.pallas_call(
        adjoint_kernel,
        in_specs=[HBM_SPEC] * 5,
        out_specs=[VMEM_SPEC] * 5,
        out_shape=[
            jax.ShapeDtypeStruct(out, jnp.float32),
            edge,
            edge,
            jax.ShapeDtypeStruct((cols // shards, LANES), jnp.int32),
            jax.ShapeDtypeStruct((ROWS, cells), jnp.float32),
        ],
        scratch_shapes=[
            pltpu.VMEM(columns.shape, jnp.float32),
            pltpu.VMEM(blocks.shape, jnp.float32),
            pltpu.VMEM((1, cells), jnp.int32),
            pltpu.SMEM(band_rates.shape, jnp.float32),
            pltpu.SMEM(causal_cutoffs.shape, jnp.int32),
            pltpu.SemaphoreType.DMA((held,)),
            pltpu.SemaphoreType.DMA((2 * held,)),
            pltpu.SemaphoreType.DMA((3,)),
        ],
        compiler_params=grant(16),
        cost_estimate=pl.CostEstimate(
            flops=24 * held * cols * sensors * cells, bytes_accessed=8 * held * sensors * cells, transcendentals=0
        ),
        name="adjoint",
    )(columns, blocks, in_hbm(band_index.reshape(1, cells)), in_hbm(band_rates), in_hbm(causal_cutoffs))


def middle_kernel(x_ref, cutoff_ref, out_hbm, out_ref, out_sem):
    shards, _, held, _, cells = x_ref.shape
    freqs = shards * held
    steps = freqs - 1
    half = freqs // 2
    to_cos, to_sin = inverse_table(steps, freqs)
    from_cos, from_sin = forward_table(steps, freqs)
    cutoff = cutoff_ref[...]
    copies = []
    for lane in range(0, cells, LANES):
        at = pl.ds(lane, LANES)
        even, odd = [], []
        for k in range(half):
            a, b = divmod(k, held)
            c, d = divmod(freqs - 1 - k, held)
            re, im = x_ref[a, 0, b, :, at], x_ref[a, 1, b, :, at]
            re2, im2 = x_ref[c, 0, d, :, at], x_ref[c, 1, d, :, at]
            even += [re + re2, im - im2]
            odd += [re - re2, im + im2]
        series = []
        for t in range(steps):
            total = None
            for k in range(half):
                pair = odd if t % 2 else even
                for value, table in ((pair[2 * k], to_cos), (pair[2 * k + 1], to_sin)):
                    term = value * float(table[t, k])
                    total = term if total is None else total + term
            series.append(jnp.where(cutoff > t, total, 0.0))
        for k in range(half):
            a, b = divmod(k, held)
            c, d = divmod(freqs - 1 - k, held)
            sums = []
            for table in (from_cos, from_sin):
                for parity in (0, 1):
                    total = None
                    for t in range(parity, steps, 2):
                        term = series[t] * float(table[k, t])
                        total = term if total is None else total + term
                    sums.append(total)
            out_ref[a, 0, b, :, at] = sums[0] + sums[1]
            out_ref[c, 0, d, :, at] = sums[0] - sums[1]
            out_ref[a, 1, b, :, at] = sums[2] + sums[3]
            out_ref[c, 1, d, :, at] = sums[3] - sums[2]
        source, target = out_ref.at[:, :, :, :, at], out_hbm.at[:, :, :, :, at]
        copy = pltpu.make_async_copy(source, target, out_sem.at[lane // LANES])
        copies.append(copy)
        copy.start()
    for copy in copies:
        copy.wait()


def middle(gathered, cutoff):
    shards, _, held, rows, cells = gathered.shape
    freqs = shards * held
    steps = freqs - 1
    if freqs <= UNROLLED_FREQS and freqs % 2 == 0:
        return pl.pallas_call(
            middle_kernel,
            in_specs=[VMEM_SPEC, VMEM_SPEC],
            out_specs=HBM_SPEC,
            out_shape=pltpu.HBM(gathered.shape, jnp.float32),
            scratch_shapes=[
                pltpu.VMEM(gathered.shape, jnp.float32),
                pltpu.SemaphoreType.DMA((cells // LANES,)),
            ],
            compiler_params=grant(8),
            cost_estimate=pl.CostEstimate(
                flops=8 * freqs * steps * rows * cells, bytes_accessed=16 * freqs * rows * cells, transcendentals=0
            ),
            name="middle",
        )(gathered, cutoff)
    to_time = jnp.asarray(np.concatenate(inverse_table(steps, freqs), axis=1), jnp.float32)
    to_freq = jnp.asarray(np.concatenate(forward_table(steps, freqs), axis=0), jnp.float32)
    x = gathered.transpose(1, 0, 2, 3, 4).reshape(2 * freqs, rows * cells)
    series = jnp.dot(to_time, x, precision=lax.Precision.HIGHEST).reshape(steps, rows, cells)
    moment = lax.broadcasted_iota(jnp.int32, (steps, rows), 0)
    series = jnp.where((moment < cutoff[None, :, 0])[:, :, None], series, 0.0)
    x = jnp.dot(to_freq, series.reshape(steps, rows * cells), precision=lax.Precision.HIGHEST)
    return x.reshape(2, shards, held, rows, cells).transpose(1, 0, 2, 3, 4)


def diagonals_of(rates):
    width = rates.shape[1]
    diagonals = jnp.where(lax.broadcasted_iota(jnp.int32, (2 * ROWS, width), 0) == ROWS, 1.0, 0.0)
    for _ in range(SWEEPS):
        up = pltpu.roll(pltpu.roll(diagonals, 1, 1), 2 * ROWS - 1, 0)
        down = pltpu.roll(pltpu.roll(diagonals, width - 1, 1), 1, 0)
        diagonals = diagonals + rates * (up - 2.0 * diagonals + down)
    return diagonals


def spread(diagonals, offset):
    tile = jnp.zeros(offset.shape, jnp.float32)
    for o in range(-SWEEPS, SWEEPS + 1):
        tile = jnp.where(offset == o, diagonals[ROWS + o : ROWS + o + 1], tile)
    return tile


def smooth_kernel(f_hbm, rates_ref, high_ref, low_ref, near_ref, f_ref, a_both, f_sem):
    _, held, _, cells = f_hbm.shape
    copies = []
    for at in range(2 * held):
        c, k = divmod(at, held)
        copies.append(pltpu.make_async_copy(f_hbm.at[c, k], f_ref.at[c, k], f_sem.at[at]))
        copies[at].start()
    diagonals = diagonals_of(jnp.concatenate([rates_ref[:1], jnp.zeros((1, LANES), jnp.float32)], axis=1))
    for lanes in range(0, cells, LANES):
        column = lax.broadcasted_iota(jnp.int32, (LANES, LANES), 1)
        row = lax.broadcasted_iota(jnp.int32, (LANES, LANES), 0)
        for rows in range(0, cells, LANES):
            high, low = split(spread(diagonals[:, lanes : lanes + LANES], row - column + (rows - lanes)))
            a_both[rows : rows + LANES, lanes : lanes + LANES] = high
            a_both[cells + rows : cells + rows + LANES, lanes : lanes + LANES] = low
    for at in range(2 * held):
        c, k = divmod(at, held)
        copies[at].wait()
        high, low = split(f_ref[c, k])
        both = product(a_both[...], high, ((1,), (1,)))
        total = both[:cells] + both[cells:] + product(a_both[:cells], low, ((1,), (1,)))
        high, low = split(total)
        high_ref[c, k] = high
        low_ref[c, k] = low
        near_ref[c, k, :NEAR] = total[:NEAR]
        near_ref[c, k, NEAR:] = total[cells - NEAR :]


def smooth(blocks, rates):
    _, held, sensors, cells = blocks.shape
    shape = jax.ShapeDtypeStruct((2, held, cells, sensors), jnp.bfloat16)
    return pl.pallas_call(
        smooth_kernel,
        in_specs=[HBM_SPEC, VMEM_SPEC],
        out_specs=[VMEM_SPEC] * 3,
        out_shape=[shape, shape, jax.ShapeDtypeStruct((2, held, 2 * NEAR, sensors), jnp.float32)],
        scratch_shapes=[
            pltpu.VMEM(blocks.shape, jnp.float32),
            pltpu.VMEM((2 * cells, cells), jnp.bfloat16),
            pltpu.SemaphoreType.DMA((2 * held,)),
        ],
        compiler_params=grant(16),
        cost_estimate=pl.CostEstimate(
            flops=12 * held * sensors * cells * cells, bytes_accessed=16 * held * sensors * cells, transcendentals=0
        ),
        name="smooth",
    )(blocks, rates)


def near_kernel(
    near_ref, own_inner_ref, own_outer_ref, inner_ref, outer_ref, rates_ref, high_ref, low_ref, sides
):
    held = near_ref.shape[1]
    sensors = near_ref.shape[3]
    cells = rates_ref.shape[1]
    even = lax.axis_index("cell") % 2 == 0
    kinds = 4
    per = kinds * SWEEPS
    pairs = LANES // (2 * per)

    def parts(first):
        rows = slice(first, first + ROWS)
        own_inner, own_outer = own_inner_ref[rows], own_outer_ref[rows]
        inner, outer = inner_ref[rows], outer_ref[rows]
        return (
            jnp.where(even, own_outer, own_inner),
            jnp.where(even, own_inner, own_outer),
            jnp.where(even, inner, outer),
            jnp.where(even, outer, inner),
        )

    lane = lax.broadcasted_iota(jnp.int32, (ROWS, LANES), 1)
    packed_rows = packed_of(sensors)
    _, _, after, before = parts(2 * held * packed_rows)
    side = jnp.where(lane < SWEEPS, after, jnp.where(lane >= LANES - SWEEPS, before, 0.0))[:1]
    own = rates_ref[:1]
    alone = diagonals_of(jnp.concatenate([own, jnp.zeros((1, LANES), jnp.float32)], axis=1))
    full = diagonals_of(jnp.concatenate([own, side], axis=1))
    first = full[:, :LANES] - alone[:, :LANES]
    last = full[:, cells - LANES : cells] - alone[:, cells - LANES : cells]
    beyond = full[:, cells:]
    kind = lax.broadcasted_iota(jnp.int32, (2 * ROWS, LANES), 1) // SWEEPS
    change = jnp.where(kind == 0, first, 0.0)
    change = jnp.where(kind == 1, pltpu.roll(last, 2 * SWEEPS, 1), change)
    change = jnp.where(kind == 2, pltpu.roll(beyond, 2 * SWEEPS, 1), change)
    change = jnp.where(kind == 3, pltpu.roll(beyond, 4 * SWEEPS, 1), change)
    for shift in (per, 2 * per, 4 * per):
        change = change + pltpu.roll(change, shift, 1)
    row = lax.broadcasted_iota(jnp.int32, (2 * NEAR, LANES), 0)
    column = lax.broadcasted_iota(jnp.int32, (2 * NEAR, LANES), 1)
    kind, i = (column // SWEEPS) % kinds, column % SWEEPS
    at_first = jnp.where(kind == 0, row - i, jnp.where(kind == 3, row + SWEEPS - i, LANES))
    end = row - 2 * NEAR
    at_last = jnp.where(kind == 1, end + SWEEPS - i, jnp.where(kind == 2, end - i, LANES))
    matrix = spread(change, jnp.where(row < NEAR, at_first, at_last))
    a_high, a_low = split(matrix)
    owner = column // per
    cell_of = lane // SWEEPS
    for begin_at in range(0, 2 * held, pairs):
        ats = range(begin_at, min(2 * held, begin_at + pairs))
        for begin in range(0, sensors, ROWS * GROUPS):
            values = [value for at in ats for value in parts(at * packed_rows + begin // GROUPS)]
            values = [pltpu.roll(value, n * SWEEPS, 1) if n else value for n, value in enumerate(values)]
            for group in range(min(GROUPS, (sensors - begin) // ROWS)):
                tile = jnp.zeros((ROWS, LANES), jnp.float32)
                for n, value in enumerate(values):
                    tile = jnp.where(cell_of == (group + n) % GROUPS, value, tile)
                tile = pltpu.roll(tile, (LANES - group * SWEEPS) % LANES, 1)
                rows_at = begin + group * ROWS
                sides[rows_at : rows_at + ROWS] = tile + pltpu.roll(tile, LANES // 2, 1)
        high, low = split(sides[...])
        low_lane = lax.broadcasted_iota(jnp.int32, (sensors, LANES), 1) >= LANES // 2
        operand = jnp.where(low_lane, low.astype(jnp.float32), high.astype(jnp.float32)).astype(jnp.bfloat16)
        left = []
        for p in range(len(ats)):
            left.append(jnp.where(owner % pairs == p, a_high.astype(jnp.float32), 0.0))
            left.append(jnp.where(owner == p, a_low.astype(jnp.float32), 0.0))
        left = jnp.concatenate(left, axis=0).astype(jnp.bfloat16)
        terms = product(left, operand, ((1,), (1,)))
        for p, at in enumerate(ats):
            c, k = divmod(at, held)
            mine = terms[4 * NEAR * p : 4 * NEAR * (p + 1)]
            high, low = split(near_ref[c, k] + mine[: 2 * NEAR] + mine[2 * NEAR :])
            high_ref[c, k] = high
            low_ref[c, k] = low


def near_edges(near, own_inner, own_outer, inner, outer, rates):
    shape = jax.ShapeDtypeStruct(near.shape, jnp.bfloat16)
    held, sensors = near.shape[1], near.shape[3]
    return pl.pallas_call(
        near_kernel,
        in_specs=[VMEM_SPEC] * 6,
        out_specs=[VMEM_SPEC] * 2,
        out_shape=[shape, shape],
        scratch_shapes=[pltpu.VMEM((sensors, LANES), jnp.float32)],
        compiler_params=grant(8),
        cost_estimate=pl.CostEstimate(
            flops=24 * held * sensors * NEAR * LANES, bytes_accessed=8 * near.size, transcendentals=0
        ),
        name="near_edges",
    )(near, own_inner, own_outer, inner, outer, rates)


def forward_kernel(
    steps, chips, wanted, x_ref, high_ref, low_ref, near_high_ref, near_low_ref, away_ref, home_ref
):
    share, sensors = home_ref.shape[3:]
    per = share // ROWS
    cell = lax.axis_index("cell")
    chip, core = cell // 2, cell % 2
    cells = x_ref.shape[4]
    order = []
    for side in (1 - core, core):
        for s in steps:
            order.append((2 * lax.rem(chip + s, chips) + side) * per)
    rows = len(order) * share

    def whole(ref, near, c, k):
        inside = ref[c, k, NEAR : cells - NEAR]
        return jnp.concatenate([near[c, k, :NEAR], inside, near[c, k, NEAR:]], axis=0)

    for at, k in enumerate(wanted):
        parts = []
        for c in range(2):
            for first in order:
                parts.append(x_ref[pl.ds(first, per), c, k].reshape(share, cells))
        high, low = split(jnp.concatenate(parts, axis=0))
        both = jnp.concatenate([high, low], axis=0)
        terms = []
        for c in range(2):
            wide = product(both, whole(high_ref, near_high_ref, c, k), ((1,), (0,)))
            small = product(high, whole(low_ref, near_low_ref, c, k), ((1,), (0,)))
            terms.append(wide[: 2 * rows] + wide[2 * rows :] + small)
        re = (terms[0][:rows] - terms[1][rows:]).reshape(2, len(steps), share, sensors)
        im = (terms[0][rows:] + terms[1][:rows]).reshape(2, len(steps), share, sensors)
        for side, ref in enumerate((away_ref, home_ref)):
            ref[:, 0, at] = re[side]
            ref[:, 1, at] = im[side]


def forward(returned, matrices, steps, chips, wanted):
    shards, _, _, rows, cells = returned.shape
    sensors = matrices[0].shape[3]
    share = shards * rows // (2 * chips)
    shape = jax.ShapeDtypeStruct((len(steps), 2, len(wanted), share, sensors), jnp.float32)
    return pl.pallas_call(
        functools.partial(forward_kernel, steps, chips, wanted),
        in_specs=[VMEM_SPEC] * 5,
        out_specs=[VMEM_SPEC] * 2,
        out_shape=[shape, shape],
        compiler_params=grant(16),
        cost_estimate=pl.CostEstimate(
            flops=48 * len(steps) * len(wanted) * share * sensors * cells,
            bytes_accessed=8 * len(wanted) * sensors * cells,
            transcendentals=0,
        ),
    )(returned, *matrices)


def total_kernel(stay_ref, *refs):
    out_ref = refs[-1]
    held = out_ref.shape[1]
    for k in range(held):
        total = stay_ref[0, :, k]
        for ref in refs[k:-1:held]:
            total += ref[:, 0]
        out_ref[:, k] = total


def on_device(columns, freq_blocks, causal_cutoffs, band_index, band_rates):
    shards, strips = lax.axis_size("freq"), lax.axis_size("cell")
    chips = strips // 2
    held = columns.shape[1]
    columns, blocks = in_hbm(columns), in_hbm(freq_blocks)
    spectrum, own_inner, own_outer, cutoff, rates = adjoint(
        columns, blocks, band_index, band_rates, causal_cutoffs, shards
    )
    gathered = lax.all_to_all(spectrum, "freq", split_axis=0, concat_axis=0, tiled=True)
    spectrum = middle(gathered, cutoff)
    spectrum, own_inner, own_outer, freq_blocks = lax.optimization_barrier(
        (spectrum, own_inner, own_outer, freq_blocks)
    )
    blocks = in_hbm(freq_blocks)
    returned = lax.all_to_all(spectrum, "freq", split_axis=0, concat_axis=0, tiled=True)
    swap = [(i, i ^ 1) for i in range(strips)]
    pairs = [(i, i + 1) for i in range(1, strips - 1, 2)]
    outer = lax.ppermute(own_outer, "cell", pairs + [(j, i) for i, j in pairs])
    inner = lax.ppermute(own_inner, "cell", swap)
    high, low, near = smooth(blocks, rates)
    near = near_edges(near, own_inner, own_outer, inner, outer, rates)
    matrices = (high, low, *near)
    leaving = []
    if chips > 1:
        for k in range(held):
            away, home = forward(returned, matrices, range(1, chips), chips, (k,))
            leaving.append(home + lax.ppermute(away, "cell", swap))
    arrived = []
    for s in range(1, chips):
        pairs = [(i, 2 * ((i // 2 + s) % chips) + i % 2) for i in range(strips)]
        for k in range(held):
            arrived.append(lax.ppermute(leaving[k][s - 1], "cell", pairs))
    away, home = forward(returned, matrices, range(1), chips, range(held))
    away = lax.ppermute(away, "cell", swap)
    share, sensors = home.shape[3:]
    return pl.pallas_call(
        total_kernel,
        in_specs=[VMEM_SPEC] * (1 + len(arrived)),
        out_specs=VMEM_SPEC,
        out_shape=jax.ShapeDtypeStruct((2, held, share, sensors), jnp.float32),
        compiler_params=grant(16),
        name="total",
    )(home + away, *arrived)


def solution(mesh):
    placed = (P(None, "freq", None, None), P(None, "freq", None, "cell"), P(), P("cell"), P())
    return jax.shard_map(
        on_device,
        mesh=mesh,
        in_specs=placed,
        out_specs=P(None, "freq", "cell", None),
        check_vma=False,
    )
```
